32 devices in a mesh: batch: 8 (over y, x, core), chan: 4 (over z).
Axes of the slice: x: 2, y: 2, z: 4, core: 2. Of those that a mesh axis runs over, the one named last changes fastest.
Arguments:
- images: bfloat16 [64, 14, 14, 4096], P('batch', None, None, 'chan'), may hold values from -12 to 12, as said below
- reduce_weight: bfloat16 [4096, 1024], P(None, 'chan'), may hold values from -0.09375 to 0.09375
- reduce_gain: float32 [1024], P('chan'), may hold values from 0.25 to 1.75
- reduce_bias: float32 [1024], P('chan'), may hold values from -0.5 to 0.5
- spatial_weight: bfloat16 [3, 3, 1024, 1024], P(None, None, None, 'chan'), may hold values from -0.0625 to 0.0625
- spatial_gain: float32 [1024], P('chan'), may hold values from 0.25 to 1.75
- spatial_bias: float32 [1024], P('chan'), may hold values from -0.5 to 0.5
- expand_weight: bfloat16 [1024, 4096], P(None, 'chan'), may hold values from -0.1875 to 0.1875
- expand_gain: float32 [4096], P('chan'), may hold values from 0.25 to 1.75
- expand_bias: float32 [4096], P('chan'), may hold values from -0.5 to 0.5
Outputs:
- block_out: bfloat16 [64, 14, 14, 4096], P('batch', None, None, 'chan')
The draws below stay inside these ranges and needn't reach their ends.
Inputs may be any that keep to these rules, and one draw needn't show every extreme that they name: In the images, the per-channel mean and scale differ from one block of 8 images to the next.
All inputs are finite; a program needn't handle non-finite values.
Results may differ from the reference program's by a relative error of at most 0.0047.
Values may be sent and summed in bfloat16 or wider, within the bound.
A program may use at most 128 MiB of HBM per device.

```python
import jax
import jax.numpy as jnp
from jax import lax

CIN = 4096
MID = 1024
SIDE = 14
IMG_DEV = 8
IMAGES = 64


def draw_images(key, part):
    k_offset, k_scale, k_base = jax.random.split(jax.random.fold_in(key, 11), 3)
    groups = IMAGES // IMG_DEV
    offset = jnp.clip(1.5 * jax.random.normal(k_offset, (groups, 1, 1, 1, CIN), jnp.float32), -3.0, 3.0)
    scales = jnp.exp(jax.random.uniform(k_scale, (groups, 1, 1, 1, CIN), jnp.float32, -0.693, 0.693))
    shape = (groups, IMG_DEV, SIDE, SIDE, CIN)
    base = jnp.clip(jax.random.normal(k_base, shape, jnp.float32), -4.0, 4.0)
    values = jnp.clip(offset + scales * base, -12.0, 12.0)
    return values.reshape(IMAGES, SIDE, SIDE, CIN).astype(jnp.bfloat16)


def steps_of(key, shape, shards, least, top_value):
    level, own = 1.0, jax.random.fold_in(key, 6)
    for position, shards_of in shards:
        steps = jnp.exp(jax.random.uniform(jax.random.fold_in(own, position), (shards_of,), jnp.float32, least / len(shards), top_value / len(shards)))
        level = level * jnp.repeat(steps, shape[position] // shards_of).reshape([-1 if axis == position else 1 for axis in range(len(shape))])
    return level


def normal_values(rng, shape, spread, reach, cuts=(), dtype=jnp.bfloat16):
    level = steps_of(rng, shape, cuts, -0.22, 0.18) if cuts else 1.0
    array = jax.random.normal(rng, shape, jnp.float32) * spread * level
    return jnp.minimum(jnp.maximum(array, -reach), reach).astype(dtype)


def setup_inputs(seed: int = 0) -> dict:
    streams_of = jax.random.split(jax.random.key(seed), 11)
    images = draw_images(jax.random.fold_in(streams_of[10], 71), 0)
    reduce_weight = normal_values(streams_of[1], (CIN, MID), CIN ** -0.5, 0.09375, ((1, 4),))
    reduce_gain = jnp.clip(1.0 + 0.15 * jax.random.normal(streams_of[2], (MID,), jnp.float32), 0.25, 1.75)
    reduce_bias = jnp.clip(jax.random.uniform(streams_of[3], (MID,), jnp.float32, -0.5, 0.5) * steps_of(streams_of[3], (MID,), ((0, 4),), -0.4, 0.0), -0.5, 0.5)
    spatial_weight = normal_values(streams_of[4], (3, 3, MID, MID), (9 * MID) ** -0.5, 0.0625, ((3, 4),))
    spatial_gain = jnp.clip(1.0 + 0.15 * jax.random.normal(streams_of[5], (MID,), jnp.float32), 0.25, 1.75)
    spatial_bias = jnp.clip(jax.random.uniform(streams_of[6], (MID,), jnp.float32, -0.5, 0.5) * steps_of(streams_of[6], (MID,), ((0, 4),), -0.4, 0.0), -0.5, 0.5)
    expand_weight = normal_values(streams_of[7], (MID, CIN), MID ** -0.5, 0.1875, ((1, 4),))
    expand_gain = jnp.clip(1.0 + 0.15 * jax.random.normal(streams_of[8], (CIN,), jnp.float32), 0.25, 1.75)
    expand_bias = jnp.clip(jax.random.uniform(streams_of[9], (CIN,), jnp.float32, -0.5, 0.5) * steps_of(streams_of[9], (CIN,), ((0, 4),), -0.4, 0.0), -0.5, 0.5)
    return dict(images=images, reduce_weight=reduce_weight, reduce_gain=reduce_gain, reduce_bias=reduce_bias, spatial_weight=spatial_weight, spatial_gain=spatial_gain, spatial_bias=spatial_bias, expand_weight=expand_weight, expand_gain=expand_gain, expand_bias=expand_bias)


eps = 0.001

def batch_norm(values, gain, bias):
    mean = lax.optimization_barrier(jnp.mean(values, axis=(0, 1, 2)))
    centred = values - mean
    var = lax.optimization_barrier(jnp.mean(centred * centred, axis=(0, 1, 2)))
    return centred * (gain / jnp.sqrt(var + eps)) + bias

def pointwise(maps, weight):
    flat = maps.reshape(-1, maps.shape[-1])
    out = jnp.dot(flat, weight, preferred_element_type=jnp.float32)
    return out.reshape(maps.shape[:-1] + (weight.shape[1],))

def reference(images, reduce_weight, reduce_gain, reduce_bias, spatial_weight, spatial_gain, spatial_bias, expand_weight, expand_gain, expand_bias):
    first = pointwise(images, reduce_weight)
    act_one = jnp.maximum(batch_norm(first, reduce_gain, reduce_bias), 0.0).astype(jnp.bfloat16)
    padded = jnp.pad(act_one, ((0, 0), (1, 1), (1, 1), (0, 0)))
    second = jnp.zeros(act_one.shape[:-1] + (spatial_weight.shape[3],), jnp.float32)
    for row_tap in range(3):
        for col_tap in range(3):
            window = padded[:, row_tap:row_tap + SIDE, col_tap:col_tap + SIDE, :]
            second = second + pointwise(window, spatial_weight[row_tap, col_tap])
    act_two = jnp.maximum(batch_norm(second, spatial_gain, spatial_bias), 0.0).astype(jnp.bfloat16)
    third = pointwise(act_two, expand_weight)
    summed = batch_norm(third, expand_gain, expand_bias) + images.astype(jnp.float32)
    return jnp.maximum(summed, 0.0).astype(jnp.bfloat16)
```

```python
import functools

import jax
import jax.numpy as jnp
from jax import lax
from jax.experimental import pallas as pl
from jax.experimental.pallas import tpu as pltpu
from jax.sharding import PartitionSpec as P

eps = 0.001
MESH = pl.DeviceIdType.MESH
LIMIT = 63 * 1024 * 1024
SKEW = 3
SINK = 1
HELD = 3
READY = 12


def remote(src, dst, send, recv, device):
    return pltpu.make_async_remote_copy(
        src_ref=src, dst_ref=dst, send_sem=send, recv_sem=recv,
        device_id=device, device_id_type=MESH,
    )


def greet(n, nb, z, b):
    barrier = pltpu.get_barrier_semaphore()
    for off in range(1, n):
        pl.semaphore_signal(
            barrier, inc=1, device_id={"chan": lax.rem(z + off, n)}, device_id_type=MESH
        )
    for off in range(1, nb):
        pl.semaphore_signal(
            barrier, inc=1, device_id={"batch": lax.rem(b + off, nb)}, device_id_type=MESH
        )
    pl.semaphore_wait(barrier, n + nb - 2)


def stats_send(nb, b, stats, send, recv):
    for off in range(1, nb):
        peer = lax.rem(b + off, nb)
        remote(stats.at[b], stats.at[b], send.at[off], recv.at[b], {"batch": peer}).start()


def stats_wait(nb, b, stats, send, recv):
    for off in range(1, nb):
        peer = lax.rem(b + off, nb)
        remote(stats.at[b], stats.at[peer], send.at[off], recv.at[peer], {"batch": peer}).wait()


def combine(stats, local):
    nb = stats.shape[0]
    means = stats[:, 0:1, :]
    mean = jnp.sum(means, axis=0) / nb
    away = means - mean[None]
    spread = jnp.sum(stats[:, 1:2, :], axis=0) + local * jnp.sum(away * away, axis=0)
    return mean, spread / (local * nb)


def column_sum(value):
    return jnp.sum(value, axis=0, keepdims=True)


def block_kernel(
    n, nb, imgs,
    img_hbm, w1_hbm, gain1, bias1, sw_hbm, gain2, bias2, w3_hbm, gain3, bias3,
    out_hbm,
    img, w1, wown, part, whole, flow, gb, shift1, sum1, square1, stat1, act, w2, acc, sec,
    shift2, sum2, square2, stat2, affine, w3, third, shift3, sum3, square3, stat3, outv,
    load_sem, out_sem,
    gb_send, gb_recv, w1_send, w1_recv, hop_send, hop_recv, pair_send, pair_recv,
    flow_send, flow_recv, st1_send, st1_recv,
    w2_send, w2_recv, w2hop_send, w2hop_recv, w2pair_send, w2pair_recv,
    sec_send, sec_recv, st2_send, st2_recv, aff_send, aff_recv, st3_send, st3_recv,
):
    z, b = lax.axis_index("chan"), lax.axis_index("batch")
    rows, height, depth = img.shape
    width = wown.shape[2]
    half = acc.shape[2]
    pieces, tall, out_local = third.shape
    join = rows // pieces
    mids = n // 2
    hops = nb // 2
    chunks = n * rows
    strip = depth // nb
    band = n * width // nb
    local = rows * height
    unit = half // 2
    per_piece = join * 2
    units = rows * 2
    partner = b + 1 - 2 * lax.rem(b, 2)
    parity = lax.rem(b, 2)
    at_first, at_last = z == 0, z == n - 1
    at_end = jnp.logical_or(at_first, at_last)
    inner = jnp.logical_not(at_end)
    side = jnp.where(at_first, 0, 1)
    owner = jnp.where(z < mids, 0, n - 1)
    my_slot = lax.rem(z, mids)
    f32, bf16 = jnp.float32, jnp.bfloat16

    w1_load = pltpu.make_async_copy(w1_hbm, w1, load_sem.at[0])
    w1_load.start()
    img_load = pltpu.make_async_copy(img_hbm, img, load_sem.at[1])
    img_load.start()
    w3_load = pltpu.make_async_copy(w3_hbm, w3, load_sem.at[2])
    w3_load.start()

    def slot_cols(slot):
        return pl.ds(pl.multiple_of(slot * width, 128), width)

    w2_load = pltpu.make_async_copy(sw_hbm, w2.at[:, :, :, slot_cols(my_slot)], load_sem.at[3])

    @pl.when(at_end)
    def _():
        w2_load.start()

    gb[z, 0:1, :] = gain1[...]
    gb[z, 1:2, :] = bias1[...]
    gb[z, 2:3, :] = gain2[...]
    gb[z, 3:4, :] = bias2[...]
    greet(n, nb, z, b)

    def rows_of(who):
        return pl.ds(pl.multiple_of(who * strip, 16), strip)

    def w1_copy(to):
        src = w1.at[pl.ds(pl.multiple_of(to * depth + b * strip, 16), strip), :]
        return remote(src, wown.at[z, rows_of(b), :], w1_send.at[to], w1_recv.at[z], {"chan": to})

    def gb_copy(to, slot):
        return remote(gb.at[z], gb.at[slot], gb_send.at[to], gb_recv.at[slot], {"chan": to})

    def band_of(who):
        return pl.ds(pl.multiple_of(who * band, 16), band)

    w2_copy = remote(
        sw_hbm.at[:, :, band_of(b), :], w2.at[:, :, band_of(b), slot_cols(my_slot)],
        w2_send.at[0], w2_recv.at[my_slot], {"chan": owner},
    )
    w1_load.wait()
    for far in range(1, n):

        @pl.when(z + far < n)
        def _():
            w1_copy(z + far).start()

        @pl.when(z - far >= 0)
        def _():
            w1_copy(z - far).start()

    for off in range(1, n):
        gb_copy(lax.rem(z + off, n), z).start()

    @pl.when(inner)
    def _():
        w2_copy.start()

    def strip_copy(g, who, send, recv, device):
        ref = wown.at[g, rows_of(who), :]
        return remote(ref, ref, send, recv, device)

    def hop_copy(g, hop):
        peer = lax.rem(b + 2 * hop, nb)
        return strip_copy(g, b, hop_send.at[g, hop], hop_recv.at[g, b], {"batch": peer})

    def pair_copy(g, hop):
        who = lax.rem(b + 2 * hop, nb)
        return strip_copy(g, who, pair_send.at[g, hop], pair_recv.at[g, who], {"batch": partner})

    def distribute(g):
        @pl.when(z != g)
        def _():
            strip_copy(g, b, w1_send.at[0], w1_recv.at[g], {"chan": g}).wait_recv()
            for hop in range(1, hops):
                hop_copy(g, hop).start()
            pair_copy(g, 0).start()

    def forward(g):
        @pl.when(z != g)
        def _():
            for hop in range(1, hops):
                peer = lax.rem(b + 2 * hop, nb)
                strip_copy(
                    g, peer, hop_send.at[g, 0], hop_recv.at[g, peer], {"batch": peer}
                ).wait_recv()
                pair_copy(g, hop).start()

    def complete(g):
        @pl.when(z != g)
        def _():
            for hop in range(hops):
                who = 2 * hop + 1 - parity
                strip_copy(
                    g, who, pair_send.at[g, 0], pair_recv.at[g, who], {"batch": partner}
                ).wait_recv()

    def flow_copy(f, k):
        to = jnp.where(f == 0, lax.rem(z + 1, n), lax.rem(z + n - 1, n))
        ref = flow.at[f, k]
        return remote(ref, ref, flow_send.at[f, k], flow_recv.at[f, k], {"chan": to})

    def chunk_of(f, position):
        q, r = lax.div(position, rows), lax.rem(position, rows)
        return jnp.where(f == 0, q, n - 1 - q) * rows + r

    img_load.wait()

    def own_products(r, carry):
        k = z * rows + r
        value = jnp.dot(
            img[r], w1[pl.ds(pl.multiple_of(z * depth, 16), depth), :], preferred_element_type=f32
        )
        part[k] = value

        @pl.when(at_end)
        def _():
            flow[side, k] = value.astype(bf16)
            flow_copy(side, k).start()

        return carry

    split = rows // 2
    lax.fori_loop(0, split, own_products, 0)
    order = [g for q in range(mids) for g in (q, n - 1 - q)]
    for g in order[:2]:
        distribute(g)
    lax.fori_loop(split, rows, own_products, 0)
    for g in order[2:]:
        distribute(g)
    act[:, 0] = jnp.zeros_like(act[:, 0])
    act[:, rows + 1] = jnp.zeros_like(act[:, 0])
    acc[...] = jnp.zeros_like(acc)
    for g in order[:2]:
        forward(g)

    def band_copy(slot, who, send, recv, device):
        ref = w2.at[:, :, band_of(who), slot_cols(slot)]
        return remote(ref, ref, send, recv, device)

    def w2hop_copy(slot, hop):
        peer = lax.rem(b + 2 * hop, nb)
        return band_copy(slot, b, w2hop_send.at[slot, hop], w2hop_recv.at[slot, b], {"batch": peer})

    def w2pair_copy(slot, hop):
        who = lax.rem(b + 2 * hop, nb)
        return band_copy(
            slot, who, w2pair_send.at[slot, hop], w2pair_recv.at[slot, who], {"batch": partner}
        )

    def each_slot(work):
        for slot in range(mids):

            @pl.when(slot != my_slot)
            def _():
                work(slot)

    def w2_distribute(slot):
        band_copy(slot, b, w2_send.at[0], w2_recv.at[slot], {"chan": z}).wait_recv()
        for hop in range(1, hops):
            w2hop_copy(slot, hop).start()
        w2pair_copy(slot, 0).start()

    def w2_forward(slot):
        for hop in range(1, hops):
            peer = lax.rem(b + 2 * hop, nb)
            band_copy(
                slot, peer, w2hop_send.at[slot, 0], w2hop_recv.at[slot, peer], {"batch": peer}
            ).wait_recv()
            w2pair_copy(slot, hop).start()

    def w2_complete(slot):
        for hop in range(hops):
            who = 2 * hop + 1 - parity
            band_copy(
                slot, who, w2pair_send.at[slot, 0], w2pair_recv.at[slot, who], {"batch": partner}
            ).wait_recv()

    def end_group(q):
        return jnp.where(at_first, n - 1 - q, q)

    def finalize(position):
        f = 1 - side
        k = chunk_of(f, position)
        g, r = lax.div(k, rows), lax.rem(k, rows)
        flow_copy(f, k).wait_recv()
        value = part[k] + flow[f, k].astype(f32)
        whole[lax.rem(lax.div(position, rows), 2), r] = value

        @pl.when(r == 0)
        def _():
            shift1[g] = column_sum(value) / height
            sum1[g] = jnp.zeros_like(sum1[g])
            square1[g] = jnp.zeros_like(square1[g])

        moved = value - shift1[g]
        sum1[g] += column_sum(moved)
        square1[g] += column_sum(moved * moved)

    def first_stats(g):
        extra = sum1[g] / local
        stat1[g, b, 0:1, :] = shift1[g] + extra
        stat1[g, b, 1:2, :] = square1[g] - sum1[g] * extra
        stats_send(nb, b, stat1.at[g], st1_send.at[g], st1_recv.at[g])

    def first_act(q):
        g = end_group(q)
        stats_wait(nb, b, stat1.at[g], st1_send.at[g], st1_recv.at[g])
        mean, var = combine(stat1[g], local)
        scale = gb[g, 0:1, :] / jnp.sqrt(var + eps)
        bias = gb[g, 1:2, :]

        def line(r, carry):
            value = (whole[lax.rem(q, 2), r] - mean) * scale + bias
            act[g, r + 1] = jnp.maximum(value, 0.0).astype(bf16)
            return carry

        lax.fori_loop(0, rows, line, 0)

    def convolve(g, t):
        for col_tap in range(3):
            total = None
            for row_tap in range(3):
                window = act[g, pl.ds(t * join + row_tap, join)].reshape(tall, width)
                weight = w2[row_tap, col_tap, pl.ds(pl.multiple_of(g * width, 128), width), :]
                term = jnp.dot(window, weight, preferred_element_type=f32)
                total = term if total is None else total + term
            total = total.reshape(join, height, half)
            lines = pl.ds(t * join, join)
            if col_tap == 0:
                acc[lines, imgs:, :] += total[:, : height - imgs]
            elif col_tap == 1:
                acc[lines] += total
            else:
                acc[lines, : height - imgs, :] += total[:, imgs:]

    reach = SKEW * (n - 1) + SINK

    def step(s, carry):
        q, r = lax.div(s, rows), lax.rem(s, rows)

        @pl.when(q < mids)
        def _():
            @pl.when(r == 0)
            def _():
                complete(q)
                complete(n - 1 - q)

            @pl.when(jnp.logical_and(r == rows // 2, q + 1 < mids))
            def _():
                forward(q + 1)
                forward(n - 2 - q)

            for g in (q, n - 1 - q):

                @pl.when(z != g)
                def _():
                    part[g * rows + r] = jnp.dot(img[r], wown[g], preferred_element_type=f32)

        for f in range(2):
            from_start = z if f == 0 else n - 1 - z
            position = s - SKEW * from_start
            k = chunk_of(f, position)
            inside = jnp.logical_and(position >= 0, position < chunks)

            @pl.when(jnp.logical_and(inside, jnp.logical_and(from_start == 0, position >= rows)))
            def _():
                flow[f, k] = part[k].astype(bf16)
                flow_copy(f, k).start()

            @pl.when(jnp.logical_and(inside, inner))
            def _():
                flow_copy(f, k).wait_recv()
                flow[f, k] = (part[k] + flow[f, k].astype(f32)).astype(bf16)
                flow_copy(f, k).start()

        @pl.when(at_end)
        def _():
            @pl.when(s == rows // 2)
            def _():
                each_slot(w2_distribute)

            @pl.when(s == rows + rows // 2)
            def _():
                each_slot(w2_forward)

            position = s - reach

            @pl.when(position >= 0)
            def _():
                finalize(position)

            after = position - (rows - 1)

            @pl.when(after >= 0)
            def _():
                q, v = lax.div(after, rows), lax.rem(after, rows)
                g = end_group(q)

                @pl.when(v == 0)
                def _():
                    first_stats(g)

                @pl.when(v == 4)
                def _():
                    @pl.when(q == 0)
                    def _():
                        for to in range(n):

                            @pl.when(z != to)
                            def _():
                                gb_copy(to, to).wait_recv()

                        w2_load.wait()
                        each_slot(w2_complete)

                    first_act(q)

                @pl.when(jnp.logical_and(v >= 5, v < 5 + pieces))
                def _():
                    convolve(g, v - 5)

        return carry

    lax.fori_loop(0, chunks + reach, step, 0)

    def sec_copy(f, u):
        to = jnp.where(f == 0, lax.rem(z + 1, n), lax.rem(z + n - 1, n))
        line, part_of = lax.div(u, 2), lax.rem(u, 2)
        ref = sec.at[f, line, :, pl.ds(pl.multiple_of(part_of * unit, 128), unit)]
        return remote(ref, ref, sec_send.at[f, u], sec_recv.at[f, u], {"chan": to})

    def sec_start(u, carry):
        sec_copy(side, u).start()
        return carry

    def affine_copy(to, f):
        return remote(affine.at[f], affine.at[f], aff_send.at[to], aff_recv.at[f], {"chan": to})

    @pl.when(at_end)
    def _():
        last = end_group(n - 1)
        first_act(n - 1)
        sum2[...] = jnp.zeros_like(sum2)
        square2[...] = jnp.zeros_like(square2)

        def tail(t, carry):
            convolve(last, t)
            lines = pl.ds(t * join, join)
            total = acc[lines].reshape(tall, half)

            @pl.when(t == 0)
            def _():
                shift2[...] = column_sum(total) / tall

            moved = total - shift2[...]
            sum2[...] += column_sum(moved)
            square2[...] += column_sum(moved * moved)
            sec[side, lines] = moved.astype(bf16).reshape(join, height, half)

            @pl.when(t < HELD)
            def _():
                lax.fori_loop(t * per_piece, (t + 1) * per_piece, sec_start, 0)

            return carry

        lax.fori_loop(0, pieces, tail, 0)
        extra = sum2[...] / local
        stat2[b, 0:1, :] = shift2[...] + extra
        stat2[b, 1:2, :] = square2[...] - sum2[...] * extra
        stats_send(nb, b, stat2, st2_send, st2_recv)
        stats_wait(nb, b, stat2, st2_send, st2_recv)
        mean, var = combine(stat2[...], local)
        inverse = 1.0 / jnp.sqrt(var + eps)
        for i in range(mids):
            cols = slice(i * width, (i + 1) * width)
            block = side * mids + i
            scale = gb[block, 2:3, :] * inverse[:, cols]
            affine[side, 0:1, cols] = scale
            affine[side, 1:2, cols] = (shift2[:, cols] - mean[:, cols]) * scale + gb[block, 3:4, :]
        for off in range(1, n):
            affine_copy(lax.rem(z + off, n), side).start()
        lax.fori_loop(min(HELD, pieces) * per_piece, units, sec_start, 0)

    w3_load.wait()
    sum3[...] = jnp.zeros_like(sum3)
    square3[...] = jnp.zeros_like(square3)
    lag = SKEW * jnp.maximum(z - 1, n - 2 - z)

    def expand(t):
        total = None
        for f in range(2):
            value = sec[f, pl.ds(t * join, join)].reshape(tall, half).astype(f32)
            value = value * affine[f, 0:1, :] + affine[f, 1:2, :]
            term = jnp.dot(
                jnp.maximum(value, 0.0).astype(bf16), w3[f * half : (f + 1) * half, :],
                preferred_element_type=f32,
            )
            total = term if total is None else total + term
        third[t] = total

        @pl.when(t == 0)
        def _():
            shift3[...] = column_sum(total) / tall

        moved = third[t] - shift3[...]
        sum3[...] += column_sum(moved)
        square3[...] += column_sum(moved * moved)

    def relay(s, carry):
        for f in range(2):
            gone = z - 1 if f == 0 else n - 2 - z
            position = s - SKEW * gone

            @pl.when(jnp.logical_and(gone >= 0, jnp.logical_and(position >= 0, position < units)))
            def _():
                sec_copy(f, position).wait_recv()

                @pl.when(inner)
                def _():
                    sec_copy(f, position).start()

        @pl.when(s == READY)
        def _():
            for f in range(2):

                @pl.when(z != f * (n - 1))
                def _():
                    affine_copy(f * (n - 1), f).wait_recv()

        late = s - READY
        t_late = lax.div(late, 2)
        catching = jnp.logical_and(late >= 0, lax.rem(late, 2) == 0)
        catching = jnp.logical_and(catching, t_late < pieces)
        catching = jnp.logical_and(catching, per_piece * (t_late + 1) - 1 + lag <= s)
        fresh = s - (per_piece - 1) - lag
        t_fresh = lax.div(fresh, per_piece)
        arriving = jnp.logical_and(fresh >= 0, lax.rem(fresh, per_piece) == 0)
        arriving = jnp.logical_and(arriving, t_fresh < pieces)
        arriving = jnp.logical_and(arriving, READY + 2 * t_fresh < s)

        @pl.when(jnp.logical_or(catching, arriving))
        def _():
            expand(jnp.where(catching, t_late, t_fresh))

        return carry

    relay_steps = max(units + SKEW * (n - 2), READY + 2 * pieces)
    lax.fori_loop(0, relay_steps, relay, 0)

    extra = sum3[...] / local
    stat3[b, 0:1, :] = shift3[...] + extra
    stat3[b, 1:2, :] = square3[...] - sum3[...] * extra
    stats_send(nb, b, stat3, st3_send, st3_recv)

    for to in range(n):

        @pl.when(z != to)
        def _():
            w1_copy(to).wait_send()
            gb_copy(to, z).wait_send()
            for hop in range(1, hops):
                hop_copy(to, hop).wait_send()
            for hop in range(hops):
                pair_copy(to, hop).wait_send()

            @pl.when(inner)
            def _():
                gb_copy(to, to).wait_recv()

            @pl.when(at_end)
            def _():
                affine_copy(to, side).wait_send()

    @pl.when(inner)
    def _():
        w2_copy.wait_send()

    def w2_drain(slot):
        for hop in range(1, hops):
            w2hop_copy(slot, hop).wait_send()
        for hop in range(hops):
            w2pair_copy(slot, hop).wait_send()

    @pl.when(at_end)
    def _():
        each_slot(w2_drain)

    for f in range(2):

        @pl.when(z != (n - 1) * (1 - f))
        def _():
            def drain_flow(k, carry):
                flow_copy(f, k).wait_send()
                return carry

            def drain_sec(u, carry):
                sec_copy(f, u).wait_send()
                return carry

            lax.fori_loop(0, chunks, drain_flow, 0)
            lax.fori_loop(0, units, drain_sec, 0)

    stats_wait(nb, b, stat3, st3_send, st3_recv)
    mean3, var3 = combine(stat3[...], local)
    scale3 = gain3[...] / jnp.sqrt(var3 + eps)
    bias3_value = bias3[...]

    def out_copy(t):
        return pltpu.make_async_copy(outv.at[t], out_hbm.at[t], out_sem.at[t])

    def finish(t, carry):
        kept = img[pl.ds(t * join, join)].reshape(tall, out_local).astype(f32)
        value = (third[t] - mean3) * scale3 + bias3_value + kept
        outv[t] = jnp.maximum(value, 0.0).astype(bf16)
        out_copy(t).start()
        return carry

    lax.fori_loop(0, pieces, finish, 0)

    def out_drain(t, carry):
        out_copy(t).wait()
        return carry

    lax.fori_loop(0, pieces, out_drain, 0)


def body(
    images,
    reduce_weight,
    reduce_gain,
    reduce_bias,
    spatial_weight,
    spatial_gain,
    spatial_bias,
    expand_weight,
    expand_gain,
    expand_bias,
):
    imgs, side = (images.shape[0], images.shape[1])
    n, nb = lax.axis_size("chan"), lax.axis_size("batch")
    width = reduce_weight.shape[1]
    depth = images.shape[3]
    out_local = expand_weight.shape[1]
    rows, height = side, side * imgs
    chunks = n * rows
    mid = n * width
    half = mid // 2
    mids = n // 2
    join = 2 if side % 2 == 0 else 1
    pieces, tall = side // join, height * join
    dma, f32, bf16 = pltpu.SemaphoreType.DMA, jnp.float32, jnp.bfloat16
    vmem = pl.BlockSpec(memory_space=pltpu.VMEM)
    anywhere = pl.BlockSpec(memory_space=pl.ANY)
    flat = images.transpose(1, 2, 0, 3).reshape(rows, height, depth)
    out = pl.pallas_call(
        functools.partial(block_kernel, n, nb, imgs),
        out_shape=jax.ShapeDtypeStruct((pieces, tall, out_local), bf16),
        in_specs=[anywhere, anywhere, vmem, vmem, anywhere, vmem, vmem, anywhere, vmem, vmem],
        out_specs=anywhere,
        scratch_shapes=[
            pltpu.VMEM((rows, height, depth), bf16),
            pltpu.VMEM(reduce_weight.shape, bf16),
            pltpu.VMEM((n, depth, width), bf16),
            pltpu.VMEM((chunks, height, width), f32),
            pltpu.VMEM((2, rows, height, width), f32),
            pltpu.VMEM((2, chunks, height, width), bf16),
            pltpu.VMEM((n, 4, width), f32),
        ]
        + [pltpu.VMEM((n, 1, width), f32)] * 3
        + [
            pltpu.VMEM((n, nb, 2, width), f32),
            pltpu.VMEM((n, rows + 2, height, width), bf16),
            pltpu.VMEM((3, 3, mid, half), bf16),
            pltpu.VMEM((rows, height, half), f32),
            pltpu.VMEM((2, rows, height, half), bf16),
        ]
        + [pltpu.VMEM((1, half), f32)] * 3
        + [
            pltpu.VMEM((nb, 2, half), f32),
            pltpu.VMEM((2, 2, half), f32),
            pltpu.VMEM(expand_weight.shape, bf16),
            pltpu.VMEM((pieces, tall, out_local), f32),
        ]
        + [pltpu.VMEM((1, out_local), f32)] * 3
        + [pltpu.VMEM((nb, 2, out_local), f32), pltpu.VMEM((pieces, tall, out_local), bf16)]
        + [dma((4,)), dma((pieces,))]
        + [dma((n,))] * 4
        + [dma((n, nb // 2)), dma((n, nb))] * 2
        + [dma((2, chunks))] * 2
        + [dma((n, nb))] * 2
        + [dma((1,)), dma((mids,))]
        + [dma((mids, nb // 2)), dma((mids, nb))] * 2
        + [dma((2, 2 * rows))] * 2
        + [dma((nb,))] * 2
        + [dma((n,)), dma((2,))]
        + [dma((nb,))] * 2,
        compiler_params=pltpu.CompilerParams(
            collective_id=0, has_side_effects=True, vmem_limit_bytes=LIMIT
        ),
        name="block",
    )(
        flat,
        reduce_weight,
        reduce_gain[None, :],
        reduce_bias[None, :],
        spatial_weight,
        spatial_gain[None, :],
        spatial_bias[None, :],
        expand_weight,
        expand_gain[None, :],
        expand_bias[None, :],
    )
    return out.reshape(side, side, imgs, out_local).transpose(2, 0, 1, 3)


def solution(mesh):
    in_specs = (
        P("batch", None, None, "chan"),
        P(None, "chan"),
        P("chan"),
        P("chan"),
        P(None, None, None, "chan"),
        P("chan"),
        P("chan"),
        P(None, "chan"),
        P("chan"),
        P("chan"),
    )
    out_specs = P("batch", None, None, "chan")
    return jax.shard_map(body, mesh=mesh, in_specs=in_specs, out_specs=out_specs, check_vma=False)
```

```python
import functools

import jax
import jax.numpy as jnp
from jax import lax
from jax.experimental import pallas as pl
from jax.experimental.pallas import tpu as pltpu
from jax.sharding import PartitionSpec as P

eps = 0.001
MESH = pl.DeviceIdType.MESH
LIMIT = 59 * 1024 * 1024
SKEW = 3
SINK = 1
HELD = 2
READY = 11
LAG = 5


def remote(src, dst, send, recv, device):
    return pltpu.make_async_remote_copy(
        src_ref=src, dst_ref=dst, send_sem=send, recv_sem=recv,
        device_id=device, device_id_type=MESH,
    )


def greet(n, nb, z, b):
    barrier = pltpu.get_barrier_semaphore()
    for off in range(1, n):
        pl.semaphore_signal(
            barrier, inc=1, device_id={"chan": lax.rem(z + off, n)}, device_id_type=MESH
        )
    for off in range(1, nb):
        pl.semaphore_signal(
            barrier, inc=1, device_id={"batch": lax.rem(b + off, nb)}, device_id_type=MESH
        )
    pl.semaphore_wait(barrier, n + nb - 2)


def stats_send(nb, b, stats, send, recv):
    for off in range(1, nb):
        peer = lax.rem(b + off, nb)
        remote(stats.at[b], stats.at[b], send, recv, {"batch": peer}).start()


def stats_wait(nb, b, stats, send, recv):
    others = stats.at[pl.ds(0, nb - 1)]
    remote(others, others, send, recv, {"batch": lax.rem(b + 1, nb)}).wait()


def combine(stats, local):
    nb = stats.shape[0]
    means = stats[:, 0:1, :]
    mean = jnp.sum(means, axis=0) / nb
    away = means - mean[None]
    spread = jnp.sum(stats[:, 1:2, :], axis=0) + local * jnp.sum(away * away, axis=0)
    return mean, spread / (local * nb)


def column_sum(value):
    return jnp.sum(value, axis=0, keepdims=True)


def block_kernel(
    n, nb, imgs,
    img_hbm, w1_hbm, gain1, bias1, sw_hbm, gain2, bias2, w3_hbm, gain3, bias3,
    outv,
    img, w1, wown, part, whole, flow, gb, shift1, sum1, square1, stat1, act, w2, acc, sec,
    shift2, sum2, square2, stat2, affine, w3, third, shift3, sum3, square3, stat3,
    load_sem,
    gb_send, gb_recv, w1_send, w1_recv, hop_send, hop_recv, pair_send, pair_recv,
    flow_send, flow_recv, st1_send, st1_recv,
    w2_send, w2_recv, w2hop_send, w2hop_recv, w2pair_send, w2pair_recv,
    sec_send, sec_recv, st2_send, st2_recv, aff_send, aff_recv, st3_send, st3_recv,
):
    z, b = lax.axis_index("chan"), lax.axis_index("batch")
    rows, height, depth = img.shape
    width = wown.shape[2]
    half = acc.shape[2]
    pieces, tall, out_local = third.shape
    join = rows // pieces
    mids = n // 2
    hops = nb // 2
    chunks = n * rows
    strip = depth // nb
    band = n * width // nb
    local = rows * height
    unit = half // 2
    per_piece = join * 2
    units = rows * 2
    partner = b + 1 - 2 * lax.rem(b, 2)
    parity = lax.rem(b, 2)
    at_first, at_last = z == 0, z == n - 1
    at_end = jnp.logical_or(at_first, at_last)
    inner = jnp.logical_not(at_end)
    side = jnp.where(at_first, 0, 1)
    owner = jnp.where(z < mids, 0, n - 1)
    my_slot = lax.rem(z, mids)
    f32, bf16 = jnp.float32, jnp.bfloat16

    w1_load = pltpu.make_async_copy(w1_hbm, w1, load_sem.at[0])
    w1_load.start()
    img_load = pltpu.make_async_copy(img_hbm, img, load_sem.at[1])
    img_load.start()
    w3_load = pltpu.make_async_copy(w3_hbm, w3, load_sem.at[2])
    w3_load.start()

    def slot_cols(slot):
        return pl.ds(pl.multiple_of(slot * width, 128), width)

    w2_load = pltpu.make_async_copy(sw_hbm, w2.at[:, :, :, slot_cols(my_slot)], load_sem.at[3])

    @pl.when(at_end)
    def _():
        w2_load.start()

    gb[z, 0:1, :] = gain1[...]
    gb[z, 1:2, :] = bias1[...]
    gb[z, 2:3, :] = gain2[...]
    gb[z, 3:4, :] = bias2[...]
    greet(n, nb, z, b)

    def rows_of(who):
        return pl.ds(pl.multiple_of(who * strip, 16), strip)

    def w1_copy(to):
        src = w1.at[pl.ds(pl.multiple_of(to * depth + b * strip, 16), strip), :]
        return remote(src, wown.at[z, rows_of(b), :], w1_send.at[0], w1_recv.at[z], {"chan": to})

    def gb_copy(to, slot):
        return remote(gb.at[z], gb.at[slot], gb_send.at[0], gb_recv.at[0], {"chan": to})

    def band_of(who):
        return pl.ds(pl.multiple_of(who * band, 16), band)

    w2_copy = remote(
        sw_hbm.at[:, :, band_of(b), :], w2.at[:, :, band_of(b), slot_cols(my_slot)],
        w2_send.at[0], w2_recv.at[my_slot], {"chan": owner},
    )
    w1_load.wait()
    for far in range(1, n):

        @pl.when(z + far < n)
        def _():
            w1_copy(z + far).start()

        @pl.when(z - far >= 0)
        def _():
            w1_copy(z - far).start()

    for off in range(1, n):
        gb_copy(lax.rem(z + off, n), z).start()

    @pl.when(inner)
    def _():
        w2_copy.start()

    def strip_copy(g, who, send, recv, device):
        ref = wown.at[g, rows_of(who), :]
        return remote(ref, ref, send, recv, device)

    def distribute(g):
        @pl.when(z != g)
        def _():
            strip_copy(g, b, w1_send.at[0], w1_recv.at[g], {"chan": g}).wait_recv()
            for hop in range(1, hops):
                peer = lax.rem(b + 2 * hop, nb)
                strip_copy(g, b, hop_send.at[g], hop_recv.at[g], {"batch": peer}).start()
            strip_copy(g, b, pair_send.at[g], pair_recv.at[g], {"batch": partner}).start()

    def hop_all(g):
        ref = wown.at[g, pl.ds(0, (hops - 1) * strip), :]
        return remote(ref, ref, hop_send.at[g], hop_recv.at[g], {"batch": partner})

    def pair_all(g):
        ref = wown.at[g, pl.ds(0, hops * strip), :]
        return remote(ref, ref, pair_send.at[g], pair_recv.at[g], {"batch": partner})

    def forward(g):
        @pl.when(z != g)
        def _():
            hop_all(g).wait_recv()
            for hop in range(1, hops):
                peer = lax.rem(b + 2 * hop, nb)
                strip_copy(g, peer, pair_send.at[g], pair_recv.at[g], {"batch": partner}).start()

    def complete(g):
        @pl.when(z != g)
        def _():
            pair_all(g).wait_recv()

    def flow_copy(f, k):
        to = jnp.where(f == 0, lax.rem(z + 1, n), lax.rem(z + n - 1, n))
        ref = flow.at[f, k]
        return remote(ref, ref, flow_send.at[f], flow_recv.at[f, k], {"chan": to})

    def chunk_of(f, position):
        q, r = lax.div(position, rows), lax.rem(position, rows)
        return jnp.where(f == 0, q, n - 1 - q) * rows + r

    img_load.wait()

    def own_products(r, carry):
        k = z * rows + r
        value = jnp.dot(
            img[r], w1[pl.ds(pl.multiple_of(z * depth, 16), depth), :], preferred_element_type=f32
        )
        part[k] = value

        @pl.when(at_end)
        def _():
            flow[side, k] = value.astype(bf16)
            flow_copy(side, k).start()

        return carry

    def near(q):
        return jnp.where(z < mids, q, n - 1 - q)

    def far(q):
        return n - 1 - near(q)

    split = rows // 2
    lax.fori_loop(0, split, own_products, 0)
    distribute(near(0))
    lax.fori_loop(split, rows, own_products, 0)
    distribute(far(0))
    for q in range(1, mids):
        distribute(near(q))
        distribute(far(q))
    act[:, 0] = jnp.zeros_like(act[:, 0])
    act[:, rows + 1] = jnp.zeros_like(act[:, 0])
    acc[...] = jnp.zeros_like(acc)
    forward(near(0))

    def band_copy(slot, who, send, recv, device):
        ref = w2.at[:, :, band_of(who), slot_cols(slot)]
        return remote(ref, ref, send, recv, device)

    def each_slot(work):
        for slot in range(mids):

            @pl.when(slot != my_slot)
            def _():
                work(slot)

    def w2_distribute(slot):
        band_copy(slot, b, w2_send.at[0], w2_recv.at[slot], {"chan": z}).wait_recv()
        for hop in range(1, hops):
            peer = lax.rem(b + 2 * hop, nb)
            band_copy(slot, b, w2hop_send.at[slot], w2hop_recv.at[slot], {"batch": peer}).start()
        band_copy(slot, b, w2pair_send.at[slot], w2pair_recv.at[slot], {"batch": partner}).start()

    def w2hop_all(slot):
        ref = w2.at[:, :, pl.ds(0, (hops - 1) * band), slot_cols(slot)]
        return remote(ref, ref, w2hop_send.at[slot], w2hop_recv.at[slot], {"batch": partner})

    def w2pair_all(slot):
        ref = w2.at[:, :, pl.ds(0, hops * band), slot_cols(slot)]
        return remote(ref, ref, w2pair_send.at[slot], w2pair_recv.at[slot], {"batch": partner})

    def w2_forward(slot):
        w2hop_all(slot).wait_recv()
        for hop in range(1, hops):
            peer = lax.rem(b + 2 * hop, nb)
            band_copy(
                slot, peer, w2pair_send.at[slot], w2pair_recv.at[slot], {"batch": partner}
            ).start()

    def w2_complete(slot):
        w2pair_all(slot).wait_recv()

    def gb_all():
        ref = gb.at[pl.ds(0, n - 1)]
        return remote(ref, ref, gb_send.at[0], gb_recv.at[0], {"chan": lax.rem(z + 1, n)})

    def end_group(q):
        return jnp.where(at_first, n - 1 - q, q)

    def finalize(position):
        f = 1 - side
        k = chunk_of(f, position)
        g, r = lax.div(k, rows), lax.rem(k, rows)
        flow_copy(f, k).wait_recv()
        value = part[k] + flow[f, k].astype(f32)
        whole[lax.rem(lax.div(position, rows), 2), r] = value

        @pl.when(r == 0)
        def _():
            shift1[g] = column_sum(value) / height
            sum1[g] = jnp.zeros_like(sum1[g])
            square1[g] = jnp.zeros_like(square1[g])

        moved = value - shift1[g]
        sum1[g] += column_sum(moved)
        square1[g] += column_sum(moved * moved)

    def first_stats(g):
        extra = sum1[g] / local
        stat1[g, b, 0:1, :] = shift1[g] + extra
        stat1[g, b, 1:2, :] = square1[g] - sum1[g] * extra
        stats_send(nb, b, stat1.at[g], st1_send.at[g], st1_recv.at[g])

    def first_affine(q):
        g = end_group(q)
        stats_wait(nb, b, stat1.at[g], st1_send.at[g], st1_recv.at[g])
        mean, var = combine(stat1[g], local)
        scale = gb[g, 0:1, :] / jnp.sqrt(var + eps)
        bias = gb[g, 1:2, :]

        def line(r):
            value = (whole[lax.rem(q, 2), r] - mean) * scale + bias
            act[g, r + 1] = jnp.maximum(value, 0.0).astype(bf16)

        return line

    def convolve(g, t):
        for col_tap in range(3):
            total = None
            for row_tap in range(3):
                window = act[g, pl.ds(t * join + row_tap, join)].reshape(tall, width)
                weight = w2[row_tap, col_tap, pl.ds(pl.multiple_of(g * width, 128), width), :]
                term = jnp.dot(window, weight, preferred_element_type=f32)
                total = term if total is None else total + term
            total = total.reshape(join, height, half)
            lines = pl.ds(t * join, join)
            if col_tap == 0:
                acc[lines, imgs:, :] += total[:, : height - imgs]
            elif col_tap == 1:
                acc[lines] += total
            else:
                acc[lines, : height - imgs, :] += total[:, imgs:]

    reach = SKEW * (n - 1) + SINK

    pace = (rows + 1) // 2
    packed = (n - 1) * (rows - pieces) + 1
    lag1 = min(LAG, SKEW * mids)

    def make(g, r):
        @pl.when(jnp.logical_and(z != g, r < rows))
        def _():
            part[g * rows + r] = jnp.dot(img[r], wown[g], preferred_element_type=f32)

    def produce(tick, pick):
        @pl.when(jnp.logical_and(tick >= 0, tick < rows))
        def _():
            g = pick(0)

            @pl.when(tick == 0)
            def _():
                complete(g)

            make(g, tick)

        late = tick - rows

        @pl.when(jnp.logical_and(late >= 0, late < (mids - 1) * pace))
        def _():
            g, i = pick(1 + lax.div(late, pace)), lax.rem(late, pace)

            @pl.when(i == 0)
            def _():
                complete(g)

            make(g, 2 * i)
            make(g, 2 * i + 1)

    def step(s, carry):
        @pl.when(s == 2)
        def _():
            forward(far(0))

        for q in range(1, mids):

            @pl.when(s == 6 + (q - 1) * pace)
            def _():
                forward(near(q))
                forward(far(q))

        produce(s, near)
        produce(s - lag1, far)

        for extra in range(2):
            position = rows + 2 * (s - rows) + extra
            k = chunk_of(side, position)

            @pl.when(jnp.logical_and(at_end, jnp.logical_and(s >= rows, position < chunks)))
            def _():
                flow[side, k] = part[k].astype(bf16)
                flow_copy(side, k).start()

        for f in range(2):
            position = s - SKEW * (z if f == 0 else n - 1 - z)
            k = chunk_of(f, position)

            @pl.when(jnp.logical_and(inner, jnp.logical_and(position >= 0, position < chunks)))
            def _():
                flow_copy(f, k).wait_recv()
                flow[f, k] = (part[k] + flow[f, k].astype(f32)).astype(bf16)
                flow_copy(f, k).start()

        @pl.when(at_end)
        def _():
            position = s - reach
            after = position - (rows - 1)

            @pl.when(position == 0)
            def _():
                each_slot(w2_distribute)

            @pl.when(after == packed - 6)
            def _():
                each_slot(w2_forward)

            @pl.when(after == packed)
            def _():
                w2_load.wait()
                each_slot(w2_complete)

            @pl.when(position >= 0)
            def _():
                finalize(position)

            @pl.when(after >= 0)
            def _():
                q, v = lax.div(after, rows), lax.rem(after, rows)

                @pl.when(v == 0)
                def _():
                    first_stats(end_group(q))

                @pl.when(v == 4)
                def _():
                    @pl.when(q == 0)
                    def _():
                        gb_all().wait_recv()

                    line = first_affine(q)

                    def each_line(r, carry):
                        line(r)
                        return carry

                    lax.fori_loop(0, rows, each_line, 0)

            item = after - packed

            @pl.when(item >= 0)
            def _():
                convolve(end_group(lax.div(item, pieces)), lax.rem(item, pieces))

        return carry

    lax.fori_loop(0, chunks + reach, step, 0)

    def sec_copy(f, u):
        to = jnp.where(f == 0, lax.rem(z + 1, n), lax.rem(z + n - 1, n))
        line, part_of = lax.div(u, 2), lax.rem(u, 2)
        ref = sec.at[f, line, :, pl.ds(pl.multiple_of(part_of * unit, 128), unit)]
        return remote(ref, ref, sec_send.at[f], sec_recv.at[f, u], {"chan": to})

    def sec_start(u, carry):
        sec_copy(side, u).start()
        return carry

    def affine_copy(to, f):
        return remote(affine.at[f], affine.at[f], aff_send.at[to], aff_recv.at[f], {"chan": to})

    @pl.when(at_end)
    def _():
        last = end_group(n - 1)
        line = first_affine(n - 1)
        line(0)
        sum2[...] = jnp.zeros_like(sum2)
        square2[...] = jnp.zeros_like(square2)

        def tail(t, carry):
            for ahead in range(1, join + 1):

                @pl.when(t * join + ahead < rows)
                def _():
                    line(t * join + ahead)

            convolve(last, t)
            lines = pl.ds(t * join, join)
            total = acc[lines].reshape(tall, half)

            @pl.when(t == 0)
            def _():
                shift2[...] = column_sum(total) / tall

            moved = total - shift2[...]
            sum2[...] += column_sum(moved)
            square2[...] += column_sum(moved * moved)
            sec[side, lines] = moved.astype(bf16).reshape(join, height, half)

            @pl.when(t < HELD)
            def _():
                lax.fori_loop(t * per_piece, (t + 1) * per_piece, sec_start, 0)

            return carry

        lax.fori_loop(0, pieces, tail, 0)
        extra = sum2[...] / local
        stat2[b, 0:1, :] = shift2[...] + extra
        stat2[b, 1:2, :] = square2[...] - sum2[...] * extra
        stats_send(nb, b, stat2, st2_send.at[0], st2_recv.at[0])
        stats_wait(nb, b, stat2, st2_send.at[0], st2_recv.at[0])
        mean, var = combine(stat2[...], local)
        inverse = 1.0 / jnp.sqrt(var + eps)
        for i in range(mids):
            cols = slice(i * width, (i + 1) * width)
            block = side * mids + i
            scale = gb[block, 2:3, :] * inverse[:, cols]
            affine[side, 0:1, cols] = scale
            affine[side, 1:2, cols] = (shift2[:, cols] - mean[:, cols]) * scale + gb[block, 3:4, :]
        for off in range(1, n):
            affine_copy(lax.rem(z + off, n), side).start()
        lax.fori_loop(min(HELD, pieces) * per_piece, units, sec_start, 0)

    w3_load.wait()
    sum3[...] = jnp.zeros_like(sum3)
    square3[...] = jnp.zeros_like(square3)
    lag = SKEW * jnp.maximum(z - 1, n - 2 - z)

    def expand(t):
        total = None
        for f in range(2):
            value = sec[f, pl.ds(t * join, join)].reshape(tall, half).astype(f32)
            value = value * affine[f, 0:1, :] + affine[f, 1:2, :]
            term = jnp.dot(
                jnp.maximum(value, 0.0).astype(bf16), w3[f * half : (f + 1) * half, :],
                preferred_element_type=f32,
            )
            total = term if total is None else total + term
        third[t] = total

        @pl.when(t == 0)
        def _():
            shift3[...] = column_sum(total) / tall

        moved = third[t] - shift3[...]
        sum3[...] += column_sum(moved)
        square3[...] += column_sum(moved * moved)

    def relay(s, carry):
        for f in range(2):
            gone = z - 1 if f == 0 else n - 2 - z
            position = s - SKEW * gone

            @pl.when(jnp.logical_and(gone >= 0, jnp.logical_and(position >= 0, position < units)))
            def _():
                sec_copy(f, position).wait_recv()

                @pl.when(inner)
                def _():
                    sec_copy(f, position).start()

        @pl.when(s == READY)
        def _():
            for f in range(2):

                @pl.when(z != f * (n - 1))
                def _():
                    affine_copy(f * (n - 1), f).wait_recv()

        late = s - READY
        t_late = lax.div(late, 2)
        catching = jnp.logical_and(late >= 0, lax.rem(late, 2) == 0)
        catching = jnp.logical_and(catching, t_late < pieces)
        catching = jnp.logical_and(catching, per_piece * (t_late + 1) - 1 + lag <= s)
        fresh = s - (per_piece - 1) - lag
        t_fresh = lax.div(fresh, per_piece)
        arriving = jnp.logical_and(fresh >= 0, lax.rem(fresh, per_piece) == 0)
        arriving = jnp.logical_and(arriving, t_fresh < pieces)
        arriving = jnp.logical_and(arriving, READY + 2 * t_fresh < s)

        @pl.when(jnp.logical_or(catching, arriving))
        def _():
            expand(jnp.where(catching, t_late, t_fresh))

        return carry

    relay_steps = max(units + SKEW * (n - 2), READY + 2 * pieces)
    lax.fori_loop(0, relay_steps, relay, 0)

    extra = sum3[...] / local
    stat3[b, 0:1, :] = shift3[...] + extra
    stat3[b, 1:2, :] = square3[...] - sum3[...] * extra
    stats_send(nb, b, stat3, st3_send.at[0], st3_recv.at[0])

    sent = wown.at[0, pl.ds(0, (n - 1) * strip), :]
    remote(sent, sent, w1_send.at[0], w1_recv.at[0], {"batch": partner}).wait_send()
    gb_all().wait_send()
    for to in range(n):

        @pl.when(z != to)
        def _():
            hop_all(to).wait_send()
            pair_all(to).wait_send()

            @pl.when(at_end)
            def _():
                affine_copy(to, side).wait_send()

    @pl.when(inner)
    def _():
        gb_all().wait_recv()
        w2_copy.wait_send()

    def w2_drain(slot):
        w2hop_all(slot).wait_send()
        w2pair_all(slot).wait_send()

    @pl.when(at_end)
    def _():
        each_slot(w2_drain)

    for f in range(2):

        @pl.when(z != (n - 1) * (1 - f))
        def _():
            right = {"chan": lax.rem(z + 1, n)}
            remote(flow.at[f], flow.at[f], flow_send.at[f], flow_recv.at[f, 0], right).wait_send()
            remote(sec.at[f], sec.at[f], sec_send.at[f], sec_recv.at[f, 0], right).wait_send()

    stats_wait(nb, b, stat3, st3_send.at[0], st3_recv.at[0])
    mean3, var3 = combine(stat3[...], local)
    scale3 = gain3[...] / jnp.sqrt(var3 + eps)
    bias3_value = bias3[...]

    def finish(t, carry):
        kept = img[pl.ds(t * join, join)].reshape(tall, out_local).astype(f32)
        value = (third[t] - mean3) * scale3 + bias3_value + kept
        outv[t] = jnp.maximum(value, 0.0).astype(bf16)
        return carry

    lax.fori_loop(0, pieces, finish, 0)


def body(
    images,
    reduce_weight,
    reduce_gain,
    reduce_bias,
    spatial_weight,
    spatial_gain,
    spatial_bias,
    expand_weight,
    expand_gain,
    expand_bias,
):
    imgs, side = (images.shape[0], images.shape[1])
    n, nb = lax.axis_size("chan"), lax.axis_size("batch")
    width = reduce_weight.shape[1]
    depth = images.shape[3]
    out_local = expand_weight.shape[1]
    rows, height = side, side * imgs
    chunks = n * rows
    mid = n * width
    half = mid // 2
    mids = n // 2
    join = 2 if side % 2 == 0 else 1
    pieces, tall = side // join, height * join
    dma, f32, bf16 = pltpu.SemaphoreType.DMA, jnp.float32, jnp.bfloat16
    vmem = pl.BlockSpec(memory_space=pltpu.VMEM)
    anywhere = pl.BlockSpec(memory_space=pl.ANY)
    flat = images.transpose(1, 2, 0, 3).reshape(rows, height, depth)
    out = pl.pallas_call(
        functools.partial(block_kernel, n, nb, imgs),
        out_shape=pltpu.VMEM((pieces, tall, out_local), bf16),
        in_specs=[anywhere, anywhere, vmem, vmem, anywhere, vmem, vmem, anywhere, vmem, vmem],
        out_specs=vmem,
        scratch_shapes=[
            pltpu.VMEM((rows, height, depth), bf16),
            pltpu.VMEM(reduce_weight.shape, bf16),
            pltpu.VMEM((n, depth, width), bf16),
            pltpu.VMEM((chunks, height, width), f32),
            pltpu.VMEM((2, rows, height, width), f32),
            pltpu.VMEM((2, chunks, height, width), bf16),
            pltpu.VMEM((n, 4, width), f32),
        ]
        + [pltpu.VMEM((n, 1, width), f32)] * 3
        + [
            pltpu.VMEM((n, nb, 2, width), f32),
            pltpu.VMEM((n, rows + 2, height, width), bf16),
            pltpu.VMEM((3, 3, mid, half), bf16),
            pltpu.VMEM((rows, height, half), f32),
            pltpu.VMEM((2, rows, height, half), bf16),
        ]
        + [pltpu.VMEM((1, half), f32)] * 3
        + [
            pltpu.VMEM((nb, 2, half), f32),
            pltpu.VMEM((2, 2, half), f32),
            pltpu.VMEM(expand_weight.shape, bf16),
            pltpu.VMEM((pieces, tall, out_local), f32),
        ]
        + [pltpu.VMEM((1, out_local), f32)] * 3
        + [pltpu.VMEM((nb, 2, out_local), f32)]
        + [dma((4,))]
        + [dma((1,))] * 2
        + [dma((1,)), dma((n,))]
        + [dma((n,))] * 4
        + [dma((2,)), dma((2, chunks))]
        + [dma((n,))] * 2
        + [dma((1,)), dma((mids,))]
        + [dma((mids,))] * 4
        + [dma((2,)), dma((2, 2 * rows))]
        + [dma((1,))] * 2
        + [dma((n,)), dma((2,))]
        + [dma((1,))] * 2,
        compiler_params=pltpu.CompilerParams(
            collective_id=0, has_side_effects=True, vmem_limit_bytes=LIMIT
        ),
        name="block",
    )(
        flat,
        reduce_weight,
        reduce_gain[None, :],
        reduce_bias[None, :],
        spatial_weight,
        spatial_gain[None, :],
        spatial_bias[None, :],
        expand_weight,
        expand_gain[None, :],
        expand_bias[None, :],
    )
    return out.reshape(side, side, imgs, out_local).transpose(2, 0, 1, 3)


def solution(mesh):
    in_specs = (
        P("batch", None, None, "chan"),
        P(None, "chan"),
        P("chan"),
        P("chan"),
        P(None, None, None, "chan"),
        P("chan"),
        P("chan"),
        P(None, "chan"),
        P("chan"),
        P("chan"),
    )
    out_specs = P("batch", None, None, "chan")
    return jax.shard_map(body, mesh=mesh, in_specs=in_specs, out_specs=out_specs, check_vma=False)
```

```python
import functools

import jax
import jax.numpy as jnp
from jax import lax
from jax.experimental import pallas as pl
from jax.experimental.pallas import tpu as pltpu
from jax.sharding import PartitionSpec as P

eps = 0.001
MESH = pl.DeviceIdType.MESH
LIMIT = 59 * 1024 * 1024
SKEW = 3
EXTRA = 1
HELD = 4
SETTLE = 8
OUTER_GIVE = (0, 3, 6)
INNER_SHARE = (0, 18, 22)
OUTER_SHARE = (0, 2, 4)
INNER_MORE = (1, 26, 33)
OUTER_MORE = (21, 25, 33)
MORE_CHAIN = (1, 3, 5)


def remote(src, dst, send, recv, device):
    return pltpu.make_async_remote_copy(
        src_ref=src, dst_ref=dst, send_sem=send, recv_sem=recv,
        device_id=device, device_id_type=MESH,
    )


def greet(n, nb, z, b):
    barrier = pltpu.get_barrier_semaphore()
    for off in range(1, n):
        pl.semaphore_signal(
            barrier, inc=1, device_id={"chan": lax.rem(z + off, n)}, device_id_type=MESH
        )
    for off in range(1, nb):
        pl.semaphore_signal(
            barrier, inc=1, device_id={"batch": lax.rem(b + off, nb)}, device_id_type=MESH
        )
    pl.semaphore_wait(barrier, n + nb - 2)


def stats_send(nb, b, stats, send, recv):
    for off in range(1, nb):
        peer = lax.rem(b + off, nb)
        remote(stats.at[b], stats.at[b], send, recv, {"batch": peer}).start()


def stats_wait(nb, b, stats, send, recv):
    others = stats.at[pl.ds(0, nb - 1)]
    remote(others, others, send, recv, {"batch": lax.rem(b + 1, nb)}).wait()


def combine(stats, local):
    nb = stats.shape[0]
    means = stats[..., 0:1, :]
    mean = jnp.sum(means, axis=0) / nb
    away = means - mean[None]
    spread = jnp.sum(stats[..., 1:2, :], axis=0) + local * jnp.sum(away * away, axis=0)
    return mean, spread / (local * nb)


def column_sum(value):
    return jnp.sum(value, axis=0, keepdims=True)


def block_kernel(
    n, nb, imgs,
    img_hbm, w1_hbm, gain1, bias1, sw_hbm, gain2, bias2, w3_hbm, gain3, bias3,
    outv,
    img, w1, wown, part, whole, flow, gb, shift1, sum1, square1, stat1, act, w2, acc, sec,
    shift2, sum2, square2, stat_out, stat_keep, affine, w3, third, shift3, sum3, square3, stat3,
    load_sem,
    gb_send, gb_recv, w1_send, w1_recv, hop_send, hop_recv, pair_send, pair_recv,
    flow_send, flow_recv, st1_send, st1_recv,
    w2_send, w2_recv, w2hop_send, w2hop_recv, w2pair_send, w2pair_recv,
    sec_send, sec_recv, st2_send, st2_recv, st4_send, st4_recv, aff_send, aff_recv, st3_send, st3_recv,
):
    z, b = lax.axis_index("chan"), lax.axis_index("batch")
    rows, height, depth = img.shape
    width = wown.shape[2]
    slots = w2.shape[0]
    pieces, tall, out_local = third.shape
    join = rows // pieces
    mids = n // 2
    more = slots - mids
    lacking = mids - more
    hops = nb // 2
    chunks = n * rows
    strip = depth // nb
    band = n * width // nb
    local = rows * height
    per_piece = lacking * join
    units = lacking * rows
    partner = b + 1 - 2 * lax.rem(b, 2)
    at_first, at_last = z == 0, z == n - 1
    at_end = jnp.logical_or(at_first, at_last)
    inner = jnp.logical_not(at_end)
    side = jnp.where(z < mids, 0, 1)
    gone = jnp.where(z < mids, mids - 1 - z, z - mids)
    first_block = side * (mids - more)
    my_slot = z - first_block
    half_slot = side * more
    more_slot = (1 - side) * mids
    out_slot = side * (slots - lacking)
    keep_slot = (1 - side) * lacking
    late_flow = 1 - side
    late_skew = SKEW * jnp.maximum(z, n - 1 - z)
    early_skew = SKEW * jnp.minimum(z, n - 1 - z)
    f32, bf16 = jnp.float32, jnp.bfloat16

    w1_load = pltpu.make_async_copy(w1_hbm, w1, load_sem.at[0])
    w1_load.start()
    img_load = pltpu.make_async_copy(img_hbm, img, load_sem.at[1])
    img_load.start()
    w3_load = pltpu.make_async_copy(w3_hbm, w3, load_sem.at[2])
    w3_load.start()

    w2_load = pltpu.make_async_copy(sw_hbm, w2.at[my_slot], load_sem.at[3])
    w2_load.start()
    gb[z, 0:1, :] = gain1[...]
    gb[z, 1:2, :] = bias1[...]
    gb[z, 2:3, :] = gain2[...]
    gb[z, 3:4, :] = bias2[...]
    greet(n, nb, z, b)

    def rows_of(who):
        return pl.ds(pl.multiple_of(who * strip, 16), strip)

    def w1_copy(to):
        src = w1.at[pl.ds(pl.multiple_of(to * depth + b * strip, 16), strip), :]
        return remote(src, wown.at[z, rows_of(b), :], w1_send.at[0], w1_recv.at[z], {"chan": to})

    def gb_copy(to, slot):
        return remote(gb.at[z], gb.at[slot], gb_send.at[0], gb_recv.at[0], {"chan": to})

    def band_of(who):
        return pl.ds(pl.multiple_of(who * band, 16), band)

    w1_load.wait()
    for far in range(n - 1, 0, -1):

        @pl.when(z + far < n)
        def _():
            w1_copy(z + far).start()

        @pl.when(z - far >= 0)
        def _():
            w1_copy(z - far).start()

    for off in range(1, n):
        gb_copy(lax.rem(z + off, n), z).start()

    def band_ref(slot, row_tap, who):
        return w2.at[slot, row_tap, :, band_of(who), :]

    def w2_give(row_tap, to, slot, kind):
        src = sw_hbm.at[row_tap, :, band_of(b), :]
        return remote(
            src, band_ref(slot, row_tap, b), w2_send.at[kind], w2_recv.at[slot, row_tap],
            {"chan": to},
        )

    def half_give(row_tap):
        for off in range(1, mids):
            to = side * mids + lax.rem(z - side * mids + off, mids)
            w2_give(row_tap, to, my_slot, 0).start()

    for row_tap in range(3):
        if more:

            @pl.when(gone == 0)
            def _():
                to = jnp.where(side == 0, mids, mids - 1)
                w2_give(row_tap, to, jnp.where(side == 0, 0, mids), 1).start()

        if row_tap == 0:
            half_give(row_tap)
        else:

            @pl.when(inner)
            def _():
                half_give(row_tap)

    def strip_copy(g, who, send, recv, device):
        ref = wown.at[g, rows_of(who), :]
        return remote(ref, ref, send, recv, device)

    def distribute(g):
        @pl.when(z != g)
        def _():
            strip_copy(g, b, w1_send.at[0], w1_recv.at[g], {"chan": g}).wait_recv()
            for hop in range(1, hops):
                peer = lax.rem(b + 2 * hop, nb)
                strip_copy(g, b, hop_send.at[g], hop_recv.at[g], {"batch": peer}).start()
            strip_copy(g, b, pair_send.at[g], pair_recv.at[g], {"batch": partner}).start()

    def hop_all(g):
        ref = wown.at[g, pl.ds(0, (hops - 1) * strip), :]
        return remote(ref, ref, hop_send.at[g], hop_recv.at[g], {"batch": partner})

    def pair_all(g):
        ref = wown.at[g, pl.ds(0, hops * strip), :]
        return remote(ref, ref, pair_send.at[g], pair_recv.at[g], {"batch": partner})

    def forward(g):
        @pl.when(z != g)
        def _():
            hop_all(g).wait_recv()
            for hop in range(1, hops):
                peer = lax.rem(b + 2 * hop, nb)
                strip_copy(g, peer, pair_send.at[g], pair_recv.at[g], {"batch": partner}).start()

    def complete(g):
        @pl.when(z != g)
        def _():
            pair_all(g).wait_recv()

    def flow_copy(f, k):
        to = jnp.where(f == 0, lax.rem(z + 1, n), lax.rem(z + n - 1, n))
        ref = flow.at[f, k]
        return remote(ref, ref, flow_send.at[f], flow_recv.at[f, k], {"chan": to})

    img_load.wait()

    def own_products(r, carry):
        k = z * rows + r
        value = jnp.dot(
            img[r], w1[pl.ds(pl.multiple_of(z * depth, 16), depth), :], preferred_element_type=f32
        )
        part[k] = value

        @pl.when(at_first)
        def _():
            flow[0, k] = value.astype(bf16)
            flow_copy(0, k).start()

        return carry

    lax.fori_loop(0, rows, own_products, 0)
    for g in range(n):
        distribute(g)
    act[:, 0] = jnp.zeros_like(act[:, 0])
    act[:, rows + 1] = jnp.zeros_like(act[:, 0])

    def clear(r, carry):
        acc[:, r] = jnp.zeros_like(acc[:, r])
        return carry

    lax.fori_loop(0, rows, clear, 0)
    forward(0)

    def w2_share(slot, row_tap):
        ref = band_ref(slot, row_tap, b)
        for hop in range(1, hops):
            peer = lax.rem(b + 2 * hop, nb)
            remote(ref, ref, w2hop_send.at[slot], w2hop_recv.at[slot], {"batch": peer}).start()
        remote(ref, ref, w2pair_send.at[slot], w2pair_recv.at[slot], {"batch": partner}).start()

    def w2_arrive(slot, row_tap):
        ref = band_ref(slot, row_tap, b)
        remote(ref, ref, w2_send.at[0], w2_recv.at[slot, row_tap], {"chan": z}).wait_recv()

    def half_share(row_tap):
        def work(slot):
            w2_arrive(slot, row_tap)
            w2_share(slot, row_tap)

        half_slots(work)

    def w2_chain(row_tap):
        ref = band_ref(more_slot, row_tap, b)
        to = jnp.where(side == 0, lax.rem(z + n - 1, n), lax.rem(z + 1, n))
        return remote(ref, ref, w2_send.at[2], w2_recv.at[more_slot, row_tap], {"chan": to})

    def w2hop_all(slot):
        ref = w2.at[slot, :, :, pl.ds(0, (hops - 1) * band), :]
        return remote(ref, ref, w2hop_send.at[slot], w2hop_recv.at[slot], {"batch": partner})

    def w2pair_all(slot):
        ref = w2.at[slot, :, :, pl.ds(0, hops * band), :]
        return remote(ref, ref, w2pair_send.at[slot], w2pair_recv.at[slot], {"batch": partner})

    def w2_forward(slot):
        w2hop_all(slot).wait_recv()
        for row_tap in range(3):
            for hop in range(1, hops):
                ref = band_ref(slot, row_tap, lax.rem(b + 2 * hop, nb))
                remote(
                    ref, ref, w2pair_send.at[slot], w2pair_recv.at[slot], {"batch": partner}
                ).start()

    def half_slots(work):
        for off in range(1, mids):
            work(half_slot + lax.rem(my_slot - half_slot + off, mids))

    def gb_all():
        ref = gb.at[pl.ds(0, n - 1)]
        return remote(ref, ref, gb_send.at[0], gb_recv.at[0], {"chan": lax.rem(z + 1, n)})

    def finalize(k, value):
        g, r = lax.div(k, rows), lax.rem(k, rows)
        whole[lax.rem(g, 2), r] = value

        @pl.when(r == 0)
        def _():
            shift1[g] = column_sum(value) / height
            sum1[g] = jnp.zeros_like(sum1[g])
            square1[g] = jnp.zeros_like(square1[g])

        moved = value - shift1[g]
        sum1[g] += column_sum(moved)
        square1[g] += column_sum(moved * moved)

    def first_stats(g):
        extra = sum1[g] / local
        stat1[g, b, 0:1, :] = shift1[g] + extra
        stat1[g, b, 1:2, :] = square1[g] - sum1[g] * extra
        stats_send(nb, b, stat1.at[g], st1_send.at[g], st1_recv.at[g])

    def first_affine(g):
        stats_wait(nb, b, stat1.at[g], st1_send.at[g], st1_recv.at[g])
        mean, var = combine(stat1[g], local)
        scale = gb[g, 0:1, :] / jnp.sqrt(var + eps)
        bias = gb[g, 1:2, :]

        def line(r):
            value = (whole[lax.rem(g, 2), r] - mean) * scale + bias
            act[g, r + 1] = jnp.maximum(value, 0.0).astype(bf16)

        return line

    def convolve(g, t, slot):
        lines = pl.ds(t * join, join)
        for col_tap in range(3):
            total = None
            for row_tap in range(3):
                window = act[g, pl.ds(t * join + row_tap, join)].reshape(tall, width)
                weight = w2[slot, row_tap, col_tap, pl.ds(pl.multiple_of(g * width, 128), width), :]
                term = jnp.dot(window, weight, preferred_element_type=f32)
                total = term if total is None else total + term
            total = total.reshape(join, height, width)
            if col_tap == 0:
                acc[slot, lines, imgs:, :] += total[:, : height - imgs]
            elif col_tap == 1:
                acc[slot, lines] += total
            else:
                acc[slot, lines, : height - imgs, :] += total[:, imgs:]

    last = n - 1
    all_begin = last * rows - pieces + 1
    more_begin = all_begin - pieces
    half_begin = more_begin - (last - 1) * pieces

    def step(s, carry):
        for g in range(1, n):

            @pl.when(s == (g - 1) * (rows // 2) + 2)
            def _():
                forward(g)

        for row_tap in range(3):
            if row_tap:

                @pl.when(jnp.logical_and(at_end, s == OUTER_GIVE[row_tap]))
                def _():
                    half_give(row_tap)

            if more:

                @pl.when(s == jnp.where(at_end, OUTER_MORE[row_tap], MORE_CHAIN[row_tap]))
                def _():
                    w2_arrive(more_slot, row_tap)

                    @pl.when(inner)
                    def _():
                        w2_chain(row_tap).start()

                @pl.when(s == jnp.where(at_end, OUTER_MORE[row_tap], INNER_MORE[row_tap]))
                def _():
                    w2_share(more_slot, row_tap)

            @pl.when(s == jnp.where(at_end, OUTER_SHARE[row_tap], INNER_SHARE[row_tap]))
            def _():
                half_share(row_tap)

        for extra in range(2):
            k = 2 * s + extra
            g, r = lax.div(k, rows), lax.rem(k, rows)

            @pl.when(k < chunks)
            def _():
                @pl.when(r == 0)
                def _():
                    complete(g)

                @pl.when(z != g)
                def _():
                    part[k] = jnp.dot(img[r], wown[g], preferred_element_type=f32)

                @pl.when(jnp.logical_and(at_end, jnp.logical_or(at_last, k >= rows)))
                def _():
                    flow[side, k] = part[k].astype(bf16)
                    flow_copy(side, k).start()

        early = s - early_skew

        @pl.when(jnp.logical_and(inner, jnp.logical_and(early >= 0, early < chunks)))
        def _():
            flow_copy(side, early).wait_recv()
            flow[side, early] = (part[early] + flow[side, early].astype(f32)).astype(bf16)
            flow_copy(side, early).start()

        late = s - late_skew
        after = late - (rows - 1)

        @pl.when(late >= 0)
        def _():
            flow_copy(late_flow, late).wait_recv()
            coming = flow[late_flow, late].astype(f32)

            @pl.when(inner)
            def _():
                flow[late_flow, late] = (part[late] + coming).astype(bf16)
                flow_copy(late_flow, late).start()
                finalize(late, flow[side, late].astype(f32) + coming)

            @pl.when(at_end)
            def _():
                finalize(late, part[late] + coming)

        @pl.when(after == half_begin - 6)
        def _():
            half_slots(w2_forward)

        @pl.when(after == half_begin - 1)
        def _():
            w2_load.wait()
            half_slots(lambda slot: w2pair_all(slot).wait_recv())

        if more:

            @pl.when(after == more_begin - 5)
            def _():
                w2_forward(more_slot)

            @pl.when(after == more_begin - 1)
            def _():
                w2pair_all(more_slot).wait_recv()

        @pl.when(after >= 0)
        def _():
            g, v = lax.div(after, rows), lax.rem(after, rows)

            @pl.when(v == 0)
            def _():
                first_stats(g)

            @pl.when(v == SETTLE)
            def _():
                @pl.when(g == 0)
                def _():
                    gb_all().wait_recv()

                line = first_affine(g)

                def each_line(r, carry):
                    line(r)
                    return carry

                lax.fori_loop(0, rows, each_line, 0)

        item = after - half_begin

        @pl.when(jnp.logical_and(item >= 0, item < (last - 1) * pieces))
        def _():
            for i in range(mids):
                convolve(lax.div(item, pieces), lax.rem(item, pieces), half_slot + i)

        if more:

            @pl.when(jnp.logical_and(after >= more_begin, after < more_begin + pieces))
            def _():
                for g in range(last - 1):
                    convolve(g, after - more_begin, more_slot)

        @pl.when(after >= all_begin)
        def _():
            for slot in range(slots):
                convolve(last - 1, after - all_begin, slot)

        return carry

    lax.fori_loop(0, chunks + late_skew, step, 0)

    def sec_copy(f, u):
        to = jnp.where(f == 0, lax.rem(z + 1, n), lax.rem(z + n - 1, n))
        t, rest = lax.div(u, per_piece), lax.rem(u, per_piece)
        block = lax.div(rest, join) + f * (mids + more)
        ref = sec.at[block, t * join + lax.rem(rest, join)]
        kind = jnp.where(f == side, 0, 1)
        return remote(ref, ref, sec_send.at[kind], sec_recv.at[u], {"chan": to})

    def sec_start(u, carry):
        sec_copy(side, u).start()
        return carry

    far_block = (1 - side) * (mids + more)
    near_block = side * (mids + more)

    def affine_copy(to, block):
        ref = affine.at[pl.ds(block, lacking)]
        return remote(ref, ref, aff_send.at[to], aff_recv.at[0], {"chan": to})

    def relay(tick):
        u = tick - SKEW * gone

        @pl.when(jnp.logical_and(u >= 0, u < units))
        def _():
            sec_copy(1 - side, u).wait_recv()

            @pl.when(inner)
            def _():
                sec_copy(1 - side, u).start()

    line = first_affine(last)
    line(0)
    sum2[...] = jnp.zeros_like(sum2)
    square2[...] = jnp.zeros_like(square2)

    def measure(t, slot):
        convolve(last, t, slot)
        lines = pl.ds(t * join, join)
        total = acc[slot, lines].reshape(tall, width)

        @pl.when(t == 0)
        def _():
            shift2[slot] = column_sum(total) / tall

        moved = total - shift2[slot]
        sum2[slot] += column_sum(moved)
        square2[slot] += column_sum(moved * moved)
        sec[first_block + slot, lines] = moved.astype(bf16).reshape(join, height, width)

    def record(stats, i, slot):
        extra = sum2[slot] / local
        stats[b, i, 0:1, :] = shift2[slot] + extra
        stats[b, i, 1:2, :] = square2[slot] - sum2[slot] * extra

    def derive(stats, base, count):
        mean, var = combine(stats[...], local)
        inverse = 1.0 / jnp.sqrt(var + eps)
        for i in range(count):
            block = first_block + base + i
            scale = gb[block, 2:3, :] * inverse[i]
            affine[block, 0:1, :] = scale
            affine[block, 1:2, :] = (shift2[base + i] - mean[i]) * scale + gb[block, 3:4, :]

    def outgoing(t, carry):
        for ahead in range(1, join + 1):

            @pl.when(t * join + ahead < rows)
            def _():
                line(t * join + ahead)

        for i in range(lacking):
            measure(t, out_slot + i)

        @pl.when(jnp.logical_and(gone == 0, t < HELD))
        def _():
            lax.fori_loop(t * per_piece, (t + 1) * per_piece, sec_start, 0)

        return carry

    lax.fori_loop(0, pieces, outgoing, 0)
    for i in range(lacking):
        record(stat_out, i, out_slot + i)
    stats_send(nb, b, stat_out, st2_send.at[0], st2_recv.at[0])

    def keeping(t, carry):
        for i in range(2 * more):
            measure(t, keep_slot + i)

        relay(t)
        return carry

    begun = pieces // 2 if more else 0
    if more:
        lax.fori_loop(0, begun, keeping, 0)
    stats_wait(nb, b, stat_out, st2_send.at[0], st2_recv.at[0])
    derive(stat_out, out_slot, lacking)

    @pl.when(gone == 0)
    def _():
        for i in range(mids):
            affine_copy((1 - side) * mids + i, near_block).start()
        lax.fori_loop(min(HELD, pieces) * per_piece, units, sec_start, 0)

    if more:
        lax.fori_loop(begun, pieces, keeping, 0)
        for i in range(2 * more):
            record(stat_keep, i, keep_slot + i)
        stats_send(nb, b, stat_keep, st4_send.at[0], st4_recv.at[0])
        for tick in range(pieces, pieces + 2):
            relay(tick)
        stats_wait(nb, b, stat_keep, st4_send.at[0], st4_recv.at[0])
        derive(stat_keep, keep_slot, 2 * more)

    w3_load.wait()
    sum3[...] = jnp.zeros_like(sum3)
    square3[...] = jnp.zeros_like(square3)
    lag = SKEW * gone

    def expand(t):
        values = []
        for block in range(n):
            value = sec[block, pl.ds(t * join, join)].reshape(tall, width).astype(f32)
            value = value * affine[block, 0:1, :] + affine[block, 1:2, :]
            values.append(jnp.maximum(value, 0.0).astype(bf16))
        total = jnp.dot(
            jnp.concatenate(values, axis=1), w3[...], preferred_element_type=f32
        )
        third[t] = total

        @pl.when(t == 0)
        def _():
            shift3[...] = column_sum(total) / tall

        moved = third[t] - shift3[...]
        sum3[...] += column_sum(moved)
        square3[...] += column_sum(moved * moved)

    relay_first = pieces + 2 if more else 0
    ready = relay_first + 1

    def relay_step(s, carry):
        relay(s)

        @pl.when(s == ready)
        def _():
            remote(
                affine.at[pl.ds(far_block, lacking)], affine.at[pl.ds(far_block, lacking)],
                aff_send.at[0], aff_recv.at[0], {"chan": lax.rem(z + 1, n)},
            ).wait_recv()

        t_late = s - ready
        catching = jnp.logical_and(t_late >= 0, t_late < pieces)
        catching = jnp.logical_and(catching, per_piece * (t_late + 1) - 1 + lag <= s)
        fresh = s - (per_piece - 1) - lag
        t_fresh = lax.div(fresh, per_piece)
        arriving = jnp.logical_and(fresh >= 0, lax.rem(fresh, per_piece) == 0)
        arriving = jnp.logical_and(arriving, t_fresh < pieces)
        arriving = jnp.logical_and(arriving, ready + t_fresh < s)

        @pl.when(jnp.logical_or(catching, arriving))
        def _():
            expand(jnp.where(catching, t_late, t_fresh))

        return carry

    relay_last = jnp.maximum(units + lag, ready + pieces)
    lax.fori_loop(relay_first, relay_last, relay_step, 0)

    extra = sum3[...] / local
    stat3[b, 0:1, :] = shift3[...] + extra
    stat3[b, 1:2, :] = square3[...] - sum3[...] * extra
    stats_send(nb, b, stat3, st3_send.at[0], st3_recv.at[0])

    sent = wown.at[0, pl.ds(0, (n - 1) * strip), :]
    remote(sent, sent, w1_send.at[0], w1_recv.at[0], {"batch": partner}).wait_send()
    gb_all().wait_send()
    for to in range(n):

        @pl.when(z != to)
        def _():
            hop_all(to).wait_send()
            pair_all(to).wait_send()

    w2_sent = w2.at[0, :, :, pl.ds(0, (mids - 1) * band), :]
    right = {"chan": lax.rem(z + 1, n)}
    remote(w2_sent, w2_sent, w2_send.at[0], w2_recv.at[0, 0], right).wait_send()
    half_slots(lambda slot: w2hop_all(slot).wait_send())
    half_slots(lambda slot: w2pair_all(slot).wait_send())
    if more:
        w2_one = w2.at[0, :, :, pl.ds(0, band), :]
        w2hop_all(more_slot).wait_send()
        w2pair_all(more_slot).wait_send()

        @pl.when(inner)
        def _():
            remote(w2_one, w2_one, w2_send.at[2], w2_recv.at[0, 0], right).wait_send()

        @pl.when(gone == 0)
        def _():
            remote(w2_one, w2_one, w2_send.at[1], w2_recv.at[0, 0], right).wait_send()

    for f in range(2):

        @pl.when(z != (n - 1) * (1 - f))
        def _():
            remote(flow.at[f], flow.at[f], flow_send.at[f], flow_recv.at[f, 0], right).wait_send()

    sec_sent = sec.at[pl.ds(0, lacking)]

    @pl.when(gone == 0)
    def _():
        for i in range(mids):
            affine_copy((1 - side) * mids + i, near_block).wait_send()
        remote(sec_sent, sec_sent, sec_send.at[0], sec_recv.at[0], right).wait_send()

    @pl.when(inner)
    def _():
        remote(sec_sent, sec_sent, sec_send.at[1], sec_recv.at[0], right).wait_send()

    stats_wait(nb, b, stat3, st3_send.at[0], st3_recv.at[0])
    mean3, var3 = combine(stat3[...], local)
    scale3 = gain3[...] / jnp.sqrt(var3 + eps)
    bias3_value = bias3[...]

    def finish(t, carry):
        kept = img[pl.ds(t * join, join)].reshape(tall, out_local).astype(f32)
        value = (third[t] - mean3) * scale3 + bias3_value + kept
        outv[t] = jnp.maximum(value, 0.0).astype(bf16)
        return carry

    lax.fori_loop(0, pieces, finish, 0)


def body(
    images,
    reduce_weight,
    reduce_gain,
    reduce_bias,
    spatial_weight,
    spatial_gain,
    spatial_bias,
    expand_weight,
    expand_gain,
    expand_bias,
):
    imgs, side = (images.shape[0], images.shape[1])
    n, nb = lax.axis_size("chan"), lax.axis_size("batch")
    width = reduce_weight.shape[1]
    depth = images.shape[3]
    out_local = expand_weight.shape[1]
    rows, height = side, side * imgs
    chunks = n * rows
    mid = n * width
    mids = n // 2
    more = EXTRA if mids > 1 else 0
    slots, lacking = mids + more, mids - more
    join = 2 if side % 2 == 0 else 1
    pieces, tall = side // join, height * join
    dma, f32, bf16 = pltpu.SemaphoreType.DMA, jnp.float32, jnp.bfloat16
    vmem = pl.BlockSpec(memory_space=pltpu.VMEM)
    anywhere = pl.BlockSpec(memory_space=pl.ANY)
    flat = images.transpose(1, 2, 0, 3).reshape(rows, height, depth)
    out = pl.pallas_call(
        functools.partial(block_kernel, n, nb, imgs),
        out_shape=pltpu.VMEM((pieces, tall, out_local), bf16),
        in_specs=[anywhere, anywhere, vmem, vmem, anywhere, vmem, vmem, anywhere, vmem, vmem],
        out_specs=vmem,
        scratch_shapes=[
            pltpu.VMEM((rows, height, depth), bf16),
            pltpu.VMEM(reduce_weight.shape, bf16),
            pltpu.VMEM((n, depth, width), bf16),
            pltpu.VMEM((chunks, height, width), f32),
            pltpu.VMEM((2, rows, height, width), f32),
            pltpu.VMEM((2, chunks, height, width), bf16),
            pltpu.VMEM((n, 4, width), f32),
        ]
        + [pltpu.VMEM((n, 1, width), f32)] * 3
        + [
            pltpu.VMEM((n, nb, 2, width), f32),
            pltpu.VMEM((n, rows + 2, height, width), bf16),
            pltpu.VMEM((slots, 3, 3, mid, width), bf16),
            pltpu.VMEM((slots, rows, height, width), f32),
            pltpu.VMEM((n, rows, height, width), bf16),
        ]
        + [pltpu.VMEM((slots, 1, width), f32)] * 3
        + [
            pltpu.VMEM((nb, lacking, 2, width), f32),
            pltpu.VMEM((nb, 2, 2, width), f32),
            pltpu.VMEM((n, 2, width), f32),
            pltpu.VMEM(expand_weight.shape, bf16),
            pltpu.VMEM((pieces, tall, out_local), f32),
        ]
        + [pltpu.VMEM((1, out_local), f32)] * 3
        + [pltpu.VMEM((nb, 2, out_local), f32)]
        + [dma((4,))]
        + [dma((1,))] * 2
        + [dma((1,)), dma((n,))]
        + [dma((n,))] * 4
        + [dma((2,)), dma((2, chunks))]
        + [dma((n,))] * 2
        + [dma((3,)), dma((slots, 3))]
        + [dma((slots,))] * 4
        + [dma((2,)), dma((lacking * rows,))]
        + [dma((1,))] * 4
        + [dma((n,)), dma((1,))]
        + [dma((1,))] * 2,
        compiler_params=pltpu.CompilerParams(
            collective_id=0, has_side_effects=True, vmem_limit_bytes=LIMIT
        ),
        name="block",
    )(
        flat,
        reduce_weight,
        reduce_gain[None, :],
        reduce_bias[None, :],
        spatial_weight,
        spatial_gain[None, :],
        spatial_bias[None, :],
        expand_weight,
        expand_gain[None, :],
        expand_bias[None, :],
    )
    return out.reshape(side, side, imgs, out_local).transpose(2, 0, 1, 3)


def solution(mesh):
    in_specs = (
        P("batch", None, None, "chan"),
        P(None, "chan"),
        P("chan"),
        P("chan"),
        P(None, None, None, "chan"),
        P("chan"),
        P("chan"),
        P(None, "chan"),
        P("chan"),
        P("chan"),
    )
    out_specs = P("batch", None, None, "chan")
    return jax.shard_map(body, mesh=mesh, in_specs=in_specs, out_specs=out_specs, check_vma=False)
```

```python
import functools

import jax
import jax.numpy as jnp
from jax import lax
from jax.experimental import pallas as pl
from jax.experimental.pallas import tpu as pltpu
from jax.sharding import PartitionSpec as P

eps = 0.001
MESH = pl.DeviceIdType.MESH
LIMIT = 59 * 1024 * 1024
SKEW = 3
EXTRA = 1
HELD = 4
SETTLE = 8
INNER_SHARE = (0, 2, 4)
OUTER_SHARE = (0, 2, 4)
INNER_MORE = (20, 26, 34)
OUTER_MORE = (14, 23, 33)
MORE_CHAIN = (1, 3, 5)


def remote(src, dst, send, recv, device):
    return pltpu.make_async_remote_copy(
        src_ref=src, dst_ref=dst, send_sem=send, recv_sem=recv,
        device_id=device, device_id_type=MESH,
    )


def greet(n, nb, z, b):
    barrier = pltpu.get_barrier_semaphore()
    for off in range(1, n):
        pl.semaphore_signal(
            barrier, inc=1, device_id={"chan": lax.rem(z + off, n)}, device_id_type=MESH
        )
    for off in range(1, nb):
        pl.semaphore_signal(
            barrier, inc=1, device_id={"batch": lax.rem(b + off, nb)}, device_id_type=MESH
        )
    pl.semaphore_wait(barrier, n + nb - 2)


def stats_send(nb, b, stats, send, recv):
    for off in range(1, nb):
        peer = lax.rem(b + off, nb)
        remote(stats.at[b], stats.at[b], send, recv, {"batch": peer}).start()


def stats_wait(nb, b, stats, send, recv):
    others = stats.at[pl.ds(0, nb - 1)]
    remote(others, others, send, recv, {"batch": lax.rem(b + 1, nb)}).wait()


def combine(stats, local):
    nb = stats.shape[0]
    means = stats[..., 0:1, :]
    mean = jnp.sum(means, axis=0) / nb
    away = means - mean[None]
    spread = jnp.sum(stats[..., 1:2, :], axis=0) + local * jnp.sum(away * away, axis=0)
    return mean, spread / (local * nb)


def column_sum(value):
    return jnp.sum(value, axis=0, keepdims=True)


def block_kernel(
    n, nb, imgs,
    img_hbm, w1_hbm, gain1, bias1, sw_hbm, gain2, bias2, w3_hbm, gain3, bias3,
    outv,
    img, w1, wown, part, whole, flow, gb, shift1, sum1, square1, stat1, act, w2, acc, sec,
    shift2, sum2, square2, stat_out, stat_keep, affine, w3, third, shift3, sum3, square3, stat3,
    load_sem,
    gb_send, gb_recv, w1_send, w1_recv, hop_send, hop_recv, pair_send, pair_recv,
    flow_send, flow_recv, st1_send, st1_recv,
    w2_send, w2_recv, w2hop_send, w2hop_recv, w2pair_send, w2pair_recv,
    sec_send, sec_recv, st2_send, st2_recv, st4_send, st4_recv, aff_send, aff_recv, st3_send, st3_recv,
):
    z, b = lax.axis_index("chan"), lax.axis_index("batch")
    rows, height, depth = img.shape
    width = wown.shape[2]
    slots = w2.shape[0]
    pieces, tall, out_local = third.shape
    join = rows // pieces
    mids = n // 2
    more = slots - mids
    lacking = mids - more
    hops = nb // 2
    chunks = n * rows
    strip = depth // nb
    band = n * width // nb
    local = rows * height
    per_piece = lacking * join
    units = lacking * rows
    partner = b + 1 - 2 * lax.rem(b, 2)
    at_first, at_last = z == 0, z == n - 1
    at_end = jnp.logical_or(at_first, at_last)
    inner = jnp.logical_not(at_end)
    side = jnp.where(z < mids, 0, 1)
    gone = jnp.where(z < mids, mids - 1 - z, z - mids)
    first_block = side * (mids - more)
    my_slot = z - first_block
    half_slot = side * more
    more_slot = (1 - side) * mids
    out_slot = side * (slots - lacking)
    keep_slot = (1 - side) * lacking
    late_flow = 1 - side
    late_skew = SKEW * jnp.maximum(z, n - 1 - z)
    early_skew = SKEW * jnp.minimum(z, n - 1 - z)
    f32, bf16 = jnp.float32, jnp.bfloat16

    w1_load = pltpu.make_async_copy(w1_hbm, w1, load_sem.at[0])
    w1_load.start()
    img_load = pltpu.make_async_copy(img_hbm, img, load_sem.at[1])
    img_load.start()
    w3_load = pltpu.make_async_copy(w3_hbm, w3, load_sem.at[2])
    w3_load.start()

    w2_load = pltpu.make_async_copy(sw_hbm, w2.at[my_slot], load_sem.at[3])
    w2_load.start()
    gb[z, 0:1, :] = gain1[...]
    gb[z, 1:2, :] = bias1[...]
    gb[z, 2:3, :] = gain2[...]
    gb[z, 3:4, :] = bias2[...]
    greet(n, nb, z, b)

    def rows_of(who):
        return pl.ds(pl.multiple_of(who * strip, 16), strip)

    def w1_copy(to):
        src = w1.at[pl.ds(pl.multiple_of(to * depth + b * strip, 16), strip), :]
        return remote(src, wown.at[z, rows_of(b), :], w1_send.at[0], w1_recv.at[z], {"chan": to})

    def gb_copy(to, slot):
        return remote(gb.at[z], gb.at[slot], gb_send.at[0], gb_recv.at[0], {"chan": to})

    def band_of(who):
        return pl.ds(pl.multiple_of(who * band, 16), band)

    w1_load.wait()
    for far in range(n - 1, 0, -1):

        @pl.when(z + far < n)
        def _():
            w1_copy(z + far).start()

        @pl.when(z - far >= 0)
        def _():
            w1_copy(z - far).start()

    for off in range(1, n):
        gb_copy(lax.rem(z + off, n), z).start()

    def band_ref(slot, row_tap, who):
        return w2.at[slot, row_tap, :, band_of(who), :]

    def w2_give(row_tap, to, slot, kind):
        src = sw_hbm.at[row_tap, :, band_of(b), :]
        return remote(
            src, band_ref(slot, row_tap, b), w2_send.at[kind], w2_recv.at[slot, row_tap],
            {"chan": to},
        )

    def half_give(row_tap):
        for off in range(1, mids):
            to = side * mids + lax.rem(z - side * mids + off, mids)
            w2_give(row_tap, to, my_slot, 0).start()

    for row_tap in range(3):
        if more:

            @pl.when(gone == 0)
            def _():
                to = jnp.where(side == 0, mids, mids - 1)
                w2_give(row_tap, to, jnp.where(side == 0, 0, mids), 1).start()

        half_give(row_tap)

    def strip_copy(g, who, send, recv, device):
        ref = wown.at[g, rows_of(who), :]
        return remote(ref, ref, send, recv, device)

    def distribute(g):
        @pl.when(z != g)
        def _():
            strip_copy(g, b, w1_send.at[0], w1_recv.at[g], {"chan": g}).wait_recv()
            for hop in range(1, hops):
                peer = lax.rem(b + 2 * hop, nb)
                strip_copy(g, b, hop_send.at[g], hop_recv.at[g], {"batch": peer}).start()
            strip_copy(g, b, pair_send.at[g], pair_recv.at[g], {"batch": partner}).start()

    def hop_all(g):
        ref = wown.at[g, pl.ds(0, (hops - 1) * strip), :]
        return remote(ref, ref, hop_send.at[g], hop_recv.at[g], {"batch": partner})

    def pair_all(g):
        ref = wown.at[g, pl.ds(0, hops * strip), :]
        return remote(ref, ref, pair_send.at[g], pair_recv.at[g], {"batch": partner})

    def forward(g):
        @pl.when(z != g)
        def _():
            hop_all(g).wait_recv()
            for hop in range(1, hops):
                peer = lax.rem(b + 2 * hop, nb)
                strip_copy(g, peer, pair_send.at[g], pair_recv.at[g], {"batch": partner}).start()

    def complete(g):
        @pl.when(z != g)
        def _():
            pair_all(g).wait_recv()

    def flow_copy(f, k):
        to = jnp.where(f == 0, lax.rem(z + 1, n), lax.rem(z + n - 1, n))
        ref = flow.at[f, k]
        return remote(ref, ref, flow_send.at[f], flow_recv.at[f, k], {"chan": to})

    img_load.wait()

    def own_products(r, carry):
        k = z * rows + r
        value = jnp.dot(
            img[r], w1[pl.ds(pl.multiple_of(z * depth, 16), depth), :], preferred_element_type=f32
        )
        part[k] = value

        @pl.when(at_first)
        def _():
            flow[0, k] = value.astype(bf16)
            flow_copy(0, k).start()

        return carry

    lax.fori_loop(0, rows, own_products, 0)
    for g in range(n):
        distribute(g)
    act[:, 0] = jnp.zeros_like(act[:, 0])
    act[:, rows + 1] = jnp.zeros_like(act[:, 0])

    def clear(r, carry):
        acc[:, r] = jnp.zeros_like(acc[:, r])
        return carry

    lax.fori_loop(0, rows, clear, 0)
    forward(0)

    def w2_share(slot, row_tap):
        ref = band_ref(slot, row_tap, b)
        for hop in range(1, hops):
            peer = lax.rem(b + 2 * hop, nb)
            remote(ref, ref, w2hop_send.at[slot], w2hop_recv.at[slot], {"batch": peer}).start()
        remote(ref, ref, w2pair_send.at[slot], w2pair_recv.at[slot], {"batch": partner}).start()

    def w2_arrive(slot, row_tap):
        ref = band_ref(slot, row_tap, b)
        remote(ref, ref, w2_send.at[0], w2_recv.at[slot, row_tap], {"chan": z}).wait_recv()

    def half_share(row_tap):
        def work(slot):
            w2_arrive(slot, row_tap)
            w2_share(slot, row_tap)

        half_slots(work)

    def w2_chain(row_tap):
        ref = band_ref(more_slot, row_tap, b)
        to = jnp.where(side == 0, lax.rem(z + n - 1, n), lax.rem(z + 1, n))
        return remote(ref, ref, w2_send.at[2], w2_recv.at[more_slot, row_tap], {"chan": to})

    def w2hop_all(slot):
        ref = w2.at[slot, :, :, pl.ds(0, (hops - 1) * band), :]
        return remote(ref, ref, w2hop_send.at[slot], w2hop_recv.at[slot], {"batch": partner})

    def w2pair_all(slot):
        ref = w2.at[slot, :, :, pl.ds(0, hops * band), :]
        return remote(ref, ref, w2pair_send.at[slot], w2pair_recv.at[slot], {"batch": partner})

    def w2_forward(slot):
        w2hop_all(slot).wait_recv()
        for row_tap in range(3):
            for hop in range(1, hops):
                ref = band_ref(slot, row_tap, lax.rem(b + 2 * hop, nb))
                remote(
                    ref, ref, w2pair_send.at[slot], w2pair_recv.at[slot], {"batch": partner}
                ).start()

    def half_slots(work):
        for off in range(1, mids):
            work(half_slot + lax.rem(my_slot - half_slot + off, mids))

    def gb_all():
        ref = gb.at[pl.ds(0, n - 1)]
        return remote(ref, ref, gb_send.at[0], gb_recv.at[0], {"chan": lax.rem(z + 1, n)})

    def finalize(k, value):
        g, r = lax.div(k, rows), lax.rem(k, rows)
        whole[lax.rem(g, 2), r] = value

        @pl.when(r == 0)
        def _():
            shift1[g] = column_sum(value) / height
            sum1[g] = jnp.zeros_like(sum1[g])
            square1[g] = jnp.zeros_like(square1[g])

        moved = value - shift1[g]
        sum1[g] += column_sum(moved)
        square1[g] += column_sum(moved * moved)

    def first_stats(g):
        extra = sum1[g] / local
        stat1[g, b, 0:1, :] = shift1[g] + extra
        stat1[g, b, 1:2, :] = square1[g] - sum1[g] * extra
        stats_send(nb, b, stat1.at[g], st1_send.at[g], st1_recv.at[g])

    def first_affine(g):
        stats_wait(nb, b, stat1.at[g], st1_send.at[g], st1_recv.at[g])
        mean, var = combine(stat1[g], local)
        scale = gb[g, 0:1, :] / jnp.sqrt(var + eps)
        bias = gb[g, 1:2, :]

        def line(r):
            value = (whole[lax.rem(g, 2), r] - mean) * scale + bias
            act[g, r + 1] = jnp.maximum(value, 0.0).astype(bf16)

        return line

    def tap_products(g, t, slot):
        for col_tap in range(3):
            total = None
            for row_tap in range(3):
                window = act[g, pl.ds(t * join + row_tap, join)].reshape(tall, width)
                weight = w2[slot, row_tap, col_tap, pl.ds(pl.multiple_of(g * width, 128), width), :]
                term = jnp.dot(window, weight, preferred_element_type=f32)
                total = term if total is None else total + term
            yield total.reshape(join, height, width)

    def convolve(g, t, slot):
        lines = pl.ds(t * join, join)
        left, middle, right = tap_products(g, t, slot)
        acc[slot, lines, imgs:, :] += left[:, : height - imgs]
        acc[slot, lines] += middle
        acc[slot, lines, : height - imgs, :] += right[:, imgs:]

    def convolve_last(t, slot):
        left, middle, right = tap_products(last, t, slot)
        edge = jnp.zeros((join, imgs, width), f32)
        total = acc[slot, pl.ds(t * join, join)] + middle
        total = total + jnp.concatenate([edge, left[:, : height - imgs]], axis=1)
        total = total + jnp.concatenate([right[:, imgs:], edge], axis=1)
        return total.reshape(tall, width)

    last = n - 1
    all_begin = last * rows - pieces + 1
    more_begin = all_begin - pieces
    half_begin = more_begin - (last - 1) * pieces

    def step(s, carry):
        for g in range(1, n):

            @pl.when(s == (g - 1) * (rows // 2) + 2)
            def _():
                forward(g)

        for row_tap in range(3):
            if more:

                @pl.when(s == jnp.where(at_end, OUTER_MORE[row_tap], MORE_CHAIN[row_tap]))
                def _():
                    w2_arrive(more_slot, row_tap)

                    @pl.when(inner)
                    def _():
                        w2_chain(row_tap).start()

                @pl.when(s == jnp.where(at_end, OUTER_MORE[row_tap], INNER_MORE[row_tap]))
                def _():
                    w2_share(more_slot, row_tap)

            @pl.when(s == jnp.where(at_end, OUTER_SHARE[row_tap], INNER_SHARE[row_tap]))
            def _():
                half_share(row_tap)

        for extra in range(2):
            k = 2 * s + extra
            g, r = lax.div(k, rows), lax.rem(k, rows)

            @pl.when(k < chunks)
            def _():
                @pl.when(r == 0)
                def _():
                    complete(g)

                @pl.when(z != g)
                def _():
                    part[k] = jnp.dot(img[r], wown[g], preferred_element_type=f32)

                @pl.when(jnp.logical_and(at_end, jnp.logical_or(at_last, k >= rows)))
                def _():
                    flow[side, k] = part[k].astype(bf16)
                    flow_copy(side, k).start()

        early = s - early_skew

        @pl.when(jnp.logical_and(inner, jnp.logical_and(early >= 0, early < chunks)))
        def _():
            flow_copy(side, early).wait_recv()
            flow[side, early] = (part[early] + flow[side, early].astype(f32)).astype(bf16)
            flow_copy(side, early).start()

        late = s - late_skew
        after = late - (rows - 1)

        @pl.when(late >= 0)
        def _():
            flow_copy(late_flow, late).wait_recv()
            coming = flow[late_flow, late].astype(f32)

            @pl.when(inner)
            def _():
                flow[late_flow, late] = (part[late] + coming).astype(bf16)
                flow_copy(late_flow, late).start()
                finalize(late, flow[side, late].astype(f32) + coming)

            @pl.when(at_end)
            def _():
                finalize(late, part[late] + coming)

        @pl.when(after == half_begin - 4)
        def _():
            half_slots(w2_forward)

        @pl.when(after == half_begin - 1)
        def _():
            w2_load.wait()
            half_slots(lambda slot: w2pair_all(slot).wait_recv())

        if more:

            @pl.when(after == more_begin - 5)
            def _():
                w2_forward(more_slot)

            @pl.when(after == more_begin - 1)
            def _():
                w2pair_all(more_slot).wait_recv()

        @pl.when(after >= 0)
        def _():
            g, v = lax.div(after, rows), lax.rem(after, rows)

            @pl.when(v == 0)
            def _():
                first_stats(g)

            @pl.when(v == SETTLE)
            def _():
                @pl.when(g == 0)
                def _():
                    gb_all().wait_recv()

                line = first_affine(g)

                def each_line(r, carry):
                    line(r)
                    return carry

                lax.fori_loop(0, rows, each_line, 0)

        item = after - half_begin

        @pl.when(jnp.logical_and(item >= 0, item < (last - 1) * pieces))
        def _():
            for i in range(mids):
                convolve(lax.div(item, pieces), lax.rem(item, pieces), half_slot + i)

        if more:

            @pl.when(jnp.logical_and(after >= more_begin, after < more_begin + pieces))
            def _():
                for g in range(last - 1):
                    convolve(g, after - more_begin, more_slot)

        @pl.when(after >= all_begin)
        def _():
            for slot in range(slots):
                convolve(last - 1, after - all_begin, slot)

        return carry

    lax.fori_loop(0, chunks + late_skew, step, 0)

    def sec_copy(f, u):
        to = jnp.where(f == 0, lax.rem(z + 1, n), lax.rem(z + n - 1, n))
        t, rest = lax.div(u, per_piece), lax.rem(u, per_piece)
        block = lax.div(rest, join) + f * (mids + more)
        ref = sec.at[block, t * join + lax.rem(rest, join)]
        kind = jnp.where(f == side, 0, 1)
        return remote(ref, ref, sec_send.at[kind], sec_recv.at[u], {"chan": to})

    def sec_start(u, carry):
        sec_copy(side, u).start()
        return carry

    far_block = (1 - side) * (mids + more)
    near_block = side * (mids + more)

    def affine_copy(to, block):
        ref = affine.at[pl.ds(block, lacking)]
        return remote(ref, ref, aff_send.at[to], aff_recv.at[0], {"chan": to})

    def relay(tick):
        u = tick - SKEW * gone

        @pl.when(jnp.logical_and(u >= 0, u < units))
        def _():
            sec_copy(1 - side, u).wait_recv()

            @pl.when(inner)
            def _():
                sec_copy(1 - side, u).start()

    line = first_affine(last)

    def measure(t, slot, fresh):
        total = convolve_last(t, slot)
        if fresh:
            shift2[slot] = column_sum(total) / tall
        moved = total - shift2[slot]
        sums, squares = column_sum(moved), column_sum(moved * moved)
        if fresh:
            sum2[slot] = sums
            square2[slot] = squares
        else:
            sum2[slot] += sums
            square2[slot] += squares
        lines = pl.ds(t * join, join)
        sec[first_block + slot, lines] = moved.astype(bf16).reshape(join, height, width)

    def record(stats, i, slot):
        extra = sum2[slot] / local
        stats[b, i, 0:1, :] = shift2[slot] + extra
        stats[b, i, 1:2, :] = square2[slot] - sum2[slot] * extra

    def derive(stats, base, count):
        mean, var = combine(stats[...], local)
        inverse = 1.0 / jnp.sqrt(var + eps)
        for i in range(count):
            block = first_block + base + i
            scale = gb[block, 2:3, :] * inverse[i]
            affine[block, 0:1, :] = scale
            affine[block, 1:2, :] = (shift2[base + i] - mean[i]) * scale + gb[block, 3:4, :]

    def outgoing(t, fresh):
        for ahead in range(1, join + 1):
            line(jnp.minimum(t * join + ahead, rows - 1))
        for i in range(lacking):
            measure(t, out_slot + i, fresh)

        @pl.when(jnp.logical_and(gone == 0, t < HELD))
        def _():
            lax.fori_loop(t * per_piece, (t + 1) * per_piece, sec_start, 0)

    def outgoing_next(t, carry):
        outgoing(t, False)
        return carry

    line(0)
    outgoing(0, True)
    lax.fori_loop(1, pieces, outgoing_next, 0)
    for i in range(lacking):
        record(stat_out, i, out_slot + i)
    stats_send(nb, b, stat_out, st2_send.at[0], st2_recv.at[0])

    def keeping(t, fresh):
        relay(t)
        for i in range(2 * more):
            measure(t, keep_slot + i, fresh)

    def keeping_next(t, carry):
        keeping(t, False)
        return carry

    begun = max(pieces // 2, 1)
    if more:
        keeping(0, True)
        lax.fori_loop(1, begun, keeping_next, 0)
    stats_wait(nb, b, stat_out, st2_send.at[0], st2_recv.at[0])
    derive(stat_out, out_slot, lacking)

    @pl.when(gone == 0)
    def _():
        for i in range(mids):
            affine_copy((1 - side) * mids + i, near_block).start()
        lax.fori_loop(min(HELD, pieces) * per_piece, units, sec_start, 0)

    if more:
        lax.fori_loop(begun, pieces, keeping_next, 0)
        for i in range(2 * more):
            record(stat_keep, i, keep_slot + i)
        stats_send(nb, b, stat_keep, st4_send.at[0], st4_recv.at[0])
        for tick in range(pieces, pieces + 2):
            relay(tick)
        stats_wait(nb, b, stat_keep, st4_send.at[0], st4_recv.at[0])
        derive(stat_keep, keep_slot, 2 * more)

    w3_load.wait()
    sum3[...] = jnp.zeros_like(sum3)
    square3[...] = jnp.zeros_like(square3)
    lag = SKEW * gone

    def expand(t):
        values = []
        for block in range(n):
            value = sec[block, pl.ds(t * join, join)].reshape(tall, width).astype(f32)
            value = value * affine[block, 0:1, :] + affine[block, 1:2, :]
            values.append(jnp.maximum(value, 0.0).astype(bf16))
        total = jnp.dot(
            jnp.concatenate(values, axis=1), w3[...], preferred_element_type=f32
        )
        third[t] = total

        @pl.when(t == 0)
        def _():
            shift3[...] = column_sum(total) / tall

        moved = third[t] - shift3[...]
        sum3[...] += column_sum(moved)
        square3[...] += column_sum(moved * moved)

    relay_first = pieces + 2 if more else 0
    ready = relay_first + 1

    def relay_step(s, carry):
        relay(s)

        @pl.when(s == ready)
        def _():
            remote(
                affine.at[pl.ds(far_block, lacking)], affine.at[pl.ds(far_block, lacking)],
                aff_send.at[0], aff_recv.at[0], {"chan": lax.rem(z + 1, n)},
            ).wait_recv()

        t_late = s - ready
        catching = jnp.logical_and(t_late >= 0, t_late < pieces)
        catching = jnp.logical_and(catching, per_piece * (t_late + 1) - 1 + lag <= s)
        fresh = s - (per_piece - 1) - lag
        t_fresh = lax.div(fresh, per_piece)
        arriving = jnp.logical_and(fresh >= 0, lax.rem(fresh, per_piece) == 0)
        arriving = jnp.logical_and(arriving, t_fresh < pieces)
        arriving = jnp.logical_and(arriving, ready + t_fresh < s)

        @pl.when(jnp.logical_or(catching, arriving))
        def _():
            expand(jnp.where(catching, t_late, t_fresh))

        return carry

    relay_last = jnp.maximum(units + lag, ready + pieces)
    lax.fori_loop(relay_first, relay_last, relay_step, 0)

    extra = sum3[...] / local
    stat3[b, 0:1, :] = shift3[...] + extra
    stat3[b, 1:2, :] = square3[...] - sum3[...] * extra
    stats_send(nb, b, stat3, st3_send.at[0], st3_recv.at[0])

    sent = wown.at[0, pl.ds(0, (n - 1) * strip), :]
    remote(sent, sent, w1_send.at[0], w1_recv.at[0], {"batch": partner}).wait_send()
    gb_all().wait_send()
    for to in range(n):

        @pl.when(z != to)
        def _():
            hop_all(to).wait_send()
            pair_all(to).wait_send()

    w2_sent = w2.at[0, :, :, pl.ds(0, (mids - 1) * band), :]
    right = {"chan": lax.rem(z + 1, n)}
    remote(w2_sent, w2_sent, w2_send.at[0], w2_recv.at[0, 0], right).wait_send()
    half_slots(lambda slot: w2hop_all(slot).wait_send())
    half_slots(lambda slot: w2pair_all(slot).wait_send())
    if more:
        w2_one = w2.at[0, :, :, pl.ds(0, band), :]
        w2hop_all(more_slot).wait_send()
        w2pair_all(more_slot).wait_send()

        @pl.when(inner)
        def _():
            remote(w2_one, w2_one, w2_send.at[2], w2_recv.at[0, 0], right).wait_send()

        @pl.when(gone == 0)
        def _():
            remote(w2_one, w2_one, w2_send.at[1], w2_recv.at[0, 0], right).wait_send()

    for f in range(2):

        @pl.when(z != (n - 1) * (1 - f))
        def _():
            remote(flow.at[f], flow.at[f], flow_send.at[f], flow_recv.at[f, 0], right).wait_send()

    sec_sent = sec.at[pl.ds(0, lacking)]

    @pl.when(gone == 0)
    def _():
        for i in range(mids):
            affine_copy((1 - side) * mids + i, near_block).wait_send()
        remote(sec_sent, sec_sent, sec_send.at[0], sec_recv.at[0], right).wait_send()

    @pl.when(inner)
    def _():
        remote(sec_sent, sec_sent, sec_send.at[1], sec_recv.at[0], right).wait_send()

    stats_wait(nb, b, stat3, st3_send.at[0], st3_recv.at[0])
    mean3, var3 = combine(stat3[...], local)
    scale3 = gain3[...] / jnp.sqrt(var3 + eps)
    bias3_value = bias3[...]

    def finish(t, carry):
        kept = img[pl.ds(t * join, join)].reshape(tall, out_local).astype(f32)
        value = (third[t] - mean3) * scale3 + bias3_value + kept
        outv[t] = jnp.maximum(value, 0.0).astype(bf16)
        return carry

    lax.fori_loop(0, pieces, finish, 0)


def body(
    images,
    reduce_weight,
    reduce_gain,
    reduce_bias,
    spatial_weight,
    spatial_gain,
    spatial_bias,
    expand_weight,
    expand_gain,
    expand_bias,
):
    imgs, side = (images.shape[0], images.shape[1])
    n, nb = lax.axis_size("chan"), lax.axis_size("batch")
    width = reduce_weight.shape[1]
    depth = images.shape[3]
    out_local = expand_weight.shape[1]
    rows, height = side, side * imgs
    chunks = n * rows
    mid = n * width
    mids = n // 2
    more = EXTRA if mids > 1 else 0
    slots, lacking = mids + more, mids - more
    join = 2 if side % 2 == 0 else 1
    pieces, tall = side // join, height * join
    dma, f32, bf16 = pltpu.SemaphoreType.DMA, jnp.float32, jnp.bfloat16
    vmem = pl.BlockSpec(memory_space=pltpu.VMEM)
    anywhere = pl.BlockSpec(memory_space=pl.ANY)
    flat = images.transpose(1, 2, 0, 3).reshape(rows, height, depth)
    out = pl.pallas_call(
        functools.partial(block_kernel, n, nb, imgs),
        out_shape=pltpu.VMEM((pieces, tall, out_local), bf16),
        in_specs=[anywhere, anywhere, vmem, vmem, anywhere, vmem, vmem, anywhere, vmem, vmem],
        out_specs=vmem,
        scratch_shapes=[
            pltpu.VMEM((rows, height, depth), bf16),
            pltpu.VMEM(reduce_weight.shape, bf16),
            pltpu.VMEM((n, depth, width), bf16),
            pltpu.VMEM((chunks, height, width), f32),
            pltpu.VMEM((2, rows, height, width), f32),
            pltpu.VMEM((2, chunks, height, width), bf16),
            pltpu.VMEM((n, 4, width), f32),
        ]
        + [pltpu.VMEM((n, 1, width), f32)] * 3
        + [
            pltpu.VMEM((n, nb, 2, width), f32),
            pltpu.VMEM((n, rows + 2, height, width), bf16),
            pltpu.VMEM((slots, 3, 3, mid, width), bf16),
            pltpu.VMEM((slots, rows, height, width), f32),
            pltpu.VMEM((n, rows, height, width), bf16),
        ]
        + [pltpu.VMEM((slots, 1, width), f32)] * 3
        + [
            pltpu.VMEM((nb, lacking, 2, width), f32),
            pltpu.VMEM((nb, 2, 2, width), f32),
            pltpu.VMEM((n, 2, width), f32),
            pltpu.VMEM(expand_weight.shape, bf16),
            pltpu.VMEM((pieces, tall, out_local), f32),
        ]
        + [pltpu.VMEM((1, out_local), f32)] * 3
        + [pltpu.VMEM((nb, 2, out_local), f32)]
        + [dma((4,))]
        + [dma((1,))] * 2
        + [dma((1,)), dma((n,))]
        + [dma((n,))] * 4
        + [dma((2,)), dma((2, chunks))]
        + [dma((n,))] * 2
        + [dma((3,)), dma((slots, 3))]
        + [dma((slots,))] * 4
        + [dma((2,)), dma((lacking * rows,))]
        + [dma((1,))] * 4
        + [dma((n,)), dma((1,))]
        + [dma((1,))] * 2,
        compiler_params=pltpu.CompilerParams(
            collective_id=0, has_side_effects=True, vmem_limit_bytes=LIMIT
        ),
        name="block",
    )(
        flat,
        reduce_weight,
        reduce_gain[None, :],
        reduce_bias[None, :],
        spatial_weight,
        spatial_gain[None, :],
        spatial_bias[None, :],
        expand_weight,
        expand_gain[None, :],
        expand_bias[None, :],
    )
    return out.reshape(side, side, imgs, out_local).transpose(2, 0, 1, 3)


def solution(mesh):
    in_specs = (
        P("batch", None, None, "chan"),
        P(None, "chan"),
        P("chan"),
        P("chan"),
        P(None, None, None, "chan"),
        P("chan"),
        P("chan"),
        P(None, "chan"),
        P("chan"),
        P("chan"),
    )
    out_specs = P("batch", None, None, "chan")
    return jax.shard_map(body, mesh=mesh, in_specs=in_specs, out_specs=out_specs, check_vma=False)
```

```python
import functools

import jax
import jax.numpy as jnp
from jax import lax
from jax.experimental import pallas as pl
from jax.experimental.pallas import tpu as pltpu
from jax.sharding import PartitionSpec as P

eps = 0.001
MESH = pl.DeviceIdType.MESH
LIMIT = 59 * 1024 * 1024
SKEW = 3
EXTRA = 1
HELD = 4
SETTLE = 5
AHEAD = 4
PARTIAL = 4
INNER_SHARE = (0, 2, 9)
OUTER_SHARE = (0, 2, 4)
INNER_MORE = (20, 26, 34)
OUTER_MORE = (14, 23, 37)
MORE_CHAIN = (1, 3, 5)


def remote(src, dst, send, recv, device):
    return pltpu.make_async_remote_copy(
        src_ref=src, dst_ref=dst, send_sem=send, recv_sem=recv,
        device_id=device, device_id_type=MESH,
    )


def greet(n, nb, z, b):
    barrier = pltpu.get_barrier_semaphore()
    for off in range(1, n):
        pl.semaphore_signal(
            barrier, inc=1, device_id={"chan": lax.rem(z + off, n)}, device_id_type=MESH
        )
    for off in range(1, nb):
        pl.semaphore_signal(
            barrier, inc=1, device_id={"batch": lax.rem(b + off, nb)}, device_id_type=MESH
        )
    pl.semaphore_wait(barrier, n + nb - 2)


def stats_send(nb, b, stats, send, recv):
    for off in range(1, nb):
        peer = lax.rem(b + off, nb)
        remote(stats.at[b], stats.at[b], send, recv, {"batch": peer}).start()


def stats_wait(nb, b, stats, send, recv):
    others = stats.at[pl.ds(0, nb - 1)]
    remote(others, others, send, recv, {"batch": lax.rem(b + 1, nb)}).wait()


def combine(stats, local):
    nb = stats.shape[0]
    means = stats[..., 0:1, :]
    mean = jnp.sum(means, axis=0) / nb
    away = means - mean[None]
    spread = jnp.sum(stats[..., 1:2, :], axis=0) + local * jnp.sum(away * away, axis=0)
    return mean, spread / (local * nb)


def column_sum(value):
    return jnp.sum(value, axis=0, keepdims=True)


def block_kernel(
    n, nb, imgs,
    img_hbm, w1_hbm, gain1_hbm, bias1_hbm, sw_hbm, gain2_hbm, bias2_hbm, w3_hbm, gain3_hbm, bias3_hbm,
    outv,
    img, w1, wown, part, whole, flow, gb, shift1, sum1, square1, stat1, act, w2, acc, sec,
    shift2, sum2, square2, stat_out, stat_keep, affine, w3, third, shift3, sum3, square3, stat3,
    gain1, bias1, gain2, bias2, gain3, bias3,
    load_sem, small_sem,
    gb_send, gb_recv, w1_send, w1_recv, hop_send, hop_recv, pair_send, pair_recv,
    flow_send, flow_recv, st1_send, st1_recv,
    w2_send, w2_recv, w2hop_send, w2hop_recv, w2pair_send, w2pair_recv,
    sec_send, sec_recv, st2_send, st2_recv, st4_send, st4_recv, aff_send, aff_recv, st3_send, st3_recv,
):
    z, b = lax.axis_index("chan"), lax.axis_index("batch")
    rows, height, depth = img.shape
    width = wown.shape[2]
    slots = w2.shape[0]
    pieces, tall, out_local = third.shape
    join = rows // pieces
    mids = n // 2
    more = slots - mids
    lacking = mids - more
    hops = nb // 2
    chunks = n * rows
    strip = depth // nb
    band = n * width // nb
    local = rows * height
    per_piece = lacking * join
    units = lacking * rows
    partner = b + 1 - 2 * lax.rem(b, 2)
    at_first, at_last = z == 0, z == n - 1
    at_end = jnp.logical_or(at_first, at_last)
    inner = jnp.logical_not(at_end)
    side = jnp.where(z < mids, 0, 1)
    gone = jnp.where(z < mids, mids - 1 - z, z - mids)
    first_block = side * (mids - more)
    my_slot = z - first_block
    half_slot = side * more
    more_slot = (1 - side) * mids
    out_slot = side * (slots - lacking)
    keep_slot = (1 - side) * lacking
    late_flow = 1 - side
    late_skew = SKEW * jnp.maximum(z, n - 1 - z)
    early_skew = SKEW * jnp.minimum(z, n - 1 - z)
    f32, bf16 = jnp.float32, jnp.bfloat16

    w1_load = pltpu.make_async_copy(w1_hbm, w1, load_sem.at[0])
    w1_load.start()
    img_load = pltpu.make_async_copy(img_hbm, img, load_sem.at[1])
    img_load.start()
    w3_load = pltpu.make_async_copy(w3_hbm, w3, load_sem.at[2])
    w3_load.start()

    w2_load = pltpu.make_async_copy(sw_hbm, w2.at[my_slot], load_sem.at[3])
    w2_load.start()
    pairs = [
        (gain1_hbm, gain1), (bias1_hbm, bias1), (gain2_hbm, gain2),
        (bias2_hbm, bias2), (gain3_hbm, gain3), (bias3_hbm, bias3),
    ]
    small = [
        pltpu.make_async_copy(src, dst, small_sem.at[i]) for i, (src, dst) in enumerate(pairs)
    ]
    for copy in small:
        copy.start()
    greet(n, nb, z, b)
    for copy in small:
        copy.wait()
    gb[z, 0:1, :] = gain1[...]
    gb[z, 1:2, :] = bias1[...]
    gb[z, 2:3, :] = gain2[...]
    gb[z, 3:4, :] = bias2[...]

    def rows_of(who):
        return pl.ds(pl.multiple_of(who * strip, 16), strip)

    def w1_copy(to):
        src = w1.at[pl.ds(pl.multiple_of(to * depth + b * strip, 16), strip), :]
        return remote(src, wown.at[z, rows_of(b), :], w1_send.at[0], w1_recv.at[z], {"chan": to})

    def gb_copy(to, slot):
        return remote(gb.at[z], gb.at[slot], gb_send.at[0], gb_recv.at[0], {"chan": to})

    def band_of(who):
        return pl.ds(pl.multiple_of(who * band, 16), band)

    w1_load.wait()
    for far in range(n - 1, 0, -1):

        @pl.when(z + far < n)
        def _():
            w1_copy(z + far).start()

        @pl.when(z - far >= 0)
        def _():
            w1_copy(z - far).start()

    for off in range(1, n):
        gb_copy(lax.rem(z + off, n), z).start()

    def band_ref(slot, row_tap, who):
        return w2.at[slot, row_tap, :, band_of(who), :]

    def w2_give(row_tap, to, slot, kind):
        src = sw_hbm.at[row_tap, :, band_of(b), :]
        return remote(
            src, band_ref(slot, row_tap, b), w2_send.at[kind], w2_recv.at[slot, row_tap],
            {"chan": to},
        )

    def half_give(row_tap):
        for off in range(1, mids):
            to = side * mids + lax.rem(z - side * mids + off, mids)
            w2_give(row_tap, to, my_slot, 0).start()

    for row_tap in range(3):
        if more:

            @pl.when(gone == 0)
            def _():
                to = jnp.where(side == 0, mids, mids - 1)
                w2_give(row_tap, to, jnp.where(side == 0, 0, mids), 1).start()

        if row_tap < 2:
            half_give(row_tap)
        else:

            @pl.when(inner)
            def _():
                half_give(row_tap)

    def strip_copy(g, who, send, recv, device):
        ref = wown.at[g, rows_of(who), :]
        return remote(ref, ref, send, recv, device)

    def distribute(g):
        @pl.when(z != g)
        def _():
            strip_copy(g, b, w1_send.at[0], w1_recv.at[g], {"chan": g}).wait_recv()
            for hop in range(1, hops):
                peer = lax.rem(b + 2 * hop, nb)
                strip_copy(g, b, hop_send.at[g], hop_recv.at[g], {"batch": peer}).start()
            strip_copy(g, b, pair_send.at[g], pair_recv.at[g], {"batch": partner}).start()

    def hop_all(g):
        ref = wown.at[g, pl.ds(0, (hops - 1) * strip), :]
        return remote(ref, ref, hop_send.at[g], hop_recv.at[g], {"batch": partner})

    def pair_all(g):
        ref = wown.at[g, pl.ds(0, hops * strip), :]
        return remote(ref, ref, pair_send.at[g], pair_recv.at[g], {"batch": partner})

    def forward(g):
        @pl.when(z != g)
        def _():
            hop_all(g).wait_recv()
            for hop in range(1, hops):
                peer = lax.rem(b + 2 * hop, nb)
                strip_copy(g, peer, pair_send.at[g], pair_recv.at[g], {"batch": partner}).start()

    def complete(g):
        @pl.when(z != g)
        def _():
            pair_all(g).wait_recv()

    def flow_copy(f, k):
        to = jnp.where(f == 0, lax.rem(z + 1, n), lax.rem(z + n - 1, n))
        ref = flow.at[f, k]
        return remote(ref, ref, flow_send.at[f], flow_recv.at[f, k], {"chan": to})

    img_load.wait()

    def own_products(r, carry):
        k = z * rows + r
        value = jnp.dot(
            img[r], w1[pl.ds(pl.multiple_of(z * depth, 16), depth), :], preferred_element_type=f32
        )
        part[k] = value

        @pl.when(at_first)
        def _():
            flow[0, k] = value.astype(bf16)
            flow_copy(0, k).start()

        return carry

    lax.fori_loop(0, min(AHEAD, rows), own_products, 0)

    @pl.when(at_first)
    def _():
        half_give(2)

    lax.fori_loop(min(AHEAD, rows), rows, own_products, 0)
    for g in range(n):
        distribute(g)
    act[:, 0] = jnp.zeros_like(act[:, 0])
    act[:, rows + 1] = jnp.zeros_like(act[:, 0])

    def clear(r, carry):
        acc[:, r] = jnp.zeros_like(acc[:, r])
        return carry

    lax.fori_loop(0, rows, clear, 0)
    forward(0)

    def w2_share(slot, row_tap):
        ref = band_ref(slot, row_tap, b)
        for hop in range(1, hops):
            peer = lax.rem(b + 2 * hop, nb)
            remote(ref, ref, w2hop_send.at[slot], w2hop_recv.at[slot], {"batch": peer}).start()
        remote(ref, ref, w2pair_send.at[slot], w2pair_recv.at[slot], {"batch": partner}).start()

    def w2_arrive(slot, row_tap):
        ref = band_ref(slot, row_tap, b)
        remote(ref, ref, w2_send.at[0], w2_recv.at[slot, row_tap], {"chan": z}).wait_recv()

    def half_share(row_tap):
        def work(slot):
            w2_arrive(slot, row_tap)
            w2_share(slot, row_tap)

        half_slots(work)

    def w2_chain(row_tap):
        ref = band_ref(more_slot, row_tap, b)
        to = jnp.where(side == 0, lax.rem(z + n - 1, n), lax.rem(z + 1, n))
        return remote(ref, ref, w2_send.at[2], w2_recv.at[more_slot, row_tap], {"chan": to})

    def w2hop_all(slot):
        ref = w2.at[slot, :, :, pl.ds(0, (hops - 1) * band), :]
        return remote(ref, ref, w2hop_send.at[slot], w2hop_recv.at[slot], {"batch": partner})

    def w2pair_all(slot):
        ref = w2.at[slot, :, :, pl.ds(0, hops * band), :]
        return remote(ref, ref, w2pair_send.at[slot], w2pair_recv.at[slot], {"batch": partner})

    def w2_forward(slot):
        w2hop_all(slot).wait_recv()
        for row_tap in range(3):
            for hop in range(1, hops):
                ref = band_ref(slot, row_tap, lax.rem(b + 2 * hop, nb))
                remote(
                    ref, ref, w2pair_send.at[slot], w2pair_recv.at[slot], {"batch": partner}
                ).start()

    def half_slots(work):
        for off in range(1, mids):
            work(half_slot + lax.rem(my_slot - half_slot + off, mids))

    def gb_all():
        ref = gb.at[pl.ds(0, n - 1)]
        return remote(ref, ref, gb_send.at[0], gb_recv.at[0], {"chan": lax.rem(z + 1, n)})

    def finalize(k, value):
        g, r = lax.div(k, rows), lax.rem(k, rows)
        whole[lax.rem(g, 2), r] = value

        @pl.when(r == 0)
        def _():
            shift1[g] = column_sum(value) / height
            sum1[g] = jnp.zeros_like(sum1[g])
            square1[g] = jnp.zeros_like(square1[g])

        moved = value - shift1[g]
        sum1[g] += column_sum(moved)
        square1[g] += column_sum(moved * moved)

    def first_stats(g):
        extra = sum1[g] / local
        stat1[g, b, 0:1, :] = shift1[g] + extra
        stat1[g, b, 1:2, :] = square1[g] - sum1[g] * extra
        stats_send(nb, b, stat1.at[g], st1_send.at[g], st1_recv.at[g])

    def first_affine(g):
        stats_wait(nb, b, stat1.at[g], st1_send.at[g], st1_recv.at[g])
        mean, var = combine(stat1[g], local)
        scale = gb[g, 0:1, :] / jnp.sqrt(var + eps)
        bias = gb[g, 1:2, :]

        def line(r):
            value = (whole[lax.rem(g, 2), r] - mean) * scale + bias
            act[g, r + 1] = jnp.maximum(value, 0.0).astype(bf16)

        return line

    def tap_products(g, t, slot):
        for col_tap in range(3):
            total = None
            for row_tap in range(3):
                window = act[g, pl.ds(t * join + row_tap, join)].reshape(tall, width)
                weight = w2[slot, row_tap, col_tap, pl.ds(pl.multiple_of(g * width, 128), width), :]
                term = jnp.dot(window, weight, preferred_element_type=f32)
                total = term if total is None else total + term
            yield total.reshape(join, height, width)

    def convolve(g, t, slot):
        lines = pl.ds(t * join, join)
        left, middle, right = tap_products(g, t, slot)
        acc[slot, lines, imgs:, :] += left[:, : height - imgs]
        acc[slot, lines] += middle
        acc[slot, lines, : height - imgs, :] += right[:, imgs:]

    def convolve_last(t, slot):
        left, middle, right = tap_products(last, t, slot)
        edge = jnp.zeros((join, imgs, width), f32)
        total = acc[slot, pl.ds(t * join, join)] + middle
        total = total + jnp.concatenate([edge, left[:, : height - imgs]], axis=1)
        total = total + jnp.concatenate([right[:, imgs:], edge], axis=1)
        return total.reshape(tall, width)

    last = n - 1
    all_begin = (last - 1) * rows + SETTLE + 1
    more_begin = all_begin - pieces + 1
    half_begin = SETTLE + 2

    def prepare(s):
        @pl.when(jnp.logical_and(at_last, s == AHEAD // 2))
        def _():
            half_give(2)

        for g in range(1, n):

            @pl.when(s == (g - 1) * (rows // 2) + 2)
            def _():
                forward(g)

        for row_tap in range(3):
            if more:

                @pl.when(s == jnp.where(at_end, OUTER_MORE[row_tap], MORE_CHAIN[row_tap]))
                def _():
                    w2_arrive(more_slot, row_tap)

                    @pl.when(inner)
                    def _():
                        w2_chain(row_tap).start()

                @pl.when(s == jnp.where(at_end, OUTER_MORE[row_tap], INNER_MORE[row_tap]))
                def _():
                    w2_share(more_slot, row_tap)

            @pl.when(s == jnp.where(at_end, OUTER_SHARE[row_tap], INNER_SHARE[row_tap]))
            def _():
                half_share(row_tap)

        for extra in range(2):
            k = 2 * s + extra
            g, r = lax.div(k, rows), lax.rem(k, rows)

            @pl.when(k < chunks)
            def _():
                @pl.when(r == 0)
                def _():
                    complete(g)

                @pl.when(z != g)
                def _():
                    part[k] = jnp.dot(img[r], wown[g], preferred_element_type=f32)

                @pl.when(jnp.logical_and(at_end, jnp.logical_or(at_last, k >= rows)))
                def _():
                    flow[side, k] = part[k].astype(bf16)
                    flow_copy(side, k).start()

    def step(s, carry):
        early = s - early_skew

        @pl.when(jnp.logical_and(inner, jnp.logical_and(early >= 0, early < chunks)))
        def _():
            flow_copy(side, early).wait_recv()
            flow[side, early] = (part[early] + flow[side, early].astype(f32)).astype(bf16)
            flow_copy(side, early).start()

        late = s - late_skew
        after = late - (rows - 1)

        @pl.when(late >= 0)
        def _():
            flow_copy(late_flow, late).wait_recv()
            coming = flow[late_flow, late].astype(f32)

            @pl.when(inner)
            def _():
                flow[late_flow, late] = (part[late] + coming).astype(bf16)
                flow_copy(late_flow, late).start()
                finalize(late, flow[side, late].astype(f32) + coming)

            @pl.when(at_end)
            def _():
                finalize(late, part[late] + coming)

        @pl.when(after == half_begin - 4)
        def _():
            half_slots(w2_forward)

        @pl.when(after == half_begin - 1)
        def _():
            w2_load.wait()
            half_slots(lambda slot: w2pair_all(slot).wait_recv())

        if more:

            @pl.when(after == more_begin - 5)
            def _():
                w2_forward(more_slot)

            @pl.when(after == more_begin - 1)
            def _():
                w2pair_all(more_slot).wait_recv()

        @pl.when(after >= 0)
        def _():
            g, v = lax.div(after, rows), lax.rem(after, rows)

            @pl.when(v == 0)
            def _():
                first_stats(g)

            @pl.when(v == SETTLE)
            def _():
                @pl.when(g == 0)
                def _():
                    gb_all().wait_recv()

                line = first_affine(g)

                def each_line(r, carry):
                    line(r)
                    return carry

                lax.fori_loop(0, rows, each_line, 0)

        item = after - half_begin

        turn = lax.rem(item, rows)

        @pl.when(jnp.logical_and(item >= 0, jnp.logical_and(item < (last - 1) * rows, turn < pieces)))
        def _():
            for i in range(mids):
                convolve(lax.div(item, rows), turn, half_slot + i)

        if more:

            @pl.when(jnp.logical_and(after >= more_begin, after < more_begin + pieces))
            def _():
                for g in range(last - 1):
                    convolve(g, after - more_begin, more_slot)

        since = after - all_begin
        t = lax.div(3 * since + 3, 4)

        @pl.when(jnp.logical_and(since >= 0, jnp.logical_and(t < pieces, lax.div(4 * t, 3) == since)))
        def _():
            for slot in range(slots):
                convolve(last - 1, t, slot)

        return carry

    def first_step(s, carry):
        prepare(s)
        return step(s, carry)

    settled = max(
        chunks // 2, max(OUTER_MORE) + 1, max(INNER_MORE) + 1, (n - 2) * (rows // 2) + 3
    )
    lax.fori_loop(0, settled, first_step, 0)
    lax.fori_loop(settled, chunks + late_skew, step, 0)

    def sec_copy(f, u):
        to = jnp.where(f == 0, lax.rem(z + 1, n), lax.rem(z + n - 1, n))
        t, rest = lax.div(u, per_piece), lax.rem(u, per_piece)
        block = lax.div(rest, join) + f * (mids + more)
        ref = sec.at[block, t * join + lax.rem(rest, join)]
        kind = jnp.where(f == side, 0, 1)
        return remote(ref, ref, sec_send.at[kind], sec_recv.at[u], {"chan": to})

    def sec_start(u, carry):
        sec_copy(side, u).start()
        return carry

    far_block = (1 - side) * (mids + more)
    near_block = side * (mids + more)

    def affine_copy(to, block):
        ref = affine.at[pl.ds(block, lacking)]
        return remote(ref, ref, aff_send.at[to], aff_recv.at[0], {"chan": to})

    def relay(tick):
        u = tick - SKEW * gone

        @pl.when(jnp.logical_and(u >= 0, u < units))
        def _():
            sec_copy(1 - side, u).wait_recv()

            @pl.when(inner)
            def _():
                sec_copy(1 - side, u).start()

    line = first_affine(last)

    def measure(t, slot, fresh):
        total = convolve_last(t, slot)
        if fresh:
            shift2[slot] = column_sum(total) / tall
        moved = total - shift2[slot]
        sums, squares = column_sum(moved), column_sum(moved * moved)
        if fresh:
            sum2[slot] = sums
            square2[slot] = squares
        else:
            sum2[slot] += sums
            square2[slot] += squares
        lines = pl.ds(t * join, join)
        sec[first_block + slot, lines] = moved.astype(bf16).reshape(join, height, width)

    def record(stats, i, slot):
        extra = sum2[slot] / local
        stats[b, i, 0:1, :] = shift2[slot] + extra
        stats[b, i, 1:2, :] = square2[slot] - sum2[slot] * extra

    def derive(stats, base, count):
        mean, var = combine(stats[...], local)
        inverse = 1.0 / jnp.sqrt(var + eps)
        for i in range(count):
            block = first_block + base + i
            scale = gb[block, 2:3, :] * inverse[i]
            affine[block, 0:1, :] = scale
            affine[block, 1:2, :] = (shift2[base + i] - mean[i]) * scale + gb[block, 3:4, :]

    def outgoing(t, fresh):
        for ahead in range(1, join + 1):
            line(jnp.minimum(t * join + ahead, rows - 1))
        for i in range(lacking):
            measure(t, out_slot + i, fresh)

        @pl.when(jnp.logical_and(gone == 0, t < HELD))
        def _():
            lax.fori_loop(t * per_piece, (t + 1) * per_piece, sec_start, 0)

    def outgoing_next(t, carry):
        outgoing(t, False)
        return carry

    line(0)
    outgoing(0, True)
    lax.fori_loop(1, pieces, outgoing_next, 0)
    for i in range(lacking):
        record(stat_out, i, out_slot + i)
    stats_send(nb, b, stat_out, st2_send.at[0], st2_recv.at[0])

    def keeping(t, fresh):
        relay(t)
        for i in range(2 * more):
            measure(t, keep_slot + i, fresh)

    def keeping_next(t, carry):
        keeping(t, False)
        return carry

    begun = max(pieces // 2, 1)
    if more:
        keeping(0, True)
        lax.fori_loop(1, begun, keeping_next, 0)
    stats_wait(nb, b, stat_out, st2_send.at[0], st2_recv.at[0])
    derive(stat_out, out_slot, lacking)

    @pl.when(gone == 0)
    def _():
        for i in range(mids):
            affine_copy((1 - side) * mids + i, near_block).start()
        lax.fori_loop(min(HELD, pieces) * per_piece, units, sec_start, 0)

    part_count = PARTIAL
    if not more or per_piece * PARTIAL > pieces + PARTIAL - SKEW * (mids - 1):
        part_count = 0
    w3_load.wait()
    sum3[...] = jnp.zeros_like(sum3)
    square3[...] = jnp.zeros_like(square3)
    outer_blocks = list(range(lacking)) + list(range(mids + more, n))
    inner_blocks = list(range(lacking, mids + more))

    def product(t, blocks):
        total = None
        while blocks:
            run = [blocks[0]]
            while run[-1] + 1 in blocks:
                run.append(run[-1] + 1)
            blocks = [block for block in blocks if block not in run]
            values = []
            for block in run:
                value = sec[block, pl.ds(t * join, join)].reshape(tall, width).astype(f32)
                value = value * affine[block, 0:1, :] + affine[block, 1:2, :]
                values.append(jnp.maximum(value, 0.0).astype(bf16))
            lines = slice(run[0] * width, (run[-1] + 1) * width)
            term = jnp.dot(
                jnp.concatenate(values, axis=1), w3[lines, :], preferred_element_type=f32
            )
            total = term if total is None else total + term
        return total

    def settle(t, total, fresh):
        if fresh:
            shift3[...] = column_sum(total) / tall
        moved = total - shift3[...]
        third[t] = moved
        sum3[...] += column_sum(moved)
        square3[...] += column_sum(moved * moved)

    def far_affine():
        ref = affine.at[pl.ds(far_block, lacking)]
        return remote(ref, ref, aff_send.at[0], aff_recv.at[0], {"chan": lax.rem(z + 1, n)})

    if more:
        lax.fori_loop(begun, pieces, keeping_next, 0)
        for i in range(2 * more):
            record(stat_keep, i, keep_slot + i)
        stats_send(nb, b, stat_keep, st4_send.at[0], st4_recv.at[0])
        if part_count:
            far_affine().wait_recv()

            def part_step(t, carry):
                relay(pieces + t)
                third[t] = product(t, outer_blocks)
                return carry

            lax.fori_loop(0, part_count, part_step, 0)
        else:
            for tick in range(pieces, pieces + 2):
                relay(tick)
        stats_wait(nb, b, stat_keep, st4_send.at[0], st4_recv.at[0])
        derive(stat_keep, keep_slot, 2 * more)

    lag = SKEW * gone
    relay_first = pieces + (part_count or 2) if more else 0
    if part_count:
        settle(0, third[0] + product(0, inner_blocks), True)

        def rest_step(t, carry):
            settle(t, third[t] + product(t, inner_blocks), False)
            return carry

        lax.fori_loop(1, part_count, rest_step, 0)
    ready = relay_first if part_count else relay_first + 1

    def relay_step(s, carry):
        relay(s)
        if not part_count:

            @pl.when(s == ready)
            def _():
                far_affine().wait_recv()

        t_late = s - ready + part_count
        catching = jnp.logical_and(s >= ready, t_late < pieces)
        catching = jnp.logical_and(catching, per_piece * (t_late + 1) - 1 + lag <= s)
        fresh = s - (per_piece - 1) - lag
        t_fresh = lax.div(fresh, per_piece)
        arriving = jnp.logical_and(fresh >= 0, lax.rem(fresh, per_piece) == 0)
        arriving = jnp.logical_and(arriving, t_fresh < pieces)
        arriving = jnp.logical_and(arriving, ready + t_fresh - part_count < s)
        arriving = jnp.logical_and(arriving, t_fresh >= part_count)
        t = jnp.where(catching, t_late, t_fresh)
        due = jnp.logical_or(catching, arriving)
        if not part_count:

            @pl.when(jnp.logical_and(due, t == 0))
            def _():
                settle(t, product(t, list(range(n))), True)

            due = jnp.logical_and(due, t > 0)

        @pl.when(due)
        def _():
            settle(t, product(t, list(range(n))), False)

        return carry

    relay_last = jnp.maximum(units + lag, ready + pieces - part_count)
    lax.fori_loop(relay_first, relay_last, relay_step, 0)

    extra = sum3[...] / local
    stat3[b, 0:1, :] = shift3[...] + extra
    stat3[b, 1:2, :] = square3[...] - sum3[...] * extra
    stats_send(nb, b, stat3, st3_send.at[0], st3_recv.at[0])

    sent = wown.at[0, pl.ds(0, (n - 1) * strip), :]
    remote(sent, sent, w1_send.at[0], w1_recv.at[0], {"batch": partner}).wait_send()
    gb_all().wait_send()
    for to in range(n):

        @pl.when(z != to)
        def _():
            hop_all(to).wait_send()
            pair_all(to).wait_send()

    w2_sent = w2.at[0, :, :, pl.ds(0, (mids - 1) * band), :]
    right = {"chan": lax.rem(z + 1, n)}
    remote(w2_sent, w2_sent, w2_send.at[0], w2_recv.at[0, 0], right).wait_send()
    half_slots(lambda slot: w2hop_all(slot).wait_send())
    half_slots(lambda slot: w2pair_all(slot).wait_send())
    if more:
        w2_one = w2.at[0, :, :, pl.ds(0, band), :]
        w2hop_all(more_slot).wait_send()
        w2pair_all(more_slot).wait_send()

        @pl.when(inner)
        def _():
            remote(w2_one, w2_one, w2_send.at[2], w2_recv.at[0, 0], right).wait_send()

        @pl.when(gone == 0)
        def _():
            remote(w2_one, w2_one, w2_send.at[1], w2_recv.at[0, 0], right).wait_send()

    for f in range(2):

        @pl.when(z != (n - 1) * (1 - f))
        def _():
            remote(flow.at[f], flow.at[f], flow_send.at[f], flow_recv.at[f, 0], right).wait_send()

    sec_sent = sec.at[pl.ds(0, lacking)]

    @pl.when(gone == 0)
    def _():
        for i in range(mids):
            affine_copy((1 - side) * mids + i, near_block).wait_send()
        remote(sec_sent, sec_sent, sec_send.at[0], sec_recv.at[0], right).wait_send()

    @pl.when(inner)
    def _():
        remote(sec_sent, sec_sent, sec_send.at[1], sec_recv.at[0], right).wait_send()

    stats_wait(nb, b, stat3, st3_send.at[0], st3_recv.at[0])
    mean3, var3 = combine(stat3[...], local)
    scale3 = gain3[...] / jnp.sqrt(var3 + eps)
    offset3 = (shift3[...] - mean3) * scale3 + bias3[...]

    def finish(t, carry):
        kept = img[pl.ds(t * join, join)].reshape(tall, out_local).astype(f32)
        value = third[t] * scale3 + offset3 + kept
        outv[t] = jnp.maximum(value, 0.0).astype(bf16)
        return carry

    lax.fori_loop(0, pieces, finish, 0)


def body(
    images,
    reduce_weight,
    reduce_gain,
    reduce_bias,
    spatial_weight,
    spatial_gain,
    spatial_bias,
    expand_weight,
    expand_gain,
    expand_bias,
):
    imgs, side = (images.shape[0], images.shape[1])
    n, nb = lax.axis_size("chan"), lax.axis_size("batch")
    width = reduce_weight.shape[1]
    depth = images.shape[3]
    out_local = expand_weight.shape[1]
    rows, height = side, side * imgs
    chunks = n * rows
    mid = n * width
    mids = n // 2
    more = EXTRA if mids > 1 else 0
    slots, lacking = mids + more, mids - more
    join = 2 if side % 2 == 0 else 1
    pieces, tall = side // join, height * join
    dma, f32, bf16 = pltpu.SemaphoreType.DMA, jnp.float32, jnp.bfloat16
    vmem = pl.BlockSpec(memory_space=pltpu.VMEM)
    anywhere = pl.BlockSpec(memory_space=pl.ANY)
    flat = images.transpose(1, 2, 0, 3).reshape(rows, height, depth)
    out = pl.pallas_call(
        functools.partial(block_kernel, n, nb, imgs),
        out_shape=pltpu.VMEM((pieces, tall, out_local), bf16),
        in_specs=[anywhere] * 10,
        out_specs=vmem,
        scratch_shapes=[
            pltpu.VMEM((rows, height, depth), bf16),
            pltpu.VMEM(reduce_weight.shape, bf16),
            pltpu.VMEM((n, depth, width), bf16),
            pltpu.VMEM((chunks, height, width), f32),
            pltpu.VMEM((2, rows, height, width), f32),
            pltpu.VMEM((2, chunks, height, width), bf16),
            pltpu.VMEM((n, 4, width), f32),
        ]
        + [pltpu.VMEM((n, 1, width), f32)] * 3
        + [
            pltpu.VMEM((n, nb, 2, width), f32),
            pltpu.VMEM((n, rows + 2, height, width), bf16),
            pltpu.VMEM((slots, 3, 3, mid, width), bf16),
            pltpu.VMEM((slots, rows, height, width), f32),
            pltpu.VMEM((n, rows, height, width), bf16),
        ]
        + [pltpu.VMEM((slots, 1, width), f32)] * 3
        + [
            pltpu.VMEM((nb, lacking, 2, width), f32),
            pltpu.VMEM((nb, 2, 2, width), f32),
            pltpu.VMEM((n, 2, width), f32),
            pltpu.VMEM(expand_weight.shape, bf16),
            pltpu.VMEM((pieces, tall, out_local), f32),
        ]
        + [pltpu.VMEM((1, out_local), f32)] * 3
        + [pltpu.VMEM((nb, 2, out_local), f32)]
        + [pltpu.VMEM((1, width), f32)] * 4
        + [pltpu.VMEM((1, out_local), f32)] * 2
        + [dma((4,)), dma((6,))]
        + [dma((1,))] * 2
        + [dma((1,)), dma((n,))]
        + [dma((n,))] * 4
        + [dma((2,)), dma((2, chunks))]
        + [dma((n,))] * 2
        + [dma((3,)), dma((slots, 3))]
        + [dma((slots,))] * 4
        + [dma((2,)), dma((lacking * rows,))]
        + [dma((1,))] * 4
        + [dma((n,)), dma((1,))]
        + [dma((1,))] * 2,
        compiler_params=pltpu.CompilerParams(
            collective_id=0, has_side_effects=True, vmem_limit_bytes=LIMIT
        ),
        name="block",
    )(
        flat,
        reduce_weight,
        reduce_gain[None, :],
        reduce_bias[None, :],
        spatial_weight,
        spatial_gain[None, :],
        spatial_bias[None, :],
        expand_weight,
        expand_gain[None, :],
        expand_bias[None, :],
    )
    return out.reshape(side, side, imgs, out_local).transpose(2, 0, 1, 3)


def solution(mesh):
    in_specs = (
        P("batch", None, None, "chan"),
        P(None, "chan"),
        P("chan"),
        P("chan"),
        P(None, None, None, "chan"),
        P("chan"),
        P("chan"),
        P(None, "chan"),
        P("chan"),
        P("chan"),
    )
    out_specs = P("batch", None, None, "chan")
    return jax.shard_map(body, mesh=mesh, in_specs=in_specs, out_specs=out_specs, check_vma=False)
```

```python
import functools

import jax
import jax.numpy as jnp
from jax import lax
from jax.experimental import pallas as pl
from jax.experimental.pallas import tpu as pltpu
from jax.sharding import PartitionSpec as P

eps = 0.001
MESH = pl.DeviceIdType.MESH
LIMIT = 59 * 1024 * 1024
SKEW = 3
EXTRA = 1
HELD = 4
SETTLE = 5
AHEAD = 8
PARTIAL = 4
INNER_SHARE = (0, 2, 11)
OUTER_SHARE = (0, 2, 4)
INNER_MORE = (20, 26, 34)
OUTER_MORE = (14, 23, 37)
MORE_CHAIN = (1, 3, 5)


def remote(src, dst, send, recv, device):
    return pltpu.make_async_remote_copy(
        src_ref=src, dst_ref=dst, send_sem=send, recv_sem=recv,
        device_id=device, device_id_type=MESH,
    )


def greet(n, nb, z, b):
    barrier = pltpu.get_barrier_semaphore()
    for off in range(1, n):
        pl.semaphore_signal(
            barrier, inc=1, device_id={"chan": lax.rem(z + off, n)}, device_id_type=MESH
        )
    for off in range(1, nb):
        pl.semaphore_signal(
            barrier, inc=1, device_id={"batch": lax.rem(b + off, nb)}, device_id_type=MESH
        )
    pl.semaphore_wait(barrier, n + nb - 2)


def stats_send(nb, b, stats, send, recv):
    for off in range(1, nb):
        peer = lax.rem(b + off, nb)
        remote(stats.at[b], stats.at[b], send, recv, {"batch": peer}).start()


def stats_wait(nb, b, stats, send, recv):
    others = stats.at[pl.ds(0, nb - 1)]
    remote(others, others, send, recv, {"batch": lax.rem(b + 1, nb)}).wait()


def combine(stats, local):
    nb = stats.shape[0]
    means = stats[..., 0:1, :]
    mean = jnp.sum(means, axis=0) / nb
    away = means - mean[None]
    spread = jnp.sum(stats[..., 1:2, :], axis=0) + local * jnp.sum(away * away, axis=0)
    return mean, spread / (local * nb)


def column_sum(value):
    return jnp.sum(value, axis=0, keepdims=True)


def block_kernel(
    n, nb, imgs,
    img_hbm, w1_hbm, gain1_hbm, bias1_hbm, sw_hbm, gain2_hbm, bias2_hbm, w3_hbm, gain3_hbm, bias3_hbm,
    outv,
    img, w1, wown, part, whole, flow, gb, shift1, sum1, square1, stat1, act, w2, acc, sec,
    shift2, sum2, square2, stat_out, stat_keep, affine, w3, third, shift3, sum3, square3, stat3,
    gain1, bias1, gain2, bias2, gain3, bias3, norm,
    load_sem, small_sem, norm_send, norm_recv,
    gb_send, gb_recv, w1_send, w1_recv, hop_send, hop_recv, pair_send, pair_recv,
    flow_send, flow_recv, st1_send, st1_recv,
    w2_send, w2_recv, w2hop_send, w2hop_recv, w2pair_send, w2pair_recv,
    sec_send, sec_recv, st2_send, st2_recv, st4_send, st4_recv, aff_send, aff_recv, st3_send, st3_recv,
):
    z, b = lax.axis_index("chan"), lax.axis_index("batch")
    rows, height, depth = img.shape
    width = wown.shape[2]
    slots = w2.shape[0]
    pieces, tall, out_local = third.shape
    join = rows // pieces
    mids = n // 2
    more = slots - mids
    lacking = mids - more
    hops = nb // 2
    chunks = n * rows
    strip = depth // nb
    band = n * width // nb
    local = rows * height
    per_piece = lacking * join
    units = lacking * rows
    partner = b + 1 - 2 * lax.rem(b, 2)
    at_first, at_last = z == 0, z == n - 1
    at_end = jnp.logical_or(at_first, at_last)
    inner = jnp.logical_not(at_end)
    side = jnp.where(z < mids, 0, 1)
    gone = jnp.where(z < mids, mids - 1 - z, z - mids)
    first_block = side * (mids - more)
    my_slot = z - first_block
    half_slot = side * more
    more_slot = (1 - side) * mids
    out_slot = side * (slots - lacking)
    keep_slot = (1 - side) * lacking
    late_flow = 1 - side
    late_skew = SKEW * jnp.maximum(z, n - 1 - z)
    early_skew = SKEW * jnp.minimum(z, n - 1 - z)
    f32, bf16 = jnp.float32, jnp.bfloat16

    w1_load = pltpu.make_async_copy(w1_hbm, w1, load_sem.at[0])
    w1_load.start()
    img_load = pltpu.make_async_copy(img_hbm, img, load_sem.at[1])
    img_load.start()
    w3_load = pltpu.make_async_copy(w3_hbm, w3, load_sem.at[2])
    w3_load.start()

    w2_load = pltpu.make_async_copy(sw_hbm, w2.at[my_slot], load_sem.at[3])
    w2_load.start()
    pairs = [
        (gain1_hbm, gain1), (bias1_hbm, bias1), (gain2_hbm, gain2),
        (bias2_hbm, bias2), (gain3_hbm, gain3), (bias3_hbm, bias3),
    ]
    small = [
        pltpu.make_async_copy(src, dst, small_sem.at[i]) for i, (src, dst) in enumerate(pairs)
    ]
    for copy in small:
        copy.start()
    greet(n, nb, z, b)
    for copy in small:
        copy.wait()
    gb[z, 0:1, :] = gain1[...]
    gb[z, 1:2, :] = bias1[...]
    gb[z, 2:3, :] = gain2[...]
    gb[z, 3:4, :] = bias2[...]

    def rows_of(who):
        return pl.ds(pl.multiple_of(who * strip, 16), strip)

    def w1_copy(to):
        src = w1.at[pl.ds(pl.multiple_of(to * depth + b * strip, 16), strip), :]
        return remote(src, wown.at[z, rows_of(b), :], w1_send.at[0], w1_recv.at[z], {"chan": to})

    def gb_copy(to, slot):
        return remote(gb.at[z], gb.at[slot], gb_send.at[0], gb_recv.at[0], {"chan": to})

    def band_of(who):
        return pl.ds(pl.multiple_of(who * band, 16), band)

    w1_load.wait()
    for far in range(n - 1, 0, -1):

        @pl.when(z + far < n)
        def _():
            w1_copy(z + far).start()

        @pl.when(z - far >= 0)
        def _():
            w1_copy(z - far).start()

    for off in range(1, n):
        gb_copy(lax.rem(z + off, n), z).start()

    def band_ref(slot, row_tap, who):
        return w2.at[slot, row_tap, :, band_of(who), :]

    def w2_give(row_tap, to, slot, kind):
        src = sw_hbm.at[row_tap, :, band_of(b), :]
        return remote(
            src, band_ref(slot, row_tap, b), w2_send.at[kind], w2_recv.at[slot, row_tap],
            {"chan": to},
        )

    def half_give(row_tap):
        for off in range(1, mids):
            to = side * mids + lax.rem(z - side * mids + off, mids)
            w2_give(row_tap, to, my_slot, 0).start()

    for row_tap in range(3):
        if more:

            @pl.when(gone == 0)
            def _():
                to = jnp.where(side == 0, mids, mids - 1)
                w2_give(row_tap, to, jnp.where(side == 0, 0, mids), 1).start()

        if row_tap < 2:
            half_give(row_tap)
        else:

            @pl.when(inner)
            def _():
                half_give(row_tap)

    def strip_copy(g, who, send, recv, device):
        ref = wown.at[g, rows_of(who), :]
        return remote(ref, ref, send, recv, device)

    def distribute(g):
        @pl.when(z != g)
        def _():
            strip_copy(g, b, w1_send.at[0], w1_recv.at[g], {"chan": g}).wait_recv()
            for hop in range(1, hops):
                peer = lax.rem(b + 2 * hop, nb)
                strip_copy(g, b, hop_send.at[g], hop_recv.at[g], {"batch": peer}).start()
            strip_copy(g, b, pair_send.at[g], pair_recv.at[g], {"batch": partner}).start()

    def hop_all(g):
        ref = wown.at[g, pl.ds(0, (hops - 1) * strip), :]
        return remote(ref, ref, hop_send.at[g], hop_recv.at[g], {"batch": partner})

    def pair_all(g):
        ref = wown.at[g, pl.ds(0, hops * strip), :]
        return remote(ref, ref, pair_send.at[g], pair_recv.at[g], {"batch": partner})

    def forward(g):
        @pl.when(z != g)
        def _():
            hop_all(g).wait_recv()
            for hop in range(1, hops):
                peer = lax.rem(b + 2 * hop, nb)
                strip_copy(g, peer, pair_send.at[g], pair_recv.at[g], {"batch": partner}).start()

    def complete(g):
        @pl.when(z != g)
        def _():
            pair_all(g).wait_recv()

    def flow_copy(f, k):
        to = jnp.where(f == 0, lax.rem(z + 1, n), lax.rem(z + n - 1, n))
        ref = flow.at[f, k]
        return remote(ref, ref, flow_send.at[f], flow_recv.at[f, k], {"chan": to})

    img_load.wait()

    def own_products(r, carry):
        k = z * rows + r
        value = jnp.dot(
            img[r], w1[pl.ds(pl.multiple_of(z * depth, 16), depth), :], preferred_element_type=f32
        )
        part[k] = value

        @pl.when(at_first)
        def _():
            flow[0, k] = value.astype(bf16)
            flow_copy(0, k).start()

        return carry

    lax.fori_loop(0, min(AHEAD, rows), own_products, 0)

    @pl.when(at_first)
    def _():
        half_give(2)

    lax.fori_loop(min(AHEAD, rows), rows, own_products, 0)
    for g in range(n):
        distribute(g)
    act[:, 0] = jnp.zeros_like(act[:, 0])
    act[:, rows + 1] = jnp.zeros_like(act[:, 0])

    def clear(r, carry):
        acc[:, r] = jnp.zeros_like(acc[:, r])
        return carry

    lax.fori_loop(0, rows, clear, 0)
    forward(0)

    def w2_share(slot, row_tap):
        ref = band_ref(slot, row_tap, b)
        for hop in range(1, hops):
            peer = lax.rem(b + 2 * hop, nb)
            remote(ref, ref, w2hop_send.at[slot], w2hop_recv.at[slot], {"batch": peer}).start()
        remote(ref, ref, w2pair_send.at[slot], w2pair_recv.at[slot], {"batch": partner}).start()

    def w2_arrive(slot, row_tap):
        ref = band_ref(slot, row_tap, b)
        remote(ref, ref, w2_send.at[0], w2_recv.at[slot, row_tap], {"chan": z}).wait_recv()

    def half_share(row_tap):
        def work(slot):
            w2_arrive(slot, row_tap)
            w2_share(slot, row_tap)

        half_slots(work)

    def w2_chain(row_tap):
        ref = band_ref(more_slot, row_tap, b)
        to = jnp.where(side == 0, lax.rem(z + n - 1, n), lax.rem(z + 1, n))
        return remote(ref, ref, w2_send.at[2], w2_recv.at[more_slot, row_tap], {"chan": to})

    def w2hop_all(slot):
        ref = w2.at[slot, :, :, pl.ds(0, (hops - 1) * band), :]
        return remote(ref, ref, w2hop_send.at[slot], w2hop_recv.at[slot], {"batch": partner})

    def w2pair_all(slot):
        ref = w2.at[slot, :, :, pl.ds(0, hops * band), :]
        return remote(ref, ref, w2pair_send.at[slot], w2pair_recv.at[slot], {"batch": partner})

    def w2_forward(slot):
        w2hop_all(slot).wait_recv()
        for row_tap in range(3):
            for hop in range(1, hops):
                ref = band_ref(slot, row_tap, lax.rem(b + 2 * hop, nb))
                remote(
                    ref, ref, w2pair_send.at[slot], w2pair_recv.at[slot], {"batch": partner}
                ).start()

    def half_slots(work):
        for off in range(1, mids):
            work(half_slot + lax.rem(my_slot - half_slot + off, mids))

    def gb_all():
        ref = gb.at[pl.ds(0, n - 1)]
        return remote(ref, ref, gb_send.at[0], gb_recv.at[0], {"chan": lax.rem(z + 1, n)})

    def finalize(k, value):
        g, r = lax.div(k, rows), lax.rem(k, rows)
        whole[lax.rem(g, 2), r] = value

        @pl.when(r == 0)
        def _():
            shift1[g] = column_sum(value) / height
            sum1[g] = jnp.zeros_like(sum1[g])
            square1[g] = jnp.zeros_like(square1[g])

        moved = value - shift1[g]
        sum1[g] += column_sum(moved)
        square1[g] += column_sum(moved * moved)

    def first_stats(g):
        extra = sum1[g] / local
        stat1[g, b, 0:1, :] = shift1[g] + extra
        stat1[g, b, 1:2, :] = square1[g] - sum1[g] * extra
        stats_send(nb, b, stat1.at[g], st1_send.at[g], st1_recv.at[g])

    def first_scale(g, kept):
        stats_wait(nb, b, stat1.at[g], st1_send.at[g], st1_recv.at[g])
        mean, var = combine(stat1[g], local)
        norm[kept, 0:1, :] = mean
        norm[kept, 1:2, :] = gb[g, 0:1, :] / jnp.sqrt(var + eps)

    def first_affine(g, kept):
        mean, scale, bias = norm[kept, 0:1, :], norm[kept, 1:2, :], gb[g, 1:2, :]

        def line(r):
            value = (whole[lax.rem(g, 2), r] - mean) * scale + bias
            act[g, r + 1] = jnp.maximum(value, 0.0).astype(bf16)

        return line

    def tap_products(g, t, slot):
        for col_tap in range(3):
            total = None
            for row_tap in range(3):
                window = act[g, pl.ds(t * join + row_tap, join)].reshape(tall, width)
                weight = w2[slot, row_tap, col_tap, pl.ds(pl.multiple_of(g * width, 128), width), :]
                term = jnp.dot(window, weight, preferred_element_type=f32)
                total = term if total is None else total + term
            yield total.reshape(join, height, width)

    def convolve(g, t, slot):
        lines = pl.ds(t * join, join)
        left, middle, right = tap_products(g, t, slot)
        acc[slot, lines, imgs:, :] += left[:, : height - imgs]
        acc[slot, lines] += middle
        acc[slot, lines, : height - imgs, :] += right[:, imgs:]

    def convolve_last(t, slot):
        left, middle, right = tap_products(last, t, slot)
        edge = jnp.zeros((join, imgs, width), f32)
        total = acc[slot, pl.ds(t * join, join)] + middle
        total = total + jnp.concatenate([edge, left[:, : height - imgs]], axis=1)
        total = total + jnp.concatenate([right[:, imgs:], edge], axis=1)
        return total.reshape(tall, width)

    last = n - 1
    own_last = inner if mids > 1 else z >= 0
    all_begin = last * rows - pieces + 1
    more_begin = all_begin - pieces
    half_begin = SETTLE + 2

    def prepare(s):
        @pl.when(jnp.logical_and(at_last, s == AHEAD // 2))
        def _():
            half_give(2)

        for g in range(1, n):

            @pl.when(s == (g - 1) * (rows // 2) + 2)
            def _():
                forward(g)

        for row_tap in range(3):
            if more:

                @pl.when(s == jnp.where(at_end, OUTER_MORE[row_tap], MORE_CHAIN[row_tap]))
                def _():
                    w2_arrive(more_slot, row_tap)

                    @pl.when(inner)
                    def _():
                        w2_chain(row_tap).start()

                @pl.when(s == jnp.where(at_end, OUTER_MORE[row_tap], INNER_MORE[row_tap]))
                def _():
                    w2_share(more_slot, row_tap)

            @pl.when(s == jnp.where(at_end, OUTER_SHARE[row_tap], INNER_SHARE[row_tap]))
            def _():
                half_share(row_tap)

        for extra in range(2):
            k = 2 * s + extra
            g, r = lax.div(k, rows), lax.rem(k, rows)

            @pl.when(k < chunks)
            def _():
                @pl.when(r == 0)
                def _():
                    complete(g)

                @pl.when(z != g)
                def _():
                    part[k] = jnp.dot(img[r], wown[g], preferred_element_type=f32)

                @pl.when(jnp.logical_and(at_end, jnp.logical_or(at_last, k >= rows)))
                def _():
                    flow[side, k] = part[k].astype(bf16)
                    flow_copy(side, k).start()

    def step(s, carry):
        early = s - early_skew

        @pl.when(jnp.logical_and(inner, jnp.logical_and(early >= 0, early < chunks)))
        def _():
            flow_copy(side, early).wait_recv()
            flow[side, early] = (part[early] + flow[side, early].astype(f32)).astype(bf16)
            flow_copy(side, early).start()

        late = s - late_skew
        after = late - (rows - 1)

        @pl.when(late >= 0)
        def _():
            flow_copy(late_flow, late).wait_recv()
            coming = flow[late_flow, late].astype(f32)

            @pl.when(inner)
            def _():
                flow[late_flow, late] = (part[late] + coming).astype(bf16)
                flow_copy(late_flow, late).start()
                finalize(late, flow[side, late].astype(f32) + coming)

            @pl.when(at_end)
            def _():
                finalize(late, part[late] + coming)

        @pl.when(after == half_begin - 4)
        def _():
            half_slots(w2_forward)

        @pl.when(after == half_begin - 1)
        def _():
            w2_load.wait()
            half_slots(lambda slot: w2pair_all(slot).wait_recv())

        if more:

            @pl.when(after == more_begin - 5)
            def _():
                w2_forward(more_slot)

            @pl.when(after == more_begin - 1)
            def _():
                w2pair_all(more_slot).wait_recv()

        @pl.when(after >= 0)
        def _():
            g, v = lax.div(after, rows), lax.rem(after, rows)

            @pl.when(jnp.logical_and(v == 0, jnp.logical_or(own_last, g < last)))
            def _():
                first_stats(g)

            @pl.when(v == SETTLE)
            def _():
                @pl.when(g == 0)
                def _():
                    gb_all().wait_recv()

                first_scale(g, 0)
                line = first_affine(g, 0)

                def each_line(r, carry):
                    line(r)
                    return carry

                lax.fori_loop(0, rows, each_line, 0)

        item = after - half_begin

        turn = lax.rem(item, rows)

        @pl.when(jnp.logical_and(item >= 0, jnp.logical_and(item < (last - 1) * rows, turn < pieces)))
        def _():
            for i in range(mids):
                convolve(lax.div(item, rows), turn, half_slot + i)

        if more:

            @pl.when(jnp.logical_and(after >= more_begin, after < more_begin + pieces))
            def _():
                for g in range(last - 1):
                    convolve(g, after - more_begin, more_slot)

        @pl.when(after >= all_begin)
        def _():
            for slot in range(slots):
                convolve(last - 1, after - all_begin, slot)

        return carry

    def first_step(s, carry):
        prepare(s)
        return step(s, carry)

    settled = max(
        chunks // 2, max(OUTER_MORE) + 1, max(INNER_MORE) + 1, (n - 2) * (rows // 2) + 3
    )
    lax.fori_loop(0, settled, first_step, 0)
    lax.fori_loop(settled, chunks + late_skew, step, 0)

    def sec_copy(f, u):
        to = jnp.where(f == 0, lax.rem(z + 1, n), lax.rem(z + n - 1, n))
        t, rest = lax.div(u, per_piece), lax.rem(u, per_piece)
        block = lax.div(rest, join) + f * (mids + more)
        ref = sec.at[block, t * join + lax.rem(rest, join)]
        kind = jnp.where(f == side, 0, 1)
        return remote(ref, ref, sec_send.at[kind], sec_recv.at[u], {"chan": to})

    def sec_start(u, carry):
        sec_copy(side, u).start()
        return carry

    far_block = (1 - side) * (mids + more)
    near_block = side * (mids + more)

    def affine_copy(to, block):
        ref = affine.at[pl.ds(block, lacking)]
        return remote(ref, ref, aff_send.at[to], aff_recv.at[0], {"chan": to})

    def relay(tick):
        u = tick - SKEW * gone

        @pl.when(jnp.logical_and(u >= 0, u < units))
        def _():
            sec_copy(1 - side, u).wait_recv()

            @pl.when(inner)
            def _():
                sec_copy(1 - side, u).start()

    to_end = jnp.where(side == 0, 0, n - 1)
    next_to_end = jnp.logical_and(inner, jnp.logical_or(z == 1, z == n - 2))
    norm_copy = remote(norm.at[1], norm.at[1], norm_send.at[0], norm_recv.at[0], {"chan": to_end})

    @pl.when(own_last)
    def _():
        first_scale(last, 1)

    if mids > 1:

        @pl.when(next_to_end)
        def _():
            norm_copy.start()

        @pl.when(at_end)
        def _():
            norm_copy.wait_recv()

    line = first_affine(last, 1)

    def measure(t, slot, fresh):
        total = convolve_last(t, slot)
        if fresh:
            shift2[slot] = column_sum(total) / tall
        moved = total - shift2[slot]
        sums, squares = column_sum(moved), column_sum(moved * moved)
        if fresh:
            sum2[slot] = sums
            square2[slot] = squares
        else:
            sum2[slot] += sums
            square2[slot] += squares
        lines = pl.ds(t * join, join)
        sec[first_block + slot, lines] = moved.astype(bf16).reshape(join, height, width)

    def record(stats, i, slot):
        extra = sum2[slot] / local
        stats[b, i, 0:1, :] = shift2[slot] + extra
        stats[b, i, 1:2, :] = square2[slot] - sum2[slot] * extra

    def derive(stats, base, count):
        mean, var = combine(stats[...], local)
        inverse = 1.0 / jnp.sqrt(var + eps)
        for i in range(count):
            block = first_block + base + i
            scale = gb[block, 2:3, :] * inverse[i]
            affine[block, 0:1, :] = scale
            affine[block, 1:2, :] = (shift2[base + i] - mean[i]) * scale + gb[block, 3:4, :]

    def outgoing(t, fresh):
        for ahead in range(1, join + 1):
            line(jnp.minimum(t * join + ahead, rows - 1))
        for i in range(lacking):
            measure(t, out_slot + i, fresh)

        @pl.when(jnp.logical_and(gone == 0, t < HELD))
        def _():
            lax.fori_loop(t * per_piece, (t + 1) * per_piece, sec_start, 0)

    def outgoing_next(t, carry):
        outgoing(t, False)
        return carry

    line(0)
    outgoing(0, True)
    lax.fori_loop(1, pieces, outgoing_next, 0)
    for i in range(lacking):
        record(stat_out, i, out_slot + i)
    stats_send(nb, b, stat_out, st2_send.at[0], st2_recv.at[0])

    def keeping(t, fresh):
        relay(t)
        for i in range(2 * more):
            measure(t, keep_slot + i, fresh)

    def keeping_next(t, carry):
        keeping(t, False)
        return carry

    begun = max(pieces // 2, 1)
    if more:
        keeping(0, True)
        lax.fori_loop(1, begun, keeping_next, 0)
    def take_out_stats():
        stats_wait(nb, b, stat_out, st2_send.at[0], st2_recv.at[0])
        derive(stat_out, out_slot, lacking)

    @pl.when(gone == 0)
    def _():
        take_out_stats()
        for i in range(mids):
            affine_copy((1 - side) * mids + i, near_block).start()
        lax.fori_loop(min(HELD, pieces) * per_piece, units, sec_start, 0)

    part_count = PARTIAL
    if not more or per_piece * PARTIAL > pieces + PARTIAL - SKEW * (mids - 1):
        part_count = 0
    w3_load.wait()
    sum3[...] = jnp.zeros_like(sum3)
    square3[...] = jnp.zeros_like(square3)
    outer_blocks = list(range(lacking)) + list(range(mids + more, n))
    inner_blocks = list(range(lacking, mids + more))

    def product(t, blocks):
        total = None
        while blocks:
            run = [blocks[0]]
            while run[-1] + 1 in blocks:
                run.append(run[-1] + 1)
            blocks = [block for block in blocks if block not in run]
            values = []
            for block in run:
                value = sec[block, pl.ds(t * join, join)].reshape(tall, width).astype(f32)
                value = value * affine[block, 0:1, :] + affine[block, 1:2, :]
                values.append(jnp.maximum(value, 0.0).astype(bf16))
            lines = slice(run[0] * width, (run[-1] + 1) * width)
            term = jnp.dot(
                jnp.concatenate(values, axis=1), w3[lines, :], preferred_element_type=f32
            )
            total = term if total is None else total + term
        return total

    def settle(t, total, fresh):
        if fresh:
            shift3[...] = column_sum(total) / tall
        moved = total - shift3[...]
        third[t] = moved
        sum3[...] += column_sum(moved)
        square3[...] += column_sum(moved * moved)

    def far_affine():
        ref = affine.at[pl.ds(far_block, lacking)]
        return remote(ref, ref, aff_send.at[0], aff_recv.at[0], {"chan": lax.rem(z + 1, n)})

    if more:
        lax.fori_loop(begun, pieces, keeping_next, 0)
    @pl.when(gone > 0)
    def _():
        take_out_stats()

    if more:
        for i in range(2 * more):
            record(stat_keep, i, keep_slot + i)
        stats_send(nb, b, stat_keep, st4_send.at[0], st4_recv.at[0])
        if part_count:
            far_affine().wait_recv()

            def part_step(t, carry):
                relay(pieces + t)
                third[t] = product(t, outer_blocks)
                return carry

            lax.fori_loop(0, part_count, part_step, 0)
        else:
            for tick in range(pieces, pieces + 2):
                relay(tick)
        stats_wait(nb, b, stat_keep, st4_send.at[0], st4_recv.at[0])
        derive(stat_keep, keep_slot, 2 * more)

    lag = SKEW * gone
    relay_first = pieces + (part_count or 2) if more else 0
    if part_count:

        def rest_relay(t):
            @pl.when(gone == 0)
            def _():
                relay(relay_first + t)

        rest_relay(0)
        settle(0, third[0] + product(0, inner_blocks), True)

        def rest_step(t, carry):
            rest_relay(t)
            settle(t, third[t] + product(t, inner_blocks), False)
            return carry

        lax.fori_loop(1, part_count, rest_step, 0)
    if part_count:
        ready = relay_from = jnp.where(gone == 0, relay_first + part_count, relay_first)
    else:
        ready, relay_from = relay_first + 1, relay_first

    def relay_step(s, carry):
        relay(s)
        if not part_count:

            @pl.when(s == ready)
            def _():
                far_affine().wait_recv()

        t_late = s - ready + part_count
        catching = jnp.logical_and(s >= ready, t_late < pieces)
        catching = jnp.logical_and(catching, per_piece * (t_late + 1) - 1 + lag <= s)
        fresh = s - (per_piece - 1) - lag
        t_fresh = lax.div(fresh, per_piece)
        arriving = jnp.logical_and(fresh >= 0, lax.rem(fresh, per_piece) == 0)
        arriving = jnp.logical_and(arriving, t_fresh < pieces)
        arriving = jnp.logical_and(arriving, ready + t_fresh - part_count < s)
        arriving = jnp.logical_and(arriving, t_fresh >= part_count)
        t = jnp.where(catching, t_late, t_fresh)
        due = jnp.logical_or(catching, arriving)
        if not part_count:

            @pl.when(jnp.logical_and(due, t == 0))
            def _():
                settle(t, product(t, list(range(n))), True)

            due = jnp.logical_and(due, t > 0)

        @pl.when(due)
        def _():
            settle(t, product(t, list(range(n))), False)

        return carry

    relay_last = jnp.maximum(units + lag, ready + pieces - part_count)
    lax.fori_loop(relay_from, relay_last, relay_step, 0)

    extra = sum3[...] / local
    stat3[b, 0:1, :] = shift3[...] + extra
    stat3[b, 1:2, :] = square3[...] - sum3[...] * extra
    stats_send(nb, b, stat3, st3_send.at[0], st3_recv.at[0])

    sent = wown.at[0, pl.ds(0, (n - 1) * strip), :]
    remote(sent, sent, w1_send.at[0], w1_recv.at[0], {"batch": partner}).wait_send()
    gb_all().wait_send()
    for to in range(n):

        @pl.when(z != to)
        def _():
            hop_all(to).wait_send()
            pair_all(to).wait_send()

    w2_sent = w2.at[0, :, :, pl.ds(0, (mids - 1) * band), :]
    right = {"chan": lax.rem(z + 1, n)}
    remote(w2_sent, w2_sent, w2_send.at[0], w2_recv.at[0, 0], right).wait_send()
    half_slots(lambda slot: w2hop_all(slot).wait_send())
    half_slots(lambda slot: w2pair_all(slot).wait_send())
    if more:
        w2_one = w2.at[0, :, :, pl.ds(0, band), :]
        w2hop_all(more_slot).wait_send()
        w2pair_all(more_slot).wait_send()

        @pl.when(inner)
        def _():
            remote(w2_one, w2_one, w2_send.at[2], w2_recv.at[0, 0], right).wait_send()

        @pl.when(gone == 0)
        def _():
            remote(w2_one, w2_one, w2_send.at[1], w2_recv.at[0, 0], right).wait_send()

    for f in range(2):

        @pl.when(z != (n - 1) * (1 - f))
        def _():
            remote(flow.at[f], flow.at[f], flow_send.at[f], flow_recv.at[f, 0], right).wait_send()

    if mids > 1:

        @pl.when(next_to_end)
        def _():
            norm_copy.wait_send()

    sec_sent = sec.at[pl.ds(0, lacking)]

    @pl.when(gone == 0)
    def _():
        for i in range(mids):
            affine_copy((1 - side) * mids + i, near_block).wait_send()
        remote(sec_sent, sec_sent, sec_send.at[0], sec_recv.at[0], right).wait_send()

    @pl.when(inner)
    def _():
        remote(sec_sent, sec_sent, sec_send.at[1], sec_recv.at[0], right).wait_send()

    stats_wait(nb, b, stat3, st3_send.at[0], st3_recv.at[0])
    mean3, var3 = combine(stat3[...], local)
    scale3 = gain3[...] / jnp.sqrt(var3 + eps)
    offset3 = (shift3[...] - mean3) * scale3 + bias3[...]

    def finish(t, carry):
        kept = img[pl.ds(t * join, join)].reshape(tall, out_local).astype(f32)
        value = third[t] * scale3 + offset3 + kept
        outv[t] = jnp.maximum(value, 0.0).astype(bf16)
        return carry

    lax.fori_loop(0, pieces, finish, 0)


def body(
    images,
    reduce_weight,
    reduce_gain,
    reduce_bias,
    spatial_weight,
    spatial_gain,
    spatial_bias,
    expand_weight,
    expand_gain,
    expand_bias,
):
    imgs, side = (images.shape[0], images.shape[1])
    n, nb = lax.axis_size("chan"), lax.axis_size("batch")
    width = reduce_weight.shape[1]
    depth = images.shape[3]
    out_local = expand_weight.shape[1]
    rows, height = side, side * imgs
    chunks = n * rows
    mid = n * width
    mids = n // 2
    more = EXTRA if mids > 1 else 0
    slots, lacking = mids + more, mids - more
    join = 2 if side % 2 == 0 else 1
    pieces, tall = side // join, height * join
    dma, f32, bf16 = pltpu.SemaphoreType.DMA, jnp.float32, jnp.bfloat16
    vmem = pl.BlockSpec(memory_space=pltpu.VMEM)
    anywhere = pl.BlockSpec(memory_space=pl.ANY)
    flat = images.transpose(1, 2, 0, 3).reshape(rows, height, depth)
    out = pl.pallas_call(
        functools.partial(block_kernel, n, nb, imgs),
        out_shape=pltpu.VMEM((pieces, tall, out_local), bf16),
        in_specs=[anywhere] * 10,
        out_specs=vmem,
        scratch_shapes=[
            pltpu.VMEM((rows, height, depth), bf16),
            pltpu.VMEM(reduce_weight.shape, bf16),
            pltpu.VMEM((n, depth, width), bf16),
            pltpu.VMEM((chunks, height, width), f32),
            pltpu.VMEM((2, rows, height, width), f32),
            pltpu.VMEM((2, chunks, height, width), bf16),
            pltpu.VMEM((n, 4, width), f32),
        ]
        + [pltpu.VMEM((n, 1, width), f32)] * 3
        + [
            pltpu.VMEM((n, nb, 2, width), f32),
            pltpu.VMEM((n, rows + 2, height, width), bf16),
            pltpu.VMEM((slots, 3, 3, mid, width), bf16),
            pltpu.VMEM((slots, rows, height, width), f32),
            pltpu.VMEM((n, rows, height, width), bf16),
        ]
        + [pltpu.VMEM((slots, 1, width), f32)] * 3
        + [
            pltpu.VMEM((nb, lacking, 2, width), f32),
            pltpu.VMEM((nb, 2, 2, width), f32),
            pltpu.VMEM((n, 2, width), f32),
            pltpu.VMEM(expand_weight.shape, bf16),
            pltpu.VMEM((pieces, tall, out_local), f32),
        ]
        + [pltpu.VMEM((1, out_local), f32)] * 3
        + [pltpu.VMEM((nb, 2, out_local), f32)]
        + [pltpu.VMEM((1, width), f32)] * 4
        + [pltpu.VMEM((1, out_local), f32)] * 2
        + [pltpu.VMEM((2, 2, width), f32)]
        + [dma((4,)), dma((6,)), dma((1,)), dma((1,))]
        + [dma((1,))] * 2
        + [dma((1,)), dma((n,))]
        + [dma((n,))] * 4
        + [dma((2,)), dma((2, chunks))]
        + [dma((n,))] * 2
        + [dma((3,)), dma((slots, 3))]
        + [dma((slots,))] * 4
        + [dma((2,)), dma((lacking * rows,))]
        + [dma((1,))] * 4
        + [dma((n,)), dma((1,))]
        + [dma((1,))] * 2,
        compiler_params=pltpu.CompilerParams(
            collective_id=0, has_side_effects=True, vmem_limit_bytes=LIMIT
        ),
        name="block",
    )(
        flat,
        reduce_weight,
        reduce_gain[None, :],
        reduce_bias[None, :],
        spatial_weight,
        spatial_gain[None, :],
        spatial_bias[None, :],
        expand_weight,
        expand_gain[None, :],
        expand_bias[None, :],
    )
    return out.reshape(side, side, imgs, out_local).transpose(2, 0, 1, 3)


def solution(mesh):
    in_specs = (
        P("batch", None, None, "chan"),
        P(None, "chan"),
        P("chan"),
        P("chan"),
        P(None, None, None, "chan"),
        P("chan"),
        P("chan"),
        P(None, "chan"),
        P("chan"),
        P("chan"),
    )
    out_specs = P("batch", None, None, "chan")
    return jax.shard_map(body, mesh=mesh, in_specs=in_specs, out_specs=out_specs, check_vma=False)
```

```python
import functools

import jax
import jax.numpy as jnp
from jax import lax
from jax.experimental import pallas as pl
from jax.experimental.pallas import tpu as pltpu
from jax.sharding import PartitionSpec as P

eps = 0.001
MESH = pl.DeviceIdType.MESH
LIMIT = 59 * 1024 * 1024
SKEW = 3
EXTRA = 1
HELD = 4
SETTLE = 5
AHEAD = 8
PARTIAL = 4
INNER_SHARE = (0, 2, 11)
OUTER_SHARE = (0, 2, 4)
INNER_MORE = (20, 26, 34)
OUTER_MORE = (14, 23, 37)
MORE_CHAIN = (1, 3, 5)


def remote(src, dst, send, recv, device):
    return pltpu.make_async_remote_copy(
        src_ref=src, dst_ref=dst, send_sem=send, recv_sem=recv,
        device_id=device, device_id_type=MESH,
    )


def greet(n, nb, z, b):
    barrier = pltpu.get_barrier_semaphore()
    for off in range(1, n):
        pl.semaphore_signal(
            barrier, inc=1, device_id={"chan": lax.rem(z + off, n)}, device_id_type=MESH
        )
    for off in range(1, nb):
        pl.semaphore_signal(
            barrier, inc=1, device_id={"batch": lax.rem(b + off, nb)}, device_id_type=MESH
        )
    pl.semaphore_wait(barrier, n + nb - 2)


def stats_send(nb, b, stats, send, recv):
    for off in range(1, nb):
        peer = lax.rem(b + off, nb)
        remote(stats.at[b], stats.at[b], send, recv, {"batch": peer}).start()


def stats_wait(nb, b, stats, send, recv):
    others = stats.at[pl.ds(0, nb - 1)]
    remote(others, others, send, recv, {"batch": lax.rem(b + 1, nb)}).wait()


def combine(stats, local):
    nb = stats.shape[0]
    means = stats[..., 0:1, :]
    mean = jnp.sum(means, axis=0) / nb
    away = means - mean[None]
    spread = jnp.sum(stats[..., 1:2, :], axis=0) + local * jnp.sum(away * away, axis=0)
    return mean, spread / (local * nb)


def column_sum(value):
    return jnp.sum(value, axis=0, keepdims=True)


def block_kernel(
    n, nb, imgs,
    img_hbm, w1_hbm, gain1_hbm, bias1_hbm, sw_hbm, gain2_hbm, bias2_hbm, w3_hbm, gain3_hbm, bias3_hbm,
    outv,
    img, w1, wown, part, whole, flow, gb, shift1, sum1, square1, stat1, act, w2, acc, sec,
    shift2, sum2, square2, stat_out, stat_keep, affine, w3, third, shift3, sum3, square3, stat3,
    gain1, bias1, gain2, bias2, gain3, bias3, norm,
    load_sem, small_sem, norm_send, norm_recv,
    gb_send, gb_recv, w1_send, w1_recv, hop_send, hop_recv, pair_send, pair_recv,
    flow_send, flow_recv, st1_send, st1_recv,
    w2_send, w2_recv, w2hop_send, w2hop_recv, w2pair_send, w2pair_recv,
    sec_send, sec_recv, st2_send, st2_recv, st4_send, st4_recv, aff_send, aff_recv, st3_send, st3_recv,
):
    z, b = lax.axis_index("chan"), lax.axis_index("batch")
    rows, height, depth = img.shape
    width = wown.shape[2]
    slots = w2.shape[0]
    pieces, tall, out_local = third.shape
    join = rows // pieces
    mids = n // 2
    more = slots - mids
    lacking = mids - more
    hops = nb // 2
    chunks = n * rows
    strip = depth // nb
    band = n * width // nb
    local = rows * height
    per_piece = lacking * join
    units = lacking * rows
    partner = b + 1 - 2 * lax.rem(b, 2)
    at_first, at_last = z == 0, z == n - 1
    at_end = jnp.logical_or(at_first, at_last)
    inner = jnp.logical_not(at_end)
    side = jnp.where(z < mids, 0, 1)
    gone = jnp.where(z < mids, mids - 1 - z, z - mids)
    first_block = side * (mids - more)
    my_slot = z - first_block
    half_slot = side * more
    more_slot = (1 - side) * mids
    out_slot = side * (slots - lacking)
    keep_slot = (1 - side) * lacking
    late_flow = 1 - side
    late_skew = SKEW * jnp.maximum(z, n - 1 - z)
    early_skew = SKEW * jnp.minimum(z, n - 1 - z)
    f32, bf16 = jnp.float32, jnp.bfloat16

    w1_load = pltpu.make_async_copy(w1_hbm, w1, load_sem.at[0])
    w1_load.start()
    img_load = pltpu.make_async_copy(img_hbm, img, load_sem.at[1])
    img_load.start()
    w3_load = pltpu.make_async_copy(w3_hbm, w3, load_sem.at[2])
    w3_load.start()

    w2_load = pltpu.make_async_copy(sw_hbm, w2.at[my_slot], load_sem.at[3])
    w2_load.start()
    pairs = [
        (gain1_hbm, gain1), (bias1_hbm, bias1), (gain2_hbm, gain2),
        (bias2_hbm, bias2), (gain3_hbm, gain3), (bias3_hbm, bias3),
    ]
    small = [
        pltpu.make_async_copy(src, dst, small_sem.at[i]) for i, (src, dst) in enumerate(pairs)
    ]
    for copy in small:
        copy.start()
    greet(n, nb, z, b)
    for copy in small:
        copy.wait()
    gb[z, 0:1, :] = gain1[...]
    gb[z, 1:2, :] = bias1[...]
    gb[z, 2:3, :] = gain2[...]
    gb[z, 3:4, :] = bias2[...]

    def rows_of(who):
        return pl.ds(pl.multiple_of(who * strip, 16), strip)

    def w1_copy(to):
        src = w1.at[pl.ds(pl.multiple_of(to * depth + b * strip, 16), strip), :]
        return remote(src, wown.at[z, rows_of(b), :], w1_send.at[0], w1_recv.at[z], {"chan": to})

    def gb_copy(to, slot):
        return remote(gb.at[z], gb.at[slot], gb_send.at[0], gb_recv.at[0], {"chan": to})

    def band_of(who):
        return pl.ds(pl.multiple_of(who * band, 16), band)

    w1_load.wait()
    for far in range(n - 1, 0, -1):

        @pl.when(z + far < n)
        def _():
            w1_copy(z + far).start()

        @pl.when(z - far >= 0)
        def _():
            w1_copy(z - far).start()

    for off in range(1, n):
        gb_copy(lax.rem(z + off, n), z).start()

    def band_ref(slot, row_tap, who):
        return w2.at[slot, row_tap, :, band_of(who), :]

    def w2_give(row_tap, to, slot, kind):
        src = sw_hbm.at[row_tap, :, band_of(b), :]
        return remote(
            src, band_ref(slot, row_tap, b), w2_send.at[kind], w2_recv.at[slot, row_tap],
            {"chan": to},
        )

    def half_give(row_tap):
        for off in range(1, mids):
            to = side * mids + lax.rem(z - side * mids + off, mids)
            w2_give(row_tap, to, my_slot, 0).start()

    for row_tap in range(3):
        if more:

            @pl.when(gone == 0)
            def _():
                to = jnp.where(side == 0, mids, mids - 1)
                w2_give(row_tap, to, jnp.where(side == 0, 0, mids), 1).start()

        if row_tap < 2:
            half_give(row_tap)
        else:

            @pl.when(inner)
            def _():
                half_give(row_tap)

    def strip_copy(g, who, send, recv, device):
        ref = wown.at[g, rows_of(who), :]
        return remote(ref, ref, send, recv, device)

    def distribute(g):
        @pl.when(z != g)
        def _():
            strip_copy(g, b, w1_send.at[0], w1_recv.at[g], {"chan": g}).wait_recv()
            for hop in range(1, hops):
                peer = lax.rem(b + 2 * hop, nb)
                strip_copy(g, b, hop_send.at[g], hop_recv.at[g], {"batch": peer}).start()
            strip_copy(g, b, pair_send.at[g], pair_recv.at[g], {"batch": partner}).start()

    def hop_all(g):
        ref = wown.at[g, pl.ds(0, (hops - 1) * strip), :]
        return remote(ref, ref, hop_send.at[g], hop_recv.at[g], {"batch": partner})

    def pair_all(g):
        ref = wown.at[g, pl.ds(0, hops * strip), :]
        return remote(ref, ref, pair_send.at[g], pair_recv.at[g], {"batch": partner})

    def forward(g):
        @pl.when(z != g)
        def _():
            hop_all(g).wait_recv()
            for hop in range(1, hops):
                peer = lax.rem(b + 2 * hop, nb)
                strip_copy(g, peer, pair_send.at[g], pair_recv.at[g], {"batch": partner}).start()

    def complete(g):
        @pl.when(z != g)
        def _():
            pair_all(g).wait_recv()

    def flow_copy(f, k):
        to = jnp.where(f == 0, lax.rem(z + 1, n), lax.rem(z + n - 1, n))
        ref = flow.at[f, k]
        return remote(ref, ref, flow_send.at[f], flow_recv.at[f, k], {"chan": to})

    img_load.wait()

    def own_products(r, carry):
        k = z * rows + r
        value = jnp.dot(
            img[r], w1[pl.ds(pl.multiple_of(z * depth, 16), depth), :], preferred_element_type=f32
        )
        part[k] = value

        @pl.when(at_first)
        def _():
            flow[0, k] = value.astype(bf16)
            flow_copy(0, k).start()

        return carry

    lax.fori_loop(0, min(AHEAD, rows), own_products, 0)

    @pl.when(at_first)
    def _():
        half_give(2)

    lax.fori_loop(min(AHEAD, rows), rows, own_products, 0)
    for g in range(n):
        distribute(g)
    act[:, 0] = jnp.zeros_like(act[:, 0])
    act[:, rows + 1] = jnp.zeros_like(act[:, 0])

    def clear(r, carry):
        acc[:, r] = jnp.zeros_like(acc[:, r])
        return carry

    lax.fori_loop(0, rows, clear, 0)
    forward(0)

    def w2_share(slot, row_tap):
        ref = band_ref(slot, row_tap, b)
        for hop in range(1, hops):
            peer = lax.rem(b + 2 * hop, nb)
            remote(ref, ref, w2hop_send.at[slot], w2hop_recv.at[slot], {"batch": peer}).start()
        remote(ref, ref, w2pair_send.at[slot], w2pair_recv.at[slot], {"batch": partner}).start()

    def w2_arrive(slot, row_tap):
        ref = band_ref(slot, row_tap, b)
        remote(ref, ref, w2_send.at[0], w2_recv.at[slot, row_tap], {"chan": z}).wait_recv()

    def half_share(row_tap):
        def work(slot):
            w2_arrive(slot, row_tap)
            w2_share(slot, row_tap)

        half_slots(work)

    def w2_chain(row_tap):
        ref = band_ref(more_slot, row_tap, b)
        to = jnp.where(side == 0, lax.rem(z + n - 1, n), lax.rem(z + 1, n))
        return remote(ref, ref, w2_send.at[2], w2_recv.at[more_slot, row_tap], {"chan": to})

    def w2hop_all(slot):
        ref = w2.at[slot, :, :, pl.ds(0, (hops - 1) * band), :]
        return remote(ref, ref, w2hop_send.at[slot], w2hop_recv.at[slot], {"batch": partner})

    def w2pair_all(slot):
        ref = w2.at[slot, :, :, pl.ds(0, hops * band), :]
        return remote(ref, ref, w2pair_send.at[slot], w2pair_recv.at[slot], {"batch": partner})

    def w2_forward(slot):
        w2hop_all(slot).wait_recv()
        for row_tap in range(3):
            for hop in range(1, hops):
                ref = band_ref(slot, row_tap, lax.rem(b + 2 * hop, nb))
                remote(
                    ref, ref, w2pair_send.at[slot], w2pair_recv.at[slot], {"batch": partner}
                ).start()

    def half_slots(work):
        for off in range(1, mids):
            work(half_slot + lax.rem(my_slot - half_slot + off, mids))

    def gb_all():
        ref = gb.at[pl.ds(0, n - 1)]
        return remote(ref, ref, gb_send.at[0], gb_recv.at[0], {"chan": lax.rem(z + 1, n)})

    def finalize(k, value):
        g, r = lax.div(k, rows), lax.rem(k, rows)
        whole[lax.rem(g, 2), r] = value

        @pl.when(r == 0)
        def _():
            shift1[g] = column_sum(value) / height
            sum1[g] = jnp.zeros_like(sum1[g])
            square1[g] = jnp.zeros_like(square1[g])

        moved = value - shift1[g]
        sum1[g] += column_sum(moved)
        square1[g] += column_sum(moved * moved)

    def first_stats(g):
        extra = sum1[g] / local
        stat1[g, b, 0:1, :] = shift1[g] + extra
        stat1[g, b, 1:2, :] = square1[g] - sum1[g] * extra
        stats_send(nb, b, stat1.at[g], st1_send.at[g], st1_recv.at[g])

    def first_scale(g, kept):
        stats_wait(nb, b, stat1.at[g], st1_send.at[g], st1_recv.at[g])
        mean, var = combine(stat1[g], local)
        norm[kept, 0:1, :] = mean
        norm[kept, 1:2, :] = gb[g, 0:1, :] / jnp.sqrt(var + eps)

    def first_affine(g, kept):
        mean, scale, bias = norm[kept, 0:1, :], norm[kept, 1:2, :], gb[g, 1:2, :]

        def line(r):
            value = (whole[lax.rem(g, 2), r] - mean) * scale + bias
            act[g, r + 1] = jnp.maximum(value, 0.0).astype(bf16)

        return line

    def tap_products(g, t, slot):
        for col_tap in range(3):
            total = None
            for row_tap in range(3):
                window = act[g, pl.ds(t * join + row_tap, join)].reshape(tall, width)
                weight = w2[slot, row_tap, col_tap, pl.ds(pl.multiple_of(g * width, 128), width), :]
                term = jnp.dot(window, weight, preferred_element_type=f32)
                total = term if total is None else total + term
            yield total.reshape(join, height, width)

    def convolve(g, t, slot):
        lines = pl.ds(t * join, join)
        left, middle, right = tap_products(g, t, slot)
        acc[slot, lines, imgs:, :] += left[:, : height - imgs]
        acc[slot, lines] += middle
        acc[slot, lines, : height - imgs, :] += right[:, imgs:]

    def convolve_last(t, slot):
        left, middle, right = tap_products(last, t, slot)
        edge = jnp.zeros((join, imgs, width), f32)
        total = acc[slot, pl.ds(t * join, join)] + middle
        total = total + jnp.concatenate([edge, left[:, : height - imgs]], axis=1)
        total = total + jnp.concatenate([right[:, imgs:], edge], axis=1)
        return total.reshape(tall, width)

    last = n - 1
    own_last = inner if mids > 1 else z >= 0
    all_begin = last * rows - pieces + 1
    more_begin = all_begin - pieces
    half_begin = SETTLE + 2

    def prepare(s):
        @pl.when(jnp.logical_and(at_last, s == AHEAD // 2))
        def _():
            half_give(2)

        for g in range(1, n):

            @pl.when(s == (g - 1) * (rows // 2) + 2)
            def _():
                forward(g)

        for row_tap in range(3):
            if more:

                @pl.when(s == jnp.where(at_end, OUTER_MORE[row_tap], MORE_CHAIN[row_tap]))
                def _():
                    w2_arrive(more_slot, row_tap)

                    @pl.when(inner)
                    def _():
                        w2_chain(row_tap).start()

                @pl.when(s == jnp.where(at_end, OUTER_MORE[row_tap], INNER_MORE[row_tap]))
                def _():
                    w2_share(more_slot, row_tap)

            @pl.when(s == jnp.where(at_end, OUTER_SHARE[row_tap], INNER_SHARE[row_tap]))
            def _():
                half_share(row_tap)

        for extra in range(2):
            k = 2 * s + extra
            g, r = lax.div(k, rows), lax.rem(k, rows)

            @pl.when(k < chunks)
            def _():
                @pl.when(r == 0)
                def _():
                    complete(g)

                @pl.when(z != g)
                def _():
                    part[k] = jnp.dot(img[r], wown[g], preferred_element_type=f32)

                @pl.when(jnp.logical_and(at_end, jnp.logical_or(at_last, k >= rows)))
                def _():
                    flow[side, k] = part[k].astype(bf16)
                    flow_copy(side, k).start()

    def step(s, carry):
        early = s - early_skew

        @pl.when(jnp.logical_and(inner, jnp.logical_and(early >= 0, early < chunks)))
        def _():
            flow_copy(side, early).wait_recv()
            flow[side, early] = (part[early] + flow[side, early].astype(f32)).astype(bf16)
            flow_copy(side, early).start()

        late = s - late_skew
        after = late - (rows - 1)

        @pl.when(late >= 0)
        def _():
            flow_copy(late_flow, late).wait_recv()
            coming = flow[late_flow, late].astype(f32)

            @pl.when(inner)
            def _():
                flow[late_flow, late] = (part[late] + coming).astype(bf16)
                flow_copy(late_flow, late).start()
                finalize(late, flow[side, late].astype(f32) + coming)

            @pl.when(at_end)
            def _():
                finalize(late, part[late] + coming)

        @pl.when(after == half_begin - 4)
        def _():
            half_slots(w2_forward)

        @pl.when(after == half_begin - 1)
        def _():
            w2_load.wait()
            half_slots(lambda slot: w2pair_all(slot).wait_recv())

        if more:

            @pl.when(after == more_begin - 5)
            def _():
                w2_forward(more_slot)

            @pl.when(after == more_begin - 1)
            def _():
                w2pair_all(more_slot).wait_recv()

        @pl.when(after >= 0)
        def _():
            g, v = lax.div(after, rows), lax.rem(after, rows)

            @pl.when(jnp.logical_and(v == 0, jnp.logical_or(own_last, g < last)))
            def _():
                first_stats(g)

            @pl.when(v == SETTLE)
            def _():
                @pl.when(g == 0)
                def _():
                    gb_all().wait_recv()

                first_scale(g, 0)
                line = first_affine(g, 0)

                def each_line(r, carry):
                    line(r)
                    return carry

                lax.fori_loop(0, rows, each_line, 0)

        item = after - half_begin

        turn = lax.rem(item, rows)

        @pl.when(jnp.logical_and(item >= 0, jnp.logical_and(item < (last - 1) * rows, turn < pieces)))
        def _():
            for i in range(mids):
                convolve(lax.div(item, rows), turn, half_slot + i)

        if more:

            @pl.when(jnp.logical_and(after >= more_begin, after < more_begin + pieces))
            def _():
                for g in range(last - 1):
                    convolve(g, after - more_begin, more_slot)

        @pl.when(after >= all_begin)
        def _():
            for slot in range(slots):
                convolve(last - 1, after - all_begin, slot)

        return carry

    def first_step(s, carry):
        prepare(s)
        return step(s, carry)

    settled = max(
        chunks // 2, max(OUTER_MORE) + 1, max(INNER_MORE) + 1, (n - 2) * (rows // 2) + 3
    )
    lax.fori_loop(0, settled, first_step, 0)
    lax.fori_loop(settled, chunks + late_skew, step, 0)

    halves = 2 if width % 256 == 0 else 1
    thin = width // halves

    def sec_copy(f, u, part_of):
        to = jnp.where(f == 0, lax.rem(z + 1, n), lax.rem(z + n - 1, n))
        t, rest = lax.div(u, per_piece), lax.rem(u, per_piece)
        block = lax.div(rest, join) + f * (mids + more)
        ref = sec.at[block, t * join + lax.rem(rest, join), :, pl.ds(part_of * thin, thin)]
        kind = jnp.where(f == side, 0, 1)
        return remote(ref, ref, sec_send.at[kind], sec_recv.at[u, part_of], {"chan": to})

    def sec_start(u, carry):
        for part_of in range(halves):
            sec_copy(side, u, part_of).start()
        return carry

    far_block = (1 - side) * (mids + more)
    near_block = side * (mids + more)

    def affine_copy(to, block):
        ref = affine.at[pl.ds(block, lacking)]
        return remote(ref, ref, aff_send.at[to], aff_recv.at[0], {"chan": to})

    def relay(tick):
        u = tick - SKEW * gone

        @pl.when(jnp.logical_and(u >= 0, u < units))
        def _():
            for part_of in range(halves):
                coming = sec_copy(1 - side, u, part_of)
                coming.wait_recv()
                pl.when(inner)(coming.start)

    to_end = jnp.where(side == 0, 0, n - 1)
    next_to_end = jnp.logical_and(inner, jnp.logical_or(z == 1, z == n - 2))
    norm_copy = remote(norm.at[1], norm.at[1], norm_send.at[0], norm_recv.at[0], {"chan": to_end})

    @pl.when(own_last)
    def _():
        first_scale(last, 1)

    if mids > 1:

        @pl.when(next_to_end)
        def _():
            norm_copy.start()

        @pl.when(at_end)
        def _():
            norm_copy.wait_recv()

    line = first_affine(last, 1)

    def measure(t, slot, fresh):
        total = convolve_last(t, slot)
        if fresh:
            shift2[slot] = column_sum(total) / tall
        moved = total - shift2[slot]
        sums, squares = column_sum(moved), column_sum(moved * moved)
        if fresh:
            sum2[slot] = sums
            square2[slot] = squares
        else:
            sum2[slot] += sums
            square2[slot] += squares
        lines = pl.ds(t * join, join)
        sec[first_block + slot, lines] = moved.astype(bf16).reshape(join, height, width)

    def record(stats, i, slot):
        extra = sum2[slot] / local
        stats[b, i, 0:1, :] = shift2[slot] + extra
        stats[b, i, 1:2, :] = square2[slot] - sum2[slot] * extra

    def derive(stats, base, count):
        mean, var = combine(stats[...], local)
        inverse = 1.0 / jnp.sqrt(var + eps)
        for i in range(count):
            block = first_block + base + i
            scale = gb[block, 2:3, :] * inverse[i]
            affine[block, 0:1, :] = scale
            affine[block, 1:2, :] = (shift2[base + i] - mean[i]) * scale + gb[block, 3:4, :]

    def outgoing(t, fresh):
        for ahead in range(1, join + 1):
            line(jnp.minimum(t * join + ahead, rows - 1))
        for i in range(lacking):
            measure(t, out_slot + i, fresh)

        @pl.when(jnp.logical_and(gone == 0, t < HELD))
        def _():
            lax.fori_loop(t * per_piece, (t + 1) * per_piece, sec_start, 0)

    def outgoing_next(t, carry):
        outgoing(t, False)
        return carry

    line(0)
    outgoing(0, True)
    lax.fori_loop(1, pieces, outgoing_next, 0)
    for i in range(lacking):
        record(stat_out, i, out_slot + i)
    stats_send(nb, b, stat_out, st2_send.at[0], st2_recv.at[0])

    def keeping(t, fresh):
        relay(t)
        for i in range(2 * more):
            measure(t, keep_slot + i, fresh)

    def keeping_next(t, carry):
        keeping(t, False)
        return carry

    begun = max(pieces // 2, 1)
    if more:
        keeping(0, True)
        lax.fori_loop(1, begun, keeping_next, 0)
    def take_out_stats():
        stats_wait(nb, b, stat_out, st2_send.at[0], st2_recv.at[0])
        derive(stat_out, out_slot, lacking)

    @pl.when(gone == 0)
    def _():
        take_out_stats()
        for i in range(mids):
            affine_copy((1 - side) * mids + i, near_block).start()
        lax.fori_loop(min(HELD, pieces) * per_piece, units, sec_start, 0)

    part_count = PARTIAL
    if not more or per_piece * PARTIAL > pieces + PARTIAL - SKEW * (mids - 1):
        part_count = 0
    w3_load.wait()
    sum3[...] = jnp.zeros_like(sum3)
    square3[...] = jnp.zeros_like(square3)
    outer_blocks = list(range(lacking)) + list(range(mids + more, n))
    inner_blocks = list(range(lacking, mids + more))

    def product(t, blocks):
        total = None
        while blocks:
            run = [blocks[0]]
            while run[-1] + 1 in blocks:
                run.append(run[-1] + 1)
            blocks = [block for block in blocks if block not in run]
            values = []
            for block in run:
                value = sec[block, pl.ds(t * join, join)].reshape(tall, width).astype(f32)
                value = value * affine[block, 0:1, :] + affine[block, 1:2, :]
                values.append(jnp.maximum(value, 0.0).astype(bf16))
            lines = slice(run[0] * width, (run[-1] + 1) * width)
            term = jnp.dot(
                jnp.concatenate(values, axis=1), w3[lines, :], preferred_element_type=f32
            )
            total = term if total is None else total + term
        return total

    def settle(t, total, fresh):
        if fresh:
            shift3[...] = column_sum(total) / tall
        moved = total - shift3[...]
        third[t] = moved
        sum3[...] += column_sum(moved)
        square3[...] += column_sum(moved * moved)

    def far_affine():
        ref = affine.at[pl.ds(far_block, lacking)]
        return remote(ref, ref, aff_send.at[0], aff_recv.at[0], {"chan": lax.rem(z + 1, n)})

    if more:
        lax.fori_loop(begun, pieces, keeping_next, 0)
    @pl.when(gone > 0)
    def _():
        take_out_stats()

    if more:
        for i in range(2 * more):
            record(stat_keep, i, keep_slot + i)
        stats_send(nb, b, stat_keep, st4_send.at[0], st4_recv.at[0])
        if part_count:
            far_affine().wait_recv()

            def part_step(t, carry):
                relay(pieces + t)
                third[t] = product(t, outer_blocks)
                return carry

            lax.fori_loop(0, part_count, part_step, 0)
        else:
            for tick in range(pieces, pieces + 2):
                relay(tick)
        stats_wait(nb, b, stat_keep, st4_send.at[0], st4_recv.at[0])
        derive(stat_keep, keep_slot, 2 * more)

    lag = SKEW * gone
    relay_first = pieces + (part_count or 2) if more else 0
    if part_count:

        def rest_relay(t):
            @pl.when(gone == 0)
            def _():
                relay(relay_first + t)

        rest_relay(0)
        settle(0, third[0] + product(0, inner_blocks), True)

        def rest_step(t, carry):
            rest_relay(t)
            settle(t, third[t] + product(t, inner_blocks), False)
            return carry

        lax.fori_loop(1, part_count, rest_step, 0)
    if part_count:
        ready = relay_from = jnp.where(gone == 0, relay_first + part_count, relay_first)
    else:
        ready, relay_from = relay_first + 1, relay_first

    def relay_step(s, carry):
        relay(s)
        if not part_count:

            @pl.when(s == ready)
            def _():
                far_affine().wait_recv()

        t_late = s - ready + part_count
        catching = jnp.logical_and(s >= ready, t_late < pieces)
        catching = jnp.logical_and(catching, per_piece * (t_late + 1) - 1 + lag <= s)
        fresh = s - (per_piece - 1) - lag
        t_fresh = lax.div(fresh, per_piece)
        arriving = jnp.logical_and(fresh >= 0, lax.rem(fresh, per_piece) == 0)
        arriving = jnp.logical_and(arriving, t_fresh < pieces)
        arriving = jnp.logical_and(arriving, ready + t_fresh - part_count < s)
        arriving = jnp.logical_and(arriving, t_fresh >= part_count)
        t = jnp.where(catching, t_late, t_fresh)
        due = jnp.logical_or(catching, arriving)
        if not part_count:

            @pl.when(jnp.logical_and(due, t == 0))
            def _():
                settle(t, product(t, list(range(n))), True)

            due = jnp.logical_and(due, t > 0)

        @pl.when(due)
        def _():
            settle(t, product(t, list(range(n))), False)

        return carry

    relay_last = jnp.maximum(units + lag, ready + pieces - part_count)
    lax.fori_loop(relay_from, relay_last, relay_step, 0)

    extra = sum3[...] / local
    stat3[b, 0:1, :] = shift3[...] + extra
    stat3[b, 1:2, :] = square3[...] - sum3[...] * extra
    stats_send(nb, b, stat3, st3_send.at[0], st3_recv.at[0])

    sent = wown.at[0, pl.ds(0, (n - 1) * strip), :]
    remote(sent, sent, w1_send.at[0], w1_recv.at[0], {"batch": partner}).wait_send()
    gb_all().wait_send()
    for to in range(n):

        @pl.when(z != to)
        def _():
            hop_all(to).wait_send()
            pair_all(to).wait_send()

    w2_sent = w2.at[0, :, :, pl.ds(0, (mids - 1) * band), :]
    right = {"chan": lax.rem(z + 1, n)}
    remote(w2_sent, w2_sent, w2_send.at[0], w2_recv.at[0, 0], right).wait_send()
    half_slots(lambda slot: w2hop_all(slot).wait_send())
    half_slots(lambda slot: w2pair_all(slot).wait_send())
    if more:
        w2_one = w2.at[0, :, :, pl.ds(0, band), :]
        w2hop_all(more_slot).wait_send()
        w2pair_all(more_slot).wait_send()

        @pl.when(inner)
        def _():
            remote(w2_one, w2_one, w2_send.at[2], w2_recv.at[0, 0], right).wait_send()

        @pl.when(gone == 0)
        def _():
            remote(w2_one, w2_one, w2_send.at[1], w2_recv.at[0, 0], right).wait_send()

    for f in range(2):

        @pl.when(z != (n - 1) * (1 - f))
        def _():
            remote(flow.at[f], flow.at[f], flow_send.at[f], flow_recv.at[f, 0], right).wait_send()

    if mids > 1:

        @pl.when(next_to_end)
        def _():
            norm_copy.wait_send()

    sec_sent = sec.at[pl.ds(0, lacking)]

    @pl.when(gone == 0)
    def _():
        for i in range(mids):
            affine_copy((1 - side) * mids + i, near_block).wait_send()
        remote(sec_sent, sec_sent, sec_send.at[0], sec_recv.at[0, 0], right).wait_send()

    @pl.when(inner)
    def _():
        remote(sec_sent, sec_sent, sec_send.at[1], sec_recv.at[0, 0], right).wait_send()

    stats_wait(nb, b, stat3, st3_send.at[0], st3_recv.at[0])
    mean3, var3 = combine(stat3[...], local)
    scale3 = gain3[...] / jnp.sqrt(var3 + eps)
    offset3 = (shift3[...] - mean3) * scale3 + bias3[...]

    def finish(t, carry):
        kept = img[pl.ds(t * join, join)].reshape(tall, out_local).astype(f32)
        value = third[t] * scale3 + offset3 + kept
        outv[t] = jnp.maximum(value, 0.0).astype(bf16)
        return carry

    lax.fori_loop(0, pieces, finish, 0)


def body(
    images,
    reduce_weight,
    reduce_gain,
    reduce_bias,
    spatial_weight,
    spatial_gain,
    spatial_bias,
    expand_weight,
    expand_gain,
    expand_bias,
):
    imgs, side = (images.shape[0], images.shape[1])
    n, nb = lax.axis_size("chan"), lax.axis_size("batch")
    width = reduce_weight.shape[1]
    depth = images.shape[3]
    out_local = expand_weight.shape[1]
    rows, height = side, side * imgs
    chunks = n * rows
    mid = n * width
    mids = n // 2
    more = EXTRA if mids > 1 else 0
    slots, lacking = mids + more, mids - more
    join = 2 if side % 2 == 0 else 1
    pieces, tall = side // join, height * join
    dma, f32, bf16 = pltpu.SemaphoreType.DMA, jnp.float32, jnp.bfloat16
    vmem = pl.BlockSpec(memory_space=pltpu.VMEM)
    anywhere = pl.BlockSpec(memory_space=pl.ANY)
    flat = images.transpose(1, 2, 0, 3).reshape(rows, height, depth)
    out = pl.pallas_call(
        functools.partial(block_kernel, n, nb, imgs),
        out_shape=pltpu.VMEM((pieces, tall, out_local), bf16),
        in_specs=[anywhere] * 10,
        out_specs=vmem,
        scratch_shapes=[
            pltpu.VMEM((rows, height, depth), bf16),
            pltpu.VMEM(reduce_weight.shape, bf16),
            pltpu.VMEM((n, depth, width), bf16),
            pltpu.VMEM((chunks, height, width), f32),
            pltpu.VMEM((2, rows, height, width), f32),
            pltpu.VMEM((2, chunks, height, width), bf16),
            pltpu.VMEM((n, 4, width), f32),
        ]
        + [pltpu.VMEM((n, 1, width), f32)] * 3
        + [
            pltpu.VMEM((n, nb, 2, width), f32),
            pltpu.VMEM((n, rows + 2, height, width), bf16),
            pltpu.VMEM((slots, 3, 3, mid, width), bf16),
            pltpu.VMEM((slots, rows, height, width), f32),
            pltpu.VMEM((n, rows, height, width), bf16),
        ]
        + [pltpu.VMEM((slots, 1, width), f32)] * 3
        + [
            pltpu.VMEM((nb, lacking, 2, width), f32),
            pltpu.VMEM((nb, 2, 2, width), f32),
            pltpu.VMEM((n, 2, width), f32),
            pltpu.VMEM(expand_weight.shape, bf16),
            pltpu.VMEM((pieces, tall, out_local), f32),
        ]
        + [pltpu.VMEM((1, out_local), f32)] * 3
        + [pltpu.VMEM((nb, 2, out_local), f32)]
        + [pltpu.VMEM((1, width), f32)] * 4
        + [pltpu.VMEM((1, out_local), f32)] * 2
        + [pltpu.VMEM((2, 2, width), f32)]
        + [dma((4,)), dma((6,)), dma((1,)), dma((1,))]
        + [dma((1,))] * 2
        + [dma((1,)), dma((n,))]
        + [dma((n,))] * 4
        + [dma((2,)), dma((2, chunks))]
        + [dma((n,))] * 2
        + [dma((3,)), dma((slots, 3))]
        + [dma((slots,))] * 4
        + [dma((2,)), dma((lacking * rows, 2))]
        + [dma((1,))] * 4
        + [dma((n,)), dma((1,))]
        + [dma((1,))] * 2,
        compiler_params=pltpu.CompilerParams(
            collective_id=0, has_side_effects=True, vmem_limit_bytes=LIMIT
        ),
        name="block",
    )(
        flat,
        reduce_weight,
        reduce_gain[None, :],
        reduce_bias[None, :],
        spatial_weight,
        spatial_gain[None, :],
        spatial_bias[None, :],
        expand_weight,
        expand_gain[None, :],
        expand_bias[None, :],
    )
    return out.reshape(side, side, imgs, out_local).transpose(2, 0, 1, 3)


def solution(mesh):
    in_specs = (
        P("batch", None, None, "chan"),
        P(None, "chan"),
        P("chan"),
        P("chan"),
        P(None, None, None, "chan"),
        P("chan"),
        P("chan"),
        P(None, "chan"),
        P("chan"),
        P("chan"),
    )
    out_specs = P("batch", None, None, "chan")
    return jax.shard_map(body, mesh=mesh, in_specs=in_specs, out_specs=out_specs, check_vma=False)
```
